512 devices in a mesh: tm: 16 (over y, x_hi), sx: 8 (over z), sy: 4 (over x_lo, core).
Axes of the slice: x: 4 (x_hi: 2, x_lo: 2; x = x_hi * 2 + x_lo), y: 8, z: 8, core: 2. Of those that a mesh axis runs over, the one named last changes fastest.
Arguments:
- driving_input: float32 [128, 8, 64, 512], P('tm', None, 'sx', 'sy'), may hold values from -4 to 4
- regime: int32 [8, 64, 512], P(None, 'sx', 'sy'), may hold values from 0 to 7
- reaction_rates: float32 [8], replicated, may hold values from 0.005 to 1
Outputs:
- solution: float32 [128, 8, 64, 512], P('tm', None, 'sx', 'sy')
The draws below stay inside these ranges and needn't reach their ends.
All inputs are finite; a program needn't handle non-finite values.
Results may differ from the reference program's by a relative error of at most 0.00007.
Values sent between devices are 32-bit elements; how exact they have to be, the bound alone decides.
No kernel may reach another device: no remote copies, remote signals or barrier semaphores. Data moves between devices by JAX's collectives and lax.ppermute only.
A program may use at most 64 MiB of HBM per device.

```python
import jax
import jax.numpy as jnp
from jax import lax

L = 128
NZ = 8
AGGREGATE_XCELLS = 8
AGGREGATE_YCELLS = 32
RATES = 8
SWEEPS = 4
NX = 64
NY = 512
NCX = 8
NCY = 16
NC = 128


def draw_driving_input(key, part):
    full_shape = (L, NZ, NX, NY)
    return jax.random.truncated_normal(key, -4.0, 4.0, full_shape, jnp.float32)


def draw_reaction_rates(key, part):
    lower_end = 0.005
    upper_end = 1.0
    exponent = jax.random.uniform(key, (RATES,), jnp.float32, jnp.log(lower_end), jnp.log(upper_end))
    return jnp.clip(jnp.exp(exponent), 0.005, 1.0)


def plant(values, rng, smallest, high):
    shape = values.shape
    place = [jax.random.randint(jax.random.fold_in(rng, axis), (), 0, shape[axis]) for axis in range(len(shape))]
    values = values.at[tuple(place)].set(smallest)
    longest = shape.index(max(shape))
    place[longest] = (place[longest] + 1) % shape[longest]
    return values.at[tuple(place)].set(high)


def setup_inputs(seed: int = 0) -> dict:
    key_list = jax.random.split(jax.random.key(seed), 4)
    return {
        "driving_input": draw_driving_input(jax.random.fold_in(key_list[3], 71), 0),
        "regime": plant(jax.random.randint(key_list[1], (NZ, NX, NY), 0, RATES), jax.random.fold_in(key_list[1], 1), 0, RATES - 1).astype(jnp.int32),
        "reaction_rates": draw_reaction_rates(jax.random.fold_in(key_list[3], 71), 0),
    }


TWO_PI = 2.0 * 3.141592653589793

def angle_table(row_index, col_index, cycle_duration):
    product = row_index[:, None] * col_index[None, :] % cycle_duration
    angles = product.astype(jnp.float32) * (TWO_PI / cycle_duration)
    return (jnp.cos(angles), jnp.sin(angles))

def matmul(left_side, right_side):
    return jnp.dot(left_side.astype(jnp.float32), right_side.astype(jnp.float32), precision=lax.Precision.HIGHEST, preferred_element_type=jnp.float32)

def complex_mul(left_real, left_imag, pair):
    return jnp.stack([left_real * pair[0] - left_imag * pair[1], left_real * pair[1] + left_imag * pair[0]])

def neighbors(present_guess):
    padded = jnp.pad(present_guess, ((0, 0), (0, 0), (1, 1), (1, 1)))
    running = padded[:, :, 2:, 1:-1] + padded[:, :, :-2, 1:-1]
    running = running + padded[:, :, 1:-1, 2:] + padded[:, :, 1:-1, :-2]
    running = running + jnp.roll(present_guess, 1, axis=1) + jnp.roll(present_guess, -1, axis=1)
    return running

def aggregate(values):
    leading = values.shape[:-3]
    blocks = values.reshape(leading + (NZ, NCX, AGGREGATE_XCELLS, NCY, AGGREGATE_YCELLS))
    return jnp.sum(blocks, axis=(-5, -3, -1)).reshape(leading + (NCX * NCY,))

def reference(driving_input, regime, reaction_rates):
    unrolled_array = driving_input.reshape(L, -1)
    all_index = jnp.arange(L, dtype=jnp.int32)
    cosine, sine = angle_table(all_index, all_index, L)
    spec_real = matmul(cosine, unrolled_array).reshape(driving_input.shape)
    spec_imag = (-matmul(sine, unrolled_array)).reshape(driving_input.shape)
    reaction = jnp.zeros(regime.shape, jnp.float32)
    for regime_no in range(RATES):
        reaction = reaction + jnp.where(regime == regime_no, reaction_rates[regime_no], jnp.zeros((), jnp.float32))
    rate_sums = aggregate(reaction)
    position = jnp.arange(NC, dtype=jnp.int32)
    coarse_x = position // NCY
    coarse_y = position % NCY
    x_gap = jnp.abs(coarse_x[:, None] - coarse_x[None, :])
    y_gap = jnp.abs(coarse_y[:, None] - coarse_y[None, :])
    coupling = -(AGGREGATE_YCELLS * NZ) * ((x_gap == 1) & (y_gap == 0)).astype(jnp.float32)
    coupling = coupling - AGGREGATE_XCELLS * NZ * ((x_gap == 0) & (y_gap == 1)).astype(jnp.float32)
    identity = (position[:, None] == position[None, :]).astype(jnp.float32)
    face_count = 2 * (AGGREGATE_YCELLS * NZ + AGGREGATE_XCELLS * NZ)
    volume = AGGREGATE_XCELLS * AGGREGATE_YCELLS * NZ
    diagonal = rate_sums + face_count

    def solve(entry_set):
        frequency, source_real, source_imag = entry_set
        phase_angle = frequency.astype(jnp.float32) * (TWO_PI / L)
        shift_real = 1.0 - jnp.cos(phase_angle)
        shift_imag = jnp.sin(phase_angle)
        diag_real = reaction + 6.0 + shift_real
        diag_imag = jnp.zeros_like(diag_real) + shift_imag
        modulus = diag_real * diag_real + diag_imag * diag_imag
        inverse_real = diag_real / modulus
        inverse_imag = -diag_imag / modulus
        source_term = jnp.stack([source_real, source_imag])
        present_guess = complex_mul(inverse_real, inverse_imag, source_term)
        for sweep_no in range(SWEEPS - 1):
            present_guess = complex_mul(inverse_real, inverse_imag, source_term + neighbors(present_guess))
        applied = complex_mul(diag_real, diag_imag, present_guess) - neighbors(present_guess)
        residual = source_term - applied
        coarse_right = jnp.transpose(aggregate(residual), (1, 0))
        system = coupling + identity * (diagonal + volume * shift_real)[None, :]
        factor = jnp.linalg.cholesky(system)
        forward_sub = lax.linalg.triangular_solve(factor, coarse_right, left_side=True, lower=True)
        coarse = lax.linalg.triangular_solve(factor, forward_sub, left_side=True, lower=True, transpose_a=True)
        local_part = jnp.transpose(coarse, (1, 0)).reshape(2, 1, NCX, 1, NCY, 1)
        spread_values = jnp.broadcast_to(local_part, (2, NZ, NCX, AGGREGATE_XCELLS, NCY, AGGREGATE_YCELLS)).reshape(2, NZ, NCX * AGGREGATE_XCELLS, NCY * AGGREGATE_YCELLS)
        return present_guess + spread_values
    corrected = lax.map(solve, (all_index, spec_real, spec_imag))
    real_part = corrected[:, 0].reshape(L, -1)
    imag_part = corrected[:, 1].reshape(L, -1)
    result = (matmul(cosine, real_part) - matmul(sine, imag_part)) / L
    return result.reshape(driving_input.shape)
```

```python
import jax
import jax.numpy as jnp
import numpy as np
from jax import lax
from jax.experimental import pallas as pl
from jax.experimental.pallas import tpu as pltpu
from jax.sharding import PartitionSpec as P

L = 128
NZ = 8
BLOCK = 8
WIDTH = 4
SPAN = BLOCK + 2 * WIDTH
TM, SX, SY = 16, 8, 4
FACES = 2 * (32 * NZ + 8 * NZ)
VOLUME = 8 * 32 * NZ
COUPLE_X = 32.0 * NZ
COUPLE_Y = 8.0 * NZ
INTERPRET = False


def strip_of(d):
    return d // 2 if d % 2 == 0 else TM - 1 - d // 2


MEMBER = {strip_of(d): d for d in range(TM)}


def tables():
    n = np.arange(L)
    k = np.arange(64)
    ang = 2.0 * np.pi * ((n[:, None] * k[None, :]) % L) / L
    half = np.where(n % 2 == 0, 1.0, -1.0)
    forward = np.concatenate([np.cos(ang), -np.sin(ang)], axis=1)
    forward[:, 64] = half
    weight = np.full((1, 64), 2.0)
    weight[0, 0] = 1.0
    inverse = np.concatenate([weight * np.cos(ang), -weight * np.sin(ang)], axis=1) / L
    inverse[:, 64] = half / L
    theta = 2.0 * np.pi * k / L
    shift = np.concatenate([1.0 - np.cos(theta)] * 2)
    shift[64] = 2.0
    sine = np.concatenate([np.sin(theta), -np.sin(theta)])
    sine[0] = sine[64] = 0.0
    order = np.array([8 * d + 2 * tp + t2 for t2 in range(2) for d in range(TM) for tp in range(4)])
    lanes = np.zeros((8, L))
    lanes[0] = shift
    lanes[1] = sine
    as32 = lambda a: np.asarray(a, np.float32)
    return as32(forward[order]), as32(inverse[order]), as32(lanes)


FORWARD, INVERSE, LANES = tables()


def vmem(count):
    return [pl.BlockSpec(memory_space=pltpu.VMEM)] * count


def smem(count):
    return [pl.BlockSpec(memory_space=pltpu.SMEM)] * count


def shape(*dims):
    return jax.ShapeDtypeStruct(dims, jnp.float32)


def dot(a, b, dims):
    return lax.dot_general(
        a, b, (dims, ((), ())), precision=lax.Precision.HIGHEST, preferred_element_type=jnp.float32
    )


def lane_index(rows):
    return lax.broadcasted_iota(jnp.int32, (rows, L), 1)


def halves(low, high):
    first = lane_index(low.shape[0]) < 64
    return (
        jnp.where(first, low, pltpu.roll(high, 64, 1)),
        jnp.where(first, pltpu.roll(low, 64, 1), high),
    )


def pack_kernel(rates, field, regime, out, rate_rows, sums):
    for tp in range(4):
        rows = [
            field[pl.ds((2 * tp + t2) * 64 + x, 8, stride=8), :] for t2 in range(2) for x in range(8)
        ]
        turned = jnp.concatenate(rows, axis=0).T
        for d in range(TM):
            s = strip_of(d)
            out[d, tp] = turned[8 * s : 8 * s + 8]
    columns = []
    for x in range(8):
        kind = regime[pl.ds(x, 8, stride=8), :]
        c = jnp.zeros((8, L), jnp.float32)
        for r in range(8):
            c = c + jnp.where(kind == r, rates[r], 0.0)
        columns.append(c)
    columns.append(jnp.zeros((64, L), jnp.float32))
    c_turned = jnp.concatenate(columns, axis=0).T
    rate_rows[...] = c_turned
    sums[0:4, :] = jnp.zeros((4, L), jnp.float32)
    for g in range(4):
        total = jnp.sum(c_turned[32 * g : 32 * g + 32], axis=0, keepdims=True)
        total = jnp.sum(total, axis=1, keepdims=True)
        sums[4 + g : 5 + g, :] = jnp.broadcast_to(total, (1, L))


def transform_kernel(place, received, rate_rows, table, low, high):
    rows = []
    for pair in range(4):
        both = [received[pl.ds(2 * pair + j, 64, stride=8), :] for j in range(2)]
        turned = jnp.concatenate(both, axis=0).T
        rows += list(halves(turned[:64], turned[64:]))
    spectrum = dot(jnp.concatenate(rows, axis=0), table[...], ((1,), (0,)))
    start = pl.multiple_of(place[0] * 8, 8)
    own = rate_rows[pl.ds(start, 8), :]
    for y in range(8):
        part = low if y < 4 else high
        for x in range(8):
            r = (y * 8 + x) * 8
            part[(y % 4) * 8 + x] = spectrum[r : r + 8]
    low[32] = own
    high[32] = pltpu.roll(own, 4, 0)


def x_range(distance):
    return range(distance, SPAN - distance)


def edge_tiles():
    return [(d, y) for d in range(1, WIDTH + 1) for y in x_range(d)]


EDGE = edge_tiles()


def strip_rows(below, low, high, above):
    parts = (below, low, high, above)
    return lambda y, x: parts[y // 4][(y % 4) * 8 + x]


def edge_kernel(below, low, high, above, to_left, to_right):
    tile = strip_rows(below, low, high, above)
    for i, (d, y) in enumerate(EDGE):
        to_left[i] = tile(y, d - 1)
        to_right[i] = tile(y, 8 - d)
    for j, (first, second) in enumerate(((below, low), (high, above))):
        c = jnp.concatenate([first[32][0:4], second[32][0:4]], axis=0)
        to_left[len(EDGE) + j] = c
        to_right[len(EDGE) + j] = c


def solve_kernel(
    valid, below, low, high, above, left, right, lanes, own, total, source, a, b, x0, x1, rate
):
    tile = strip_rows(below, low, high, above)
    zero = jnp.zeros((8, L), jnp.float32)
    for y in range(SPAN):
        for x in range(WIDTH):
            source[y, x] = zero
            source[y, SPAN - 1 - x] = zero
        for x in range(8):
            source[y, WIDTH + x] = tile(y, x)
    for i, (d, y) in enumerate(EDGE):
        source[y, WIDTH - d] = left[i]
        source[y, WIDTH + 7 + d] = right[i]
    lane = lane_index(8)
    for j, (first, second) in enumerate(((below, low), (high, above))):
        mid = jnp.concatenate([first[32][0:4], second[32][0:4]], axis=0)
        c = jnp.where(
            lane < 32,
            pltpu.roll(left[len(EDGE) + j], 96, 1),
            jnp.where(lane < 96, pltpu.roll(mid, 32, 1), pltpu.roll(right[len(EDGE) + j], 96, 1)),
        )
        rate[8 * j : 8 * j + 8, :] = c
    base = lanes[0:1, :] + 6.0
    sine = lanes[1:2, :]
    sine_square = sine * sine

    def prepare(y, carry):
        row = rate[pl.ds(y, 1), :]
        spread = jnp.broadcast_to(row, (L, L)).T
        row_ok = jnp.where(y < WIDTH, valid[2], jnp.where(y < SPAN - WIDTH, 1.0, valid[3]))
        for x in range(SPAN):
            ok = row_ok
            if x < WIDTH:
                ok = row_ok * valid[0]
            elif x >= SPAN - WIDTH:
                ok = row_ok * valid[1]
            d = spread[8 * x : 8 * x + 8] + base
            inverse = ok / (d * d + sine_square)
            ax = d * inverse
            bx = sine * inverse
            a[y, x] = ax
            b[y, x] = bx
            s = source[y, x]
            x0[y, x] = ax * s + bx * pltpu.roll(s, 64, 1)
        return carry

    lax.fori_loop(0, SPAN, prepare, 0)

    def sweep(old, new, margin):
        def row(y, carry):
            for x in range(margin, SPAN - margin):
                v = old[y, x]
                u = source[y, x] + (old[y, x + 1] + old[y, x - 1])
                u = u + (old[y + 1, x] + old[y - 1, x])
                u = u + (pltpu.roll(v, 1, 0) + pltpu.roll(v, 7, 0))
                new[y, x] = a[y, x] * u + b[y, x] * pltpu.roll(u, 64, 1)
            return carry

        lax.fori_loop(margin, SPAN - margin, row, 0)

    sweep(x0, x1, 1)
    sweep(x1, x0, 2)
    sweep(x0, x1, 3)
    lo, hi = WIDTH, WIDTH + BLOCK

    def change(y, x):
        return x1[y, x] - x0[y, x]

    acc = zero
    for y in range(lo - 1, hi + 1):
        line = zero
        for x in range(lo, hi):
            line = line + change(y, x)
        inner = lo <= y < hi
        times = (4 if inner else 0) + (1 if lo - 1 <= y < hi - 1 else 0) + (1 if lo + 1 <= y <= hi else 0)
        acc = acc + float(times) * line
        if inner:
            acc = acc + (change(y, lo - 1) - change(y, lo)) + (change(y, hi) - change(y, hi - 1))
            for x in range(lo, hi):
                own[y - lo, x - lo] = x1[y, x]
    row = jnp.sum(acc, axis=0, keepdims=True)
    for d in range(TM):
        total[d] = row


def gather_kernel(partial, sums, out):
    rows = []
    for g in range(4):
        row = partial[MEMBER[4 * g]]
        for s in range(4 * g + 1, 4 * g + 4):
            row = row + partial[MEMBER[s]]
        rows.append(row)
    block = jnp.concatenate(rows + [sums[4:8, :]], axis=0)
    for j in range(SX * SY):
        out[j] = block


def inverse_of(rows):
    rows = list(rows)
    index = lax.broadcasted_iota(jnp.int32, (8, L), 0)
    for p in range(8):
        here = index == p
        pivot = jnp.broadcast_to(rows[p][p : p + 1], (8, L))
        scale = 1.0 / pivot
        lead = jnp.where(here, scale, rows[p] * scale)
        for r in range(8):
            if r != p:
                factor = jnp.broadcast_to(rows[r][p : p + 1], (8, L))
                rows[r] = jnp.where(here, 0.0, rows[r]) - factor * lead
        rows[p] = lead
    return rows


def apply(rows, v):
    terms = [rows[c] * jnp.broadcast_to(v[c : c + 1], (8, L)) for c in range(8)]
    while len(terms) > 1:
        terms = [terms[i] + terms[i + 1] for i in range(0, len(terms), 2)]
    return terms[0]


def coarse_kernel(place, gathered, field, lanes, table, out, answer):
    index = lax.broadcasted_iota(jnp.int32, (8, L), 0)
    shift = lanes[0:1, :] * float(VOLUME) + float(FACES)

    def right(m):
        return gathered[pl.ds((m // 4) * 8 + m % 4, 8, stride=32), :]

    def block(m, before):
        diagonal = gathered[pl.ds((m // 4) * 8 + 4 + m % 4, 8, stride=32), :] + shift
        rows = []
        for r in range(8):
            row = jnp.where(index == r, diagonal, 0.0)
            row = jnp.where((index == r - 1) | (index == r + 1), -COUPLE_X, row)
            for other in before:
                row = row - (COUPLE_Y * COUPLE_Y) * other[r]
            rows.append(row)
        return rows

    inv, part = {}, {}

    def eliminate(m, sources):
        matrix = inverse_of(block(m, [inv[q] for q in sources]))
        rhs = right(m)
        for q in sources:
            rhs = rhs + COUPLE_Y * part[q]
        inv[m] = matrix
        part[m] = apply(matrix, rhs)

    for i in range(8):
        if i < 7:
            eliminate(i, [i - 1] if i else [])
        eliminate(15 - i, [16 - i] if i else [])
    eliminate(7, [6, 8])
    solved = {7: part[7]}
    for i in range(1, 9):
        for m, q in ((7 - i, 8 - i), (7 + i, 6 + i)):
            if 0 <= m < 16:
                solved[m] = part[m] + COUPLE_Y * apply(inv[m], solved[q])
    for m in range(16):
        answer[8 * m : 8 * m + 8, :] = solved[m]
    mine = answer[pl.ds(place[1], 1), :]
    corrected = field[...] + mine
    result = dot(table[...], corrected, ((1,), (1,)))
    for pair in range(4):
        cut = result[:, 128 * pair : 128 * pair + 128]
        for j, value in enumerate(halves(cut[:64], cut[64:])):
            out[pl.ds(2 * pair + j, 64, stride=8), :] = value


def unpack_kernel(received, out):
    for tp in range(4):
        rows = [received[MEMBER[s], tp] for s in range(TM)]
        turned = jnp.concatenate(rows, axis=0).T
        for t2 in range(2):
            for x in range(8):
                r = t2 * 64 + x * 8
                out[pl.ds((2 * tp + t2) * 64 + x, 8, stride=8), :] = turned[r : r + 8]


def call(kernel, name, out_shape, scalars, arrays, scratch=()):
    outs = out_shape if isinstance(out_shape, tuple) else (out_shape,)
    return pl.pallas_call(
        kernel,
        name=name,
        out_shape=out_shape,
        in_specs=smem(len(scalars)) + vmem(len(arrays)),
        out_specs=tuple(vmem(len(outs))) if isinstance(out_shape, tuple) else vmem(1)[0],
        scratch_shapes=list(scratch),
        interpret=INTERPRET,
    )(*scalars, *arrays)


def y_steps():
    def rank(g):
        return MEMBER[g % TM] * SY + g // TM

    return [(rank(g), rank(g + 1)) for g in range(SY * TM - 1)]


def local(driving_input, regime, reaction_rates):
    tm, sx, sy = (lax.axis_index(n) for n in ("tm", "sx", "sy"))
    strip = jnp.where(tm % 2 == 0, tm // 2, TM - 1 - tm // 2)
    place = jnp.stack([strip, (sy * 4 + strip // 4) * 8 + sx]).astype(jnp.int32)
    inside = jnp.stack(
        [sx > 0, sx < SX - 1, (sy > 0) | (strip > 0), (sy < SY - 1) | (strip < TM - 1)]
    ).astype(jnp.float32)
    forward, inverse, lanes = jnp.asarray(FORWARD), jnp.asarray(INVERSE), jnp.asarray(LANES)

    packed, rate_rows, sums = call(
        pack_kernel,
        "pack",
        (shape(TM, 4, 8, L), shape(L, L), shape(8, L)),
        [reaction_rates],
        [driving_input.reshape(512, L), regime.reshape(64, L)],
    )
    received = lax.all_to_all(packed, "tm", split_axis=0, concat_axis=0, tiled=True)
    low, high = call(
        transform_kernel,
        "transform",
        (shape(33, 8, L), shape(33, 8, L)),
        [place],
        [received.reshape(512, L), rate_rows, forward],
    )
    up = y_steps()
    below = lax.ppermute(high, ("tm", "sy"), up)
    above = lax.ppermute(low, ("tm", "sy"), [(q, p) for p, q in up])
    tiles = len(EDGE) + 2
    to_left, to_right = call(
        edge_kernel, "edges", (shape(tiles, 8, L),) * 2, [], [below, low, high, above]
    )
    across = [(i, i + 1) for i in range(SX - 1)]
    left = lax.ppermute(to_right, "sx", across)
    right = lax.ppermute(to_left, "sx", [(q, p) for p, q in across])
    big = pltpu.VMEM((SPAN, SPAN, 8, L), jnp.float32)
    own, total = call(
        solve_kernel,
        "sweeps",
        (shape(8, 8, 8, L), shape(TM, 1, L)),
        [inside],
        [below, low, high, above, left, right, lanes],
        [big] * 5 + [pltpu.VMEM((SPAN, L), jnp.float32)],
    )
    partial = lax.all_to_all(total, "tm", split_axis=0, concat_axis=0, tiled=True)
    shared = call(gather_kernel, "gather", shape(SX * SY, 8, L), [], [partial, sums])
    gathered = lax.all_to_all(shared, ("sx", "sy"), split_axis=0, concat_axis=0, tiled=True)
    back = call(
        coarse_kernel,
        "coarse",
        shape(512, L),
        [place],
        [gathered.reshape(256, L), own.reshape(512, L), lanes, inverse],
        [pltpu.VMEM((L, L), jnp.float32)],
    )
    returned = lax.all_to_all(
        back.reshape(TM, 4, 8, L), "tm", split_axis=0, concat_axis=0, tiled=True
    )
    result = call(unpack_kernel, "unpack", shape(512, L), [], [returned])
    return result.reshape(driving_input.shape)


def solution(mesh):
    placed = (P("tm", None, "sx", "sy"), P(None, "sx", "sy"), P())
    return jax.shard_map(
        local, mesh=mesh, in_specs=placed, out_specs=P("tm", None, "sx", "sy"), check_vma=False
    )
```

```python
import jax
import jax.numpy as jnp
import numpy as np
from jax import lax
from jax.experimental import pallas as pl
from jax.experimental.pallas import tpu as pltpu
from jax.sharding import PartitionSpec as P

L = 128
NZ = 8
BLOCK = 8
WIDTH = 4
SPAN = BLOCK + 2 * WIDTH
TM, SX, SY = 16, 8, 4
FACES = 2 * (32 * NZ + 8 * NZ)
VOLUME = 8 * 32 * NZ
COUPLE_X = 32.0 * NZ
COUPLE_Y = 8.0 * NZ
TILES = 5


def strip_of(d):
    return d // 2 if d % 2 == 0 else TM - 1 - d // 2


MEMBER = {strip_of(d): d for d in range(TM)}


def tables():
    n = np.arange(L)
    k = np.arange(64)
    ang = 2.0 * np.pi * ((n[:, None] * k[None, :]) % L) / L
    half = np.where(n % 2 == 0, 1.0, -1.0)
    forward = np.concatenate([np.cos(ang), -np.sin(ang)], axis=1)
    forward[:, 64] = half
    weight = np.full((1, 64), 2.0)
    weight[0, 0] = 1.0
    inverse = np.concatenate([weight * np.cos(ang), -weight * np.sin(ang)], axis=1) / L
    inverse[:, 64] = half / L
    theta = 2.0 * np.pi * k / L
    shift = np.concatenate([1.0 - np.cos(theta)] * 2)
    shift[64] = 2.0
    sine = np.concatenate([np.sin(theta), -np.sin(theta)])
    sine[0] = sine[64] = 0.0
    order = np.array([8 * d + 2 * tp + t2 for t2 in range(2) for d in range(TM) for tp in range(4)])
    lanes = np.zeros((8, L))
    lanes[0] = shift
    lanes[1] = sine
    padded = np.zeros((2, TM, TILES, L))
    padded[:, :, :4] = inverse[order].reshape(2, TM, 4, L)
    as32 = lambda a: np.asarray(a, np.float32)
    return as32(forward[order]), as32(padded.reshape(-1, L)), as32(inverse), as32(lanes)


FORWARD, INVERSE, NATURAL, LANES = tables()


def vmem(count):
    return [pl.BlockSpec(memory_space=pltpu.VMEM)] * count


def smem(count):
    return [pl.BlockSpec(memory_space=pltpu.SMEM)] * count


def shape(*dims):
    return jax.ShapeDtypeStruct(dims, jnp.float32)


def dot(a, b, dims):
    return lax.dot_general(
        a, b, (dims, ((), ())), precision=lax.Precision.HIGHEST, preferred_element_type=jnp.float32
    )


def lane_index(rows):
    return lax.broadcasted_iota(jnp.int32, (rows, L), 1)


def halves(low, high):
    first = lane_index(low.shape[0]) < 64
    return (
        jnp.where(first, low, pltpu.roll(high, 64, 1)),
        jnp.where(first, pltpu.roll(low, 64, 1), high),
    )


def pack_kernel(rates, field, regime, out, rate_rows, sums):
    for tp in range(4):
        rows = [
            field[pl.ds((2 * tp + t2) * 64 + x, 8, stride=8), :] for t2 in range(2) for x in range(8)
        ]
        turned = jnp.concatenate(rows, axis=0).T
        for d in range(TM):
            s = strip_of(d)
            out[d, tp] = turned[8 * s : 8 * s + 8]
    columns = []
    for x in range(8):
        kind = regime[pl.ds(x, 8, stride=8), :]
        c = jnp.zeros((8, L), jnp.float32)
        for r in range(8):
            c = c + jnp.where(kind == r, rates[r], 0.0)
        columns.append(c)
    columns.append(jnp.zeros((64, L), jnp.float32))
    c_turned = jnp.concatenate(columns, axis=0).T
    rate_rows[...] = c_turned
    sums[0:4, :] = jnp.zeros((4, L), jnp.float32)
    for g in range(4):
        total = jnp.sum(c_turned[32 * g : 32 * g + 32], axis=0, keepdims=True)
        total = jnp.sum(total, axis=1, keepdims=True)
        sums[4 + g : 5 + g, :] = jnp.broadcast_to(total, (1, L))


def own_strip():
    tm = lax.axis_index("tm")
    return jnp.where(tm & 1 == 0, tm >> 1, TM - 1 - (tm >> 1))


def transform_kernel(received, rate_rows, table, low, high):
    rows = []
    for pair in range(4):
        both = [received[pl.ds(2 * pair + j, 64, stride=8), :] for j in range(2)]
        turned = jnp.concatenate(both, axis=0).T
        rows += list(halves(turned[:64], turned[64:]))
    spectrum = dot(jnp.concatenate(rows, axis=0), table[...], ((1,), (0,)))
    own = rate_rows[pl.ds(pl.multiple_of(own_strip() * 8, 8), 8), :]
    for y in range(8):
        part = low if y < 4 else high
        for x in range(8):
            r = (y * 8 + x) * 8
            part[(y % 4) * 8 + x] = spectrum[r : r + 8]
    low[32] = own
    high[32] = pltpu.roll(own, 4, 0)


def x_range(distance):
    return range(distance, SPAN - distance)


def edge_tiles():
    return [(d, y) for d in range(1, WIDTH + 1) for y in x_range(d)]


EDGE = edge_tiles()


def strip_rows(below, low, high, above):
    parts = (below, low, high, above)
    return lambda y, x: parts[y // 4][(y % 4) * 8 + x]


def edge_kernel(below, low, high, above, to_left, to_right):
    tile = strip_rows(below, low, high, above)
    for i, (d, y) in enumerate(EDGE):
        to_left[i] = tile(y, d - 1)
        to_right[i] = tile(y, 8 - d)
    for j, (first, second) in enumerate(((below, low), (high, above))):
        c = jnp.concatenate([first[32][0:4], second[32][0:4]], axis=0)
        to_left[len(EDGE) + j] = c
        to_right[len(EDGE) + j] = c


def solve_kernel(
    below, low, high, above, left, right, lanes, table, out, source, a, b, x0, x1, rate
):
    sx, sy, strip = lax.axis_index("sx"), lax.axis_index("sy"), own_strip()
    valid = [
        jnp.where(inside, 1.0, 0.0)
        for inside in (
            sx > 0,
            sx < SX - 1,
            (sy > 0) | (strip > 0),
            (sy < SY - 1) | (strip < TM - 1),
        )
    ]
    tile = strip_rows(below, low, high, above)
    zero = jnp.zeros((8, L), jnp.float32)
    for y in range(SPAN):
        for x in range(WIDTH):
            source[y, x] = zero
            source[y, SPAN - 1 - x] = zero
        for x in range(8):
            source[y, WIDTH + x] = tile(y, x)
    for i, (d, y) in enumerate(EDGE):
        source[y, WIDTH - d] = left[i]
        source[y, WIDTH + 7 + d] = right[i]
    lane = lane_index(8)
    for j, (first, second) in enumerate(((below, low), (high, above))):
        mid = jnp.concatenate([first[32][0:4], second[32][0:4]], axis=0)
        c = jnp.where(
            lane < 32,
            pltpu.roll(left[len(EDGE) + j], 96, 1),
            jnp.where(lane < 96, pltpu.roll(mid, 32, 1), pltpu.roll(right[len(EDGE) + j], 96, 1)),
        )
        rate[8 * j : 8 * j + 8, :] = c
    base = lanes[0:1, :] + 6.0
    sine = lanes[1:2, :]
    sine_square = sine * sine

    def prepare(y, carry):
        row = rate[pl.ds(y, 1), :]
        spread = jnp.broadcast_to(row, (L, L)).T
        row_ok = jnp.where(y < WIDTH, valid[2], jnp.where(y < SPAN - WIDTH, 1.0, valid[3]))
        for x in range(SPAN):
            ok = row_ok
            if x < WIDTH:
                ok = row_ok * valid[0]
            elif x >= SPAN - WIDTH:
                ok = row_ok * valid[1]
            d = spread[8 * x : 8 * x + 8] + base
            inverse = ok / (d * d + sine_square)
            ax = d * inverse
            bx = sine * inverse
            a[y, x] = ax
            b[y, x] = bx
            s = source[y, x]
            x0[y, x] = ax * s + bx * pltpu.roll(s, 64, 1)
        return carry

    lax.fori_loop(0, SPAN, prepare, 0)

    def sweep(old, new, margin):
        def row(y, carry):
            for x in range(margin, SPAN - margin):
                v = old[y, x]
                u = source[y, x] + (old[y, x + 1] + old[y, x - 1])
                u = u + (old[y + 1, x] + old[y - 1, x])
                u = u + (pltpu.roll(v, 1, 0) + pltpu.roll(v, 7, 0))
                new[y, x] = a[y, x] * u + b[y, x] * pltpu.roll(u, 64, 1)
            return carry

        lax.fori_loop(margin, SPAN - margin, row, 0)

    sweep(x0, x1, 1)
    sweep(x1, x0, 2)
    sweep(x0, x1, 3)
    lo, hi = WIDTH, WIDTH + BLOCK

    def change(y, x):
        return x1[y, x] - x0[y, x]

    acc = zero
    for y in range(lo - 1, hi + 1):
        line = zero
        for x in range(lo, hi):
            line = line + change(y, x)
        inner = lo <= y < hi
        times = (4 if inner else 0) + (1 if lo - 1 <= y < hi - 1 else 0) + (1 if lo + 1 <= y <= hi else 0)
        acc = acc + float(times) * line
        if inner:
            acc = acc + (change(y, lo - 1) - change(y, lo)) + (change(y, hi) - change(y, hi - 1))
    own = x1[lo:hi, lo:hi].reshape(512, L)
    result = dot(table[...], own, ((1,), (1,)))
    for pair in range(4):
        cut = result[:, 128 * pair : 128 * pair + 128]
        for j, value in enumerate(halves(cut[: TM * TILES], cut[TM * TILES :])):
            out[pl.ds(2 * pair + j, TM * TILES, stride=8), :] = value
    row = jnp.broadcast_to(jnp.sum(acc, axis=0, keepdims=True), (8, L))
    for d in range(TM):
        out[8 * (TILES * d + 4) : 8 * (TILES * d + 5), :] = row


def gather_kernel(received, sums, out):
    rows = []
    for g in range(4):
        row = received[MEMBER[4 * g], 4][0:1]
        for s in range(4 * g + 1, 4 * g + 4):
            row = row + received[MEMBER[s], 4][0:1]
        rows.append(row)
    block = jnp.concatenate(rows + [sums[4:8, :]], axis=0)
    for j in range(SX * SY):
        out[j] = block


def inverse_of(rows):
    rows = list(rows)
    index = lax.broadcasted_iota(jnp.int32, (8, L), 0)
    for p in range(8):
        here = index == p
        pivot = jnp.broadcast_to(rows[p][p : p + 1], (8, L))
        scale = 1.0 / pivot
        lead = jnp.where(here, scale, rows[p] * scale)
        for r in range(8):
            if r != p:
                factor = jnp.broadcast_to(rows[r][p : p + 1], (8, L))
                rows[r] = jnp.where(here, 0.0, rows[r]) - factor * lead
        rows[p] = lead
    return rows


def apply(rows, v):
    terms = [rows[c] * jnp.broadcast_to(v[c : c + 1], (8, L)) for c in range(8)]
    while len(terms) > 1:
        terms = [terms[i] + terms[i + 1] for i in range(0, len(terms), 2)]
    return terms[0]


def coarse_kernel(gathered, field, lanes, table, out, answer):
    index = lax.broadcasted_iota(jnp.int32, (8, L), 0)
    shift = lanes[0:1, :] * float(VOLUME) + float(FACES)

    def right(m):
        return gathered[pl.ds((m // 4) * 8 + m % 4, 8, stride=32), :]

    def block(m, before):
        diagonal = gathered[pl.ds((m // 4) * 8 + 4 + m % 4, 8, stride=32), :] + shift
        rows = []
        for r in range(8):
            row = jnp.where(index == r, diagonal, 0.0)
            row = jnp.where((index == r - 1) | (index == r + 1), -COUPLE_X, row)
            for other in before:
                row = row - (COUPLE_Y * COUPLE_Y) * other[r]
            rows.append(row)
        return rows

    inv, part = {}, {}

    def eliminate(m, sources):
        matrix = inverse_of(block(m, [inv[q] for q in sources]))
        rhs = right(m)
        for q in sources:
            rhs = rhs + COUPLE_Y * part[q]
        inv[m] = matrix
        part[m] = apply(matrix, rhs)

    for i in range(8):
        if i < 7:
            eliminate(i, [i - 1] if i else [])
        eliminate(15 - i, [16 - i] if i else [])
    eliminate(7, [6, 8])
    solved = {7: part[7]}
    for i in range(1, 9):
        for m, q in ((7 - i, 8 - i), (7 + i, 6 + i)):
            if 0 <= m < 16:
                solved[m] = part[m] + COUPLE_Y * apply(inv[m], solved[q])
    for m in range(16):
        answer[8 * m : 8 * m + 8, :] = solved[m]
    sx, sy = lax.axis_index("sx"), lax.axis_index("sy")
    own = table[pl.ds(pl.multiple_of(lax.axis_index("tm") * 8, 8), 8), :]
    group = lane_index(8) // 32
    added = jnp.zeros((8, L), jnp.float32)
    for g in range(4):
        y = answer[pl.ds((sy * 4 + g) * 8 + sx, 1), :]
        value = jnp.sum(own * y, axis=1, keepdims=True)
        added = jnp.where(group == g, value, added)
    for t in range(8):
        out[64 * t : 64 * t + 64, :] = field[64 * t : 64 * t + 64, :] + added[t : t + 1, :]


def unpack_kernel(received, out):
    for tp in range(4):
        rows = [received[MEMBER[s], tp] for s in range(TM)]
        turned = jnp.concatenate(rows, axis=0).T
        for t2 in range(2):
            for x in range(8):
                r = t2 * 64 + x * 8
                out[pl.ds((2 * tp + t2) * 64 + x, 8, stride=8), :] = turned[r : r + 8]


def call(kernel, name, out_shape, arrays, scratch=(), rates=None, keep=True, flops=0):
    if keep:
        out_shape = jax.tree.map(lambda o: pltpu.VMEM(o.shape, o.dtype), out_shape)
    if rates is None:
        arrays = [pltpu.with_memory_space_constraint(x, pltpu.VMEM) for x in arrays]
    scalars = [] if rates is None else [rates]
    many = isinstance(out_shape, tuple)
    return pl.pallas_call(
        kernel,
        name=name,
        out_shape=out_shape,
        in_specs=smem(len(scalars)) + vmem(len(arrays)),
        out_specs=tuple(vmem(len(out_shape))) if many else vmem(1)[0],
        scratch_shapes=list(scratch),
        cost_estimate=pl.CostEstimate(flops=flops, transcendentals=0, bytes_accessed=0),
    )(*scalars, *arrays)


def y_steps():
    def rank(g):
        return MEMBER[g % TM] * SY + g // TM

    return [(rank(g), rank(g + 1)) for g in range(SY * TM - 1)]


def local(driving_input, regime, reaction_rates):
    forward, inverse, natural, lanes = (jnp.asarray(t) for t in (FORWARD, INVERSE, NATURAL, LANES))
    packed, rate_rows, sums = call(
        pack_kernel,
        "pack",
        (shape(TM, 4, 8, L), shape(L, L), shape(8, L)),
        [driving_input.reshape(512, L), regime.reshape(64, L)],
        rates=reaction_rates,
    )
    received = lax.all_to_all(packed, "tm", split_axis=0, concat_axis=0, tiled=True)
    low, high = call(
        transform_kernel,
        "transform",
        (shape(33, 8, L), shape(33, 8, L)),
        [received.reshape(512, L), rate_rows, forward],
    )
    up = y_steps()
    below = lax.ppermute(high, ("tm", "sy"), up)
    above = lax.ppermute(low, ("tm", "sy"), [(q, p) for p, q in up])
    tiles = len(EDGE) + 2
    to_left, to_right = call(
        edge_kernel, "edges", (shape(tiles, 8, L),) * 2, [below, low, high, above]
    )
    across = [(i, i + 1) for i in range(SX - 1)]
    left = lax.ppermute(to_right, "sx", across)
    right = lax.ppermute(to_left, "sx", [(q, p) for p, q in across])
    big = pltpu.VMEM((SPAN, SPAN, 8, L), jnp.float32)
    message = call(
        solve_kernel,
        "sweeps",
        shape(TM * TILES * 8, L),
        [below, low, high, above, left, right, lanes, inverse],
        [big] * 5 + [pltpu.VMEM((SPAN, L), jnp.float32)],
    )
    returned = lax.all_to_all(
        message.reshape(TM, TILES, 8, L), "tm", split_axis=0, concat_axis=0, tiled=True
    )
    shared = call(gather_kernel, "gather", shape(SX * SY, 8, L), [returned, sums])
    gathered = lax.all_to_all(shared, ("sx", "sy"), split_axis=0, concat_axis=0, tiled=True)
    field = call(unpack_kernel, "unpack", shape(512, L), [returned], flops=10**8)
    result = call(
        coarse_kernel,
        "coarse",
        shape(512, L),
        [gathered.reshape(256, L), field, lanes, natural],
        [pltpu.VMEM((L, L), jnp.float32)],
        keep=False,
    )
    return result.reshape(driving_input.shape)


def solution(mesh):
    placed = (P("tm", None, "sx", "sy"), P(None, "sx", "sy"), P())
    return jax.shard_map(
        local, mesh=mesh, in_specs=placed, out_specs=P("tm", None, "sx", "sy"), check_vma=False
    )
```

```python
import jax
import jax.numpy as jnp
import numpy as np
from jax import lax
from jax.experimental import pallas as pl
from jax.experimental.pallas import tpu as pltpu
from jax.sharding import PartitionSpec as P

L = 128
NZ = 8
BLOCK = 8
WY = 3
WX = 4
SPAN_Y = BLOCK + 2 * WY
SPAN_X = BLOCK + 2 * WX
PART = 8 * WY + 1
TM, SX, SY = 16, 8, 4
FACES = 2 * (32 * NZ + 8 * NZ)
VOLUME = 8 * 32 * NZ
COUPLE_X = 32.0 * NZ
COUPLE_Y = 8.0 * NZ
TILES = 5


def strip_of(d):
    return d // 2 if d % 2 == 0 else TM - 1 - d // 2


MEMBER = {strip_of(d): d for d in range(TM)}


def tables():
    n = np.arange(L)
    k = np.arange(64)
    ang = 2.0 * np.pi * ((n[:, None] * k[None, :]) % L) / L
    half = np.where(n % 2 == 0, 1.0, -1.0)
    forward = np.concatenate([np.cos(ang), -np.sin(ang)], axis=1)
    forward[:, 64] = half
    weight = np.full((1, 64), 2.0)
    weight[0, 0] = 1.0
    inverse = np.concatenate([weight * np.cos(ang), -weight * np.sin(ang)], axis=1) / L
    inverse[:, 64] = half / L
    theta = 2.0 * np.pi * k / L
    shift = np.concatenate([1.0 - np.cos(theta)] * 2)
    shift[64] = 2.0
    sine = np.concatenate([np.sin(theta), -np.sin(theta)])
    sine[0] = sine[64] = 0.0
    order = np.array([8 * d + 2 * tp + t2 for t2 in range(2) for d in range(TM) for tp in range(4)])
    lanes = np.zeros((8, L))
    lanes[0] = shift
    lanes[1] = sine
    padded = np.zeros((2, TM, TILES, L))
    padded[:, :, :4] = inverse[order].reshape(2, TM, 4, L)
    as32 = lambda a: np.asarray(a, np.float32)
    return as32(forward[order]), as32(padded.reshape(-1, L)), as32(inverse), as32(lanes)


FORWARD, INVERSE, NATURAL, LANES = tables()


def vmem(count):
    return [pl.BlockSpec(memory_space=pltpu.VMEM)] * count


def smem(count):
    return [pl.BlockSpec(memory_space=pltpu.SMEM)] * count


def shape(*dims):
    return jax.ShapeDtypeStruct(dims, jnp.float32)


def dot(a, b, dims):
    return lax.dot_general(
        a, b, (dims, ((), ())), precision=lax.Precision.HIGHEST, preferred_element_type=jnp.float32
    )


def lane_index(rows):
    return lax.broadcasted_iota(jnp.int32, (rows, L), 1)


def halves(low, high):
    first = lane_index(low.shape[0]) < 64
    return (
        jnp.where(first, low, pltpu.roll(high, 64, 1)),
        jnp.where(first, pltpu.roll(low, 64, 1), high),
    )


def pack_kernel(rates, field, regime, out, rate_rows, sums):
    for tp in range(4):
        rows = [
            field[pl.ds((2 * tp + t2) * 64 + x, 8, stride=8), :] for t2 in range(2) for x in range(8)
        ]
        turned = jnp.concatenate(rows, axis=0).T
        for d in range(TM):
            s = strip_of(d)
            out[d, tp] = turned[8 * s : 8 * s + 8]
    columns = []
    for x in range(8):
        kind = regime[pl.ds(x, 8, stride=8), :]
        c = jnp.zeros((8, L), jnp.float32)
        for r in range(8):
            c = c + jnp.where(kind == r, rates[r], 0.0)
        columns.append(c)
    columns.append(jnp.zeros((64, L), jnp.float32))
    c_turned = jnp.concatenate(columns, axis=0).T
    rate_rows[...] = c_turned
    group = lane_index(1) // 32
    row = jnp.zeros((1, L), jnp.float32)
    for g in range(4):
        total = jnp.sum(c_turned[32 * g : 32 * g + 32], axis=0, keepdims=True)
        row = jnp.where(group == g, jnp.sum(total, axis=1, keepdims=True), row)
    sums[...] = jnp.broadcast_to(row, (8, L))


def own_strip():
    tm = lax.axis_index("tm")
    return jnp.where(tm & 1 == 0, tm >> 1, TM - 1 - (tm >> 1))


def transform_kernel(received, rate_rows, table, own, rate, low, high):
    rows = []
    for pair in range(4):
        both = [received[pl.ds(2 * pair + j, 64, stride=8), :] for j in range(2)]
        turned = jnp.concatenate(both, axis=0).T
        rows += list(halves(turned[:64], turned[64:]))
    spectrum = dot(jnp.concatenate(rows, axis=0), table[...], ((1,), (0,)))
    mine = rate_rows[pl.ds(pl.multiple_of(own_strip() * 8, 8), 8), :]
    for y in range(8):
        for x in range(8):
            r = (y * 8 + x) * 8
            own[8 * y + x] = spectrum[r : r + 8]
            if y < WY:
                low[8 * y + x] = spectrum[r : r + 8]
            if y >= 8 - WY:
                high[8 * (y - 8 + WY) + x] = spectrum[r : r + 8]
    rate[...] = mine
    low[PART - 1] = mine
    high[PART - 1] = pltpu.roll(mine, WY, 0)


def x_range(distance):
    return range(distance - 1, SPAN_Y + 1 - distance)


EDGE = [(d, y) for d in range(1, WX + 1) for y in x_range(d)]


def strip_rows(below, own, above):
    def tile(y, x):
        if y < WY:
            return below[8 * y + x]
        if y < WY + 8:
            return own[8 * (y - WY) + x]
        return above[8 * (y - WY - 8) + x]

    return tile


def strip_rates(below, rate, above):
    rows = [below[PART - 1][0:WY], rate[...], above[PART - 1][0:WY], jnp.zeros((2, L), jnp.float32)]
    rows = jnp.concatenate(rows, axis=0)
    return rows[0:8], rows[8:16]


def edge_kernel(below, own, rate, above, to_left, to_right):
    tile = strip_rows(below, own, above)
    for i, (d, y) in enumerate(EDGE):
        to_left[i] = tile(y, d - 1)
        to_right[i] = tile(y, 8 - d)
    for j, c in enumerate(strip_rates(below, rate, above)):
        to_left[len(EDGE) + j] = c
        to_right[len(EDGE) + j] = c


def solve_kernel(
    below, own, rate, above, left, right, lanes, table, out, source, a, b, x0, x1
):
    sx, sy, strip = lax.axis_index("sx"), lax.axis_index("sy"), own_strip()
    valid = [
        jnp.where(inside, 1.0, 0.0)
        for inside in (
            sx > 0,
            sx < SX - 1,
            (sy > 0) | (strip > 0),
            (sy < SY - 1) | (strip < TM - 1),
        )
    ]
    tile = strip_rows(below, own, above)
    zero = jnp.zeros((8, L), jnp.float32)
    for y in range(SPAN_Y):
        for x in range(WX):
            source[y, x] = zero
            source[y, SPAN_X - 1 - x] = zero
        for x in range(8):
            source[y, WX + x] = tile(y, x)
    for i, (d, y) in enumerate(EDGE):
        source[y, WX - d] = left[i]
        source[y, WX + 7 + d] = right[i]
    lane = lane_index(8)
    rows = []
    for j, mid in enumerate(strip_rates(below, rate, above)):
        rows.append(
            jnp.where(
                lane < 32,
                pltpu.roll(left[len(EDGE) + j], 96, 1),
                jnp.where(
                    lane < 96, pltpu.roll(mid, 32, 1), pltpu.roll(right[len(EDGE) + j], 96, 1)
                ),
            )
        )
    rows.append(jnp.zeros((112, L), jnp.float32))
    turned = jnp.concatenate(rows, axis=0).T
    base = jnp.broadcast_to(lanes[0:1, :] + 6.0, (8, L))
    sine = jnp.broadcast_to(lanes[1:2, :], (8, L))
    sine_square = sine * sine
    for y in range(SPAN_Y):
        for x in range(SPAN_X):
            d = jnp.broadcast_to(turned[8 * x : 8 * x + 8, y : y + 1], (8, L)) + base
            inverse = 1.0 / (d * d + sine_square)
            if x < WX:
                inverse = inverse * valid[0]
            elif x >= WX + 8:
                inverse = inverse * valid[1]
            if y < WY:
                inverse = inverse * valid[2]
            elif y >= WY + 8:
                inverse = inverse * valid[3]
            ax = d * inverse
            bx = sine * inverse
            a[y, x] = ax
            b[y, x] = bx
            s = source[y, x]
            x0[y, x] = ax * s + bx * pltpu.roll(s, 64, 1)

    def sweep(old, new, margin):
        def row(y, carry):
            for x in range(margin, SPAN_X - margin):
                v = old[y, x]
                u = source[y, x] + (old[y, x + 1] + old[y, x - 1])
                u = u + (old[y + 1, x] + old[y - 1, x])
                u = u + (pltpu.roll(v, 1, 0) + pltpu.roll(v, 7, 0))
                new[y, x] = a[y, x] * u + b[y, x] * pltpu.roll(u, 64, 1)
            return carry

        lax.fori_loop(margin, SPAN_Y - margin, row, 0)

    sweep(x0, x1, 1)
    sweep(x1, x0, 2)
    sweep(x0, x1, 3)
    lo, hi = WX, WX + 8

    def change(y, x):
        return x1[y, x] - x0[y, x]

    acc = zero
    faces = []
    for y in range(WY, WY + 8):
        line = zero
        for x in range(lo, hi):
            line = line + change(y, x)
        end = y in (WY, WY + 7)
        acc = acc + (5.0 if end else 6.0) * line
        acc = acc + (change(y, lo - 1) - change(y, lo)) + (change(y, hi) - change(y, hi - 1))
        if end:
            faces.append(line)
    solved = x1[WY : WY + 8, lo:hi].reshape(512, L)
    result = dot(table[...], solved, ((1,), (1,)))
    for pair in range(4):
        cut = result[:, 128 * pair : 128 * pair + 128]
        for j, value in enumerate(halves(cut[: TM * TILES], cut[TM * TILES :])):
            out[pl.ds(2 * pair + j, TM * TILES, stride=8), :] = value
    rows = [jnp.sum(v, axis=0, keepdims=True) for v in (acc, *faces)]
    rows = jnp.concatenate(rows + [jnp.zeros((5, L), jnp.float32)], axis=0)
    for d in range(TM):
        out[8 * (TILES * d + 4) : 8 * (TILES * d + 5), :] = rows


def gather_kernel(received, sums, out):
    part = [received[MEMBER[s], 4] for s in range(TM)]
    rows = []
    for g in range(4):
        row = part[4 * g][0:1]
        for s in range(4 * g + 1, 4 * g + 4):
            row = row + part[s][0:1]
        for s in range(4 * g, 4 * g + 4):
            if s > 0:
                row = row + part[s - 1][2:3]
            if s < TM - 1:
                row = row + part[s + 1][1:2]
        rows.append(row)
    rows += [part[0][1:2], part[TM - 1][2:3], sums[0:1, :], jnp.zeros((1, L), jnp.float32)]
    block = jnp.concatenate(rows, axis=0)
    for j in range(SX * SY):
        out[j] = block


def inverse_of(rows):
    rows = list(rows)
    index = lax.broadcasted_iota(jnp.int32, (8, L), 0)
    for p in range(8):
        here = index == p
        pivot = jnp.broadcast_to(rows[p][p : p + 1], (8, L))
        scale = 1.0 / pivot
        lead = jnp.where(here, scale, rows[p] * scale)
        for r in range(8):
            if r != p:
                factor = jnp.broadcast_to(rows[r][p : p + 1], (8, L))
                rows[r] = jnp.where(here, 0.0, rows[r]) - factor * lead
        rows[p] = lead
    return rows


def apply(rows, v):
    terms = [rows[c] * jnp.broadcast_to(v[c : c + 1], (8, L)) for c in range(8)]
    while len(terms) > 1:
        terms = [terms[i] + terms[i + 1] for i in range(0, len(terms), 2)]
    return terms[0]


def coarse_kernel(gathered, received, lanes, table, out, answer):
    index = lax.broadcasted_iota(jnp.int32, (8, L), 0)
    shift = jnp.broadcast_to(lanes[0:1, :] * float(VOLUME) + float(FACES), (8, L))

    def rows_of(sy, row):
        return gathered[pl.ds(sy * 8 + row, 8, stride=32), :]

    def right(m):
        sy, g = m // 4, m % 4
        rhs = rows_of(sy, g)
        if g == 0 and sy > 0:
            rhs = rhs + rows_of(sy - 1, 5)
        if g == 3 and sy < SY - 1:
            rhs = rhs + rows_of(sy + 1, 4)
        return rhs

    sums = [rows_of(sy, 6) for sy in range(SY)]

    def block(m, before):
        g = 32 * (m % 4)
        diagonal = jnp.broadcast_to(sums[m // 4][:, g : g + 1], (8, L)) + shift
        rows = []
        for r in range(8):
            row = jnp.where(index == r, diagonal, 0.0)
            row = jnp.where((index == r - 1) | (index == r + 1), -COUPLE_X, row)
            for other in before:
                row = row - (COUPLE_Y * COUPLE_Y) * other[r]
            rows.append(row)
        return rows

    inv, part = {}, {}

    def eliminate(m, sources):
        matrix = inverse_of(block(m, [inv[q] for q in sources]))
        rhs = right(m)
        for q in sources:
            rhs = rhs + COUPLE_Y * part[q]
        inv[m] = matrix
        part[m] = apply(matrix, rhs)

    for i in range(8):
        if i < 7:
            eliminate(i, [i - 1] if i else [])
        eliminate(15 - i, [16 - i] if i else [])
    eliminate(7, [6, 8])
    solved = {7: part[7]}
    for i in range(1, 9):
        for m, q in ((7 - i, 8 - i), (7 + i, 6 + i)):
            if 0 <= m < 16:
                solved[m] = part[m] + COUPLE_Y * apply(inv[m], solved[q])
    for m in range(16):
        answer[8 * m : 8 * m + 8, :] = solved[m]
    sx, sy = lax.axis_index("sx"), lax.axis_index("sy")
    own = table[pl.ds(pl.multiple_of(lax.axis_index("tm") * 8, 8), 8), :]
    group = lane_index(8) // 32
    added = jnp.zeros((8, L), jnp.float32)
    for g in range(4):
        y = answer[pl.ds((sy * 4 + g) * 8 + sx, 1), :]
        value = jnp.sum(own * y, axis=1, keepdims=True)
        added = jnp.where(group == g, value, added)
    for tp in range(4):
        rows = [received[MEMBER[s], tp] for s in range(TM)]
        turned = jnp.concatenate(rows, axis=0).T
        for t2 in range(2):
            t = 2 * tp + t2
            plus = jnp.broadcast_to(added[t : t + 1, :], (8, L))
            for x in range(8):
                r = t2 * 64 + x * 8
                out[pl.ds(t * 64 + x, 8, stride=8), :] = turned[r : r + 8] + plus


def call(kernel, name, out_shape, arrays, scratch=(), rates=None, keep=True):
    if keep:
        out_shape = jax.tree.map(lambda o: pltpu.VMEM(o.shape, o.dtype), out_shape)
    if rates is None:
        arrays = [pltpu.with_memory_space_constraint(x, pltpu.VMEM) for x in arrays]
    scalars = [] if rates is None else [rates]
    many = isinstance(out_shape, tuple)
    return pl.pallas_call(
        kernel,
        name=name,
        out_shape=out_shape,
        in_specs=smem(len(scalars)) + vmem(len(arrays)),
        out_specs=tuple(vmem(len(out_shape))) if many else vmem(1)[0],
        scratch_shapes=list(scratch),
    )(*scalars, *arrays)


def y_steps():
    def rank(g):
        return MEMBER[g % TM] * SY + g // TM

    return [(rank(g), rank(g + 1)) for g in range(SY * TM - 1)]


def local(driving_input, regime, reaction_rates):
    forward, inverse, natural, lanes = (jnp.asarray(t) for t in (FORWARD, INVERSE, NATURAL, LANES))
    packed, rate_rows, sums = call(
        pack_kernel,
        "pack",
        (shape(TM, 4, 8, L), shape(L, L), shape(8, L)),
        [driving_input.reshape(512, L), regime.reshape(64, L)],
        rates=reaction_rates,
    )
    received = lax.all_to_all(packed, "tm", split_axis=0, concat_axis=0, tiled=True)
    own, rate, low, high = call(
        transform_kernel,
        "transform",
        (shape(64, 8, L), shape(8, L), shape(PART, 8, L), shape(PART, 8, L)),
        [received.reshape(512, L), rate_rows, forward],
    )
    up = y_steps()
    below = lax.ppermute(high, ("tm", "sy"), up)
    above = lax.ppermute(low, ("tm", "sy"), [(q, p) for p, q in up])
    tiles = len(EDGE) + 2
    to_left, to_right = call(
        edge_kernel, "edges", (shape(tiles, 8, L),) * 2, [below, own, rate, above]
    )
    across = [(i, i + 1) for i in range(SX - 1)]
    left = lax.ppermute(to_right, "sx", across)
    right = lax.ppermute(to_left, "sx", [(q, p) for p, q in across])
    message = call(
        solve_kernel,
        "sweeps",
        shape(TM * TILES * 8, L),
        [below, own, rate, above, left, right, lanes, inverse],
        [pltpu.VMEM((SPAN_Y, SPAN_X, 8, L), jnp.float32)] * 5,
    )
    returned = lax.all_to_all(
        message.reshape(TM, TILES, 8, L), "tm", split_axis=0, concat_axis=0, tiled=True
    )
    shared = call(gather_kernel, "gather", shape(SX * SY, 8, L), [returned, sums])
    gathered = lax.all_to_all(shared, ("sx", "sy"), split_axis=0, concat_axis=0, tiled=True)
    result = call(
        coarse_kernel,
        "coarse",
        shape(512, L),
        [gathered.reshape(256, L), returned, lanes, natural],
        [pltpu.VMEM((L, L), jnp.float32)],
        keep=False,
    )
    return result.reshape(driving_input.shape)


def solution(mesh):
    placed = (P("tm", None, "sx", "sy"), P(None, "sx", "sy"), P())
    return jax.shard_map(
        local, mesh=mesh, in_specs=placed, out_specs=P("tm", None, "sx", "sy"), check_vma=False
    )
```

```python
import jax
import jax.numpy as jnp
import numpy as np
from jax import lax
from jax.experimental import pallas as pl
from jax.experimental.pallas import tpu as pltpu
from jax.sharding import PartitionSpec as P

L = 128
NZ = 8
BLOCK = 8
WY = 3
WX = 4
SPAN_Y = BLOCK + 2 * WY
SPAN_X = BLOCK + 2 * WX
PART = 8 * WY + 1
TM, SX, SY = 16, 8, 4
FACES = 2 * (32 * NZ + 8 * NZ)
VOLUME = 8 * 32 * NZ
COUPLE_X = 32.0 * NZ
COUPLE_Y = 8.0 * NZ
TILES = 5


def strip_of(d):
    return d // 2 if d % 2 == 0 else TM - 1 - d // 2


MEMBER = {strip_of(d): d for d in range(TM)}


def tables():
    n = np.arange(L)
    k = np.arange(64)
    ang = 2.0 * np.pi * ((n[:, None] * k[None, :]) % L) / L
    half = np.where(n % 2 == 0, 1.0, -1.0)
    forward = np.concatenate([np.cos(ang), -np.sin(ang)], axis=1)
    forward[:, 64] = half
    weight = np.full((1, 64), 2.0)
    weight[0, 0] = 1.0
    inverse = np.concatenate([weight * np.cos(ang), -weight * np.sin(ang)], axis=1) / L
    inverse[:, 64] = half / L
    theta = 2.0 * np.pi * k / L
    shift = np.concatenate([1.0 - np.cos(theta)] * 2)
    shift[64] = 2.0
    sine = np.concatenate([np.sin(theta), -np.sin(theta)])
    sine[0] = sine[64] = 0.0
    order = np.array([8 * d + 2 * tp + t2 for t2 in range(2) for d in range(TM) for tp in range(4)])
    lanes = np.zeros((8, L))
    lanes[0] = shift
    lanes[1] = sine
    padded = np.zeros((2, TM, TILES, L))
    padded[:, :, :4] = inverse[order].reshape(2, TM, 4, L)
    as32 = lambda a: np.asarray(a, np.float32)
    return as32(forward[order]), as32(padded.reshape(-1, L)), as32(inverse), as32(lanes)


FORWARD, INVERSE, NATURAL, LANES = tables()


def vmem(count):
    return [pl.BlockSpec(memory_space=pltpu.VMEM)] * count


def smem(count):
    return [pl.BlockSpec(memory_space=pltpu.SMEM)] * count


def shape(*dims):
    return jax.ShapeDtypeStruct(dims, jnp.float32)


def dot(a, b, dims):
    return lax.dot_general(
        a, b, (dims, ((), ())), precision=lax.Precision.HIGHEST, preferred_element_type=jnp.float32
    )


def lane_index(rows):
    return lax.broadcasted_iota(jnp.int32, (rows, L), 1)


def halves(low, high):
    first = lane_index(low.shape[0]) < 64
    return (
        jnp.where(first, low, pltpu.roll(high, 64, 1)),
        jnp.where(first, pltpu.roll(low, 64, 1), high),
    )


def pack_kernel(rates, field, regime, out, rate_rows, sums):
    margin = jnp.zeros((8, L), jnp.float32)
    for tp in range(4):
        rows = [
            field[pl.ds((2 * tp + t2) * 64 + x, 8, stride=8), :] for t2 in range(2) for x in range(8)
        ]
        turned = jnp.concatenate(rows, axis=0).T
        shifted = jnp.concatenate([margin[:WY], turned, margin], axis=0)
        for d in range(TM):
            s = strip_of(d)
            out[d, SPAN_Y * tp : SPAN_Y * (tp + 1)] = shifted[8 * s : 8 * s + SPAN_Y]
    columns = []
    for x in range(8):
        kind = regime[pl.ds(x, 8, stride=8), :]
        c = jnp.zeros((8, L), jnp.float32)
        for r in range(8):
            c = c + jnp.where(kind == r, rates[r], 0.0)
        columns.append(c)
    columns.append(jnp.zeros((64, L), jnp.float32))
    c_turned = jnp.concatenate(columns, axis=0).T
    rate_rows[...] = jnp.concatenate([margin, c_turned, margin], axis=0)
    group = lane_index(1) // 32
    row = jnp.zeros((1, L), jnp.float32)
    for g in range(4):
        total = jnp.sum(c_turned[32 * g : 32 * g + 32], axis=0, keepdims=True)
        row = jnp.where(group == g, jnp.sum(total, axis=1, keepdims=True), row)
    sums[...] = jnp.broadcast_to(row, (8, L))


def own_strip():
    tm = lax.axis_index("tm")
    return jnp.where(tm & 1 == 0, tm >> 1, TM - 1 - (tm >> 1))


def transform_kernel(received, rate_rows, table, window, rate, swap):
    rows = []
    for pair in range(SPAN_Y // 2):
        both = [received[pl.ds(2 * pair + j, 64, stride=SPAN_Y), :] for j in range(2)]
        turned = jnp.concatenate(both, axis=0).T
        rows += list(halves(turned[:64], turned[64:]))
    spectrum = dot(jnp.concatenate(rows, axis=0), table[...], ((1,), (0,)))
    for i in range(8 * SPAN_Y):
        window[i] = spectrum[8 * i : 8 * i + 8]
    strip = own_strip()
    near = rate_rows[pl.ds(pl.multiple_of(strip * 8, 8), 24), :]
    mine = jnp.concatenate([near[8 - WY : 16 + WY], jnp.zeros((2, L), jnp.float32)], axis=0)
    rate[...] = mine
    first = strip == 0
    for i in range(8 * WY):
        swap[i] = jnp.where(first, window[8 * WY + i], window[64 + i])
    swap[PART - 1] = jnp.where(first, pltpu.roll(mine[0:8], 8 - WY, 0), mine[8:16])


def x_range(distance):
    return range(distance - 1, SPAN_Y + 1 - distance)


EDGE = [(d, y) for d in range(1, WX + 1) for y in x_range(d)]


def completed(window, rate, swapped):
    strip = own_strip()
    first = jnp.where(strip == 0, 1.0, 0.0)
    last = jnp.where(strip == TM - 1, 1.0, 0.0)

    def tile(y, x):
        if y < WY:
            return window[8 * y + x] + first * swapped[8 * y + x]
        if y < WY + 8:
            return window[8 * y + x]
        return window[8 * y + x] + last * swapped[8 * (y - WY - 8) + x]

    row = lax.broadcasted_iota(jnp.int32, (8, L), 0)
    other = jnp.where(row < WY, swapped[PART - 1], 0.0)
    low = rate[0:8, :] + first * other
    high = rate[8:16, :] + last * pltpu.roll(other, WY, 0)
    return tile, (low, high)


def edge_kernel(window, rate, swapped, to_left, to_right):
    tile, rates = completed(window, rate, swapped)
    for i, (d, y) in enumerate(EDGE):
        to_left[i] = tile(y, d - 1)
        to_right[i] = tile(y, 8 - d)
    for j, c in enumerate(rates):
        to_left[len(EDGE) + j] = c
        to_right[len(EDGE) + j] = c


def solve_kernel(
    window, rate, swapped, left, right, sums, lanes, table, out, source, a, b, x0, x1
):
    sx, sy, strip = lax.axis_index("sx"), lax.axis_index("sy"), own_strip()
    valid = [
        jnp.where(inside, 1.0, 0.0)
        for inside in (
            sx > 0,
            sx < SX - 1,
            (sy > 0) | (strip > 0),
            (sy < SY - 1) | (strip < TM - 1),
        )
    ]
    tile, rates = completed(window, rate, swapped)
    zero = jnp.zeros((8, L), jnp.float32)
    for y in range(SPAN_Y):
        for x in range(WX):
            source[y, x] = zero
            source[y, SPAN_X - 1 - x] = zero
        for x in range(8):
            source[y, WX + x] = tile(y, x)
    for i, (d, y) in enumerate(EDGE):
        source[y, WX - d] = left[i]
        source[y, WX + 7 + d] = right[i]
    lane = lane_index(8)
    rows = []
    for j, mid in enumerate(rates):
        rows.append(
            jnp.where(
                lane < 32,
                pltpu.roll(left[len(EDGE) + j], 96, 1),
                jnp.where(
                    lane < 96, pltpu.roll(mid, 32, 1), pltpu.roll(right[len(EDGE) + j], 96, 1)
                ),
            )
        )
    rows.append(jnp.zeros((112, L), jnp.float32))
    turned = jnp.concatenate(rows, axis=0).T
    base = jnp.broadcast_to(lanes[0:1, :] + 6.0, (8, L))
    sine = jnp.broadcast_to(lanes[1:2, :], (8, L))
    sine_square = sine * sine

    def prepare(y, turned):
        row_ok = jnp.where(y < WY, valid[2], jnp.where(y < WY + 8, 1.0, valid[3]))
        for x in range(SPAN_X):
            ok = row_ok
            if x < WX:
                ok = row_ok * valid[0]
            elif x >= WX + 8:
                ok = row_ok * valid[1]
            d = jnp.broadcast_to(turned[8 * x : 8 * x + 8, 0:1], (8, L)) + base
            inverse = ok / (d * d + sine_square)
            ax = d * inverse
            bx = sine * inverse
            a[y, x] = ax
            b[y, x] = bx
            s = source[y, x]
            x0[y, x] = ax * s + bx * pltpu.roll(s, 64, 1)
        return pltpu.roll(turned, L - 1, 1)

    lax.fori_loop(0, SPAN_Y, prepare, turned)

    def sweep(old, new, margin):
        def row(y, carry):
            for x in range(margin, SPAN_X - margin):
                v = old[y, x]
                u = source[y, x] + (old[y, x + 1] + old[y, x - 1])
                u = u + (old[y + 1, x] + old[y - 1, x])
                u = u + (pltpu.roll(v, 1, 0) + pltpu.roll(v, 7, 0))
                new[y, x] = a[y, x] * u + b[y, x] * pltpu.roll(u, 64, 1)
            return carry

        lax.fori_loop(margin, SPAN_Y - margin, row, 0)

    sweep(x0, x1, 1)
    sweep(x1, x0, 2)
    sweep(x0, x1, 3)
    lo, hi = WX, WX + 8

    def change(y, x):
        return x1[y, x] - x0[y, x]

    acc = zero
    faces = []
    for y in range(WY, WY + 8):
        line = zero
        for x in range(lo, hi):
            line = line + change(y, x)
        end = y in (WY, WY + 7)
        acc = acc + (5.0 if end else 6.0) * line
        acc = acc + (change(y, lo - 1) - change(y, lo)) + (change(y, hi) - change(y, hi - 1))
        if end:
            faces.append(line)
    solved = x1[WY : WY + 8, lo:hi].reshape(512, L)
    result = dot(table[...], solved, ((1,), (1,)))
    for pair in range(4):
        cut = result[:, 128 * pair : 128 * pair + 128]
        for j, value in enumerate(halves(cut[: TM * TILES], cut[TM * TILES :])):
            out[pl.ds(2 * pair + j, TM * TILES, stride=8), :] = value
    homes = (
        strip >> 2,
        jnp.where(strip == 0, 4, (strip - 1) >> 2),
        jnp.where(strip == TM - 1, 5, (strip + 1) >> 2),
    )
    index = lax.broadcasted_iota(jnp.int32, (8, L), 0)
    share = jnp.where((index == 6) & (strip == 0), sums[...], 0.0)
    for home, v in zip(homes, (acc, *faces)):
        v = jnp.broadcast_to(jnp.sum(v, axis=0, keepdims=True), (8, L))
        share = share + jnp.where(index == home, v, 0.0)
    for d in range(TM):
        out[8 * (TILES * d + 4) : 8 * (TILES * d + 5), :] = share


def gather_kernel(received, out):
    block = received[0, 4]
    for d in range(1, TM):
        block = block + received[d, 4]
    for j in range(SX * SY):
        out[j] = block


def inverse_of(rows):
    rows = list(rows)
    index = lax.broadcasted_iota(jnp.int32, (8, L), 0)
    for p in range(8):
        here = index == p
        pivot = jnp.broadcast_to(rows[p][p : p + 1], (8, L))
        scale = 1.0 / pivot
        lead = jnp.where(here, scale, rows[p] * scale)
        for r in range(8):
            if r != p:
                factor = jnp.broadcast_to(rows[r][p : p + 1], (8, L))
                rows[r] = jnp.where(here, 0.0, rows[r]) - factor * lead
        rows[p] = lead
    return rows


def apply(rows, v):
    terms = [rows[c] * jnp.broadcast_to(v[c : c + 1], (8, L)) for c in range(8)]
    while len(terms) > 1:
        terms = [terms[i] + terms[i + 1] for i in range(0, len(terms), 2)]
    return terms[0]


def coarse_kernel(gathered, received, lanes, table, out, answer, diagonal, rhs, inverses):
    index = lax.broadcasted_iota(jnp.int32, (8, L), 0)
    shift = jnp.broadcast_to(lanes[0:1, :] * float(VOLUME) + float(FACES), (8, L))

    def rows_of(sy, row):
        return gathered[pl.ds(sy * 8 + row, 8, stride=32), :]

    for sy in range(SY):
        sums = rows_of(sy, 6)
        for g in range(4):
            f = rows_of(sy, g)
            if g == 0 and sy > 0:
                f = f + rows_of(sy - 1, 5)
            if g == 3 and sy < SY - 1:
                f = f + rows_of(sy + 1, 4)
            rhs[4 * sy + g] = f
            diagonal[4 * sy + g] = jnp.broadcast_to(sums[:, 32 * g : 32 * g + 1], (8, L)) + shift

    def eliminate(m, before):
        d = diagonal[m]
        f = rhs[m]
        rows = []
        for r in range(8):
            row = jnp.where(index == r, d, 0.0)
            row = jnp.where((index == r - 1) | (index == r + 1), -COUPLE_X, row)
            for other, _ in before:
                row = row - (COUPLE_Y * COUPLE_Y) * other[r]
            rows.append(row)
        for _, part in before:
            f = f + COUPLE_Y * part
        matrix = inverse_of(rows)
        part = apply(matrix, f)
        for r in range(8):
            inverses[m, r] = matrix[r]
        rhs[m] = part
        return matrix, part

    def both_ends(i, carry):
        return eliminate(i, [carry[0]]), eliminate(15 - i, [carry[1]])

    nothing = ([jnp.zeros((8, L), jnp.float32)] * 8, jnp.zeros((8, L), jnp.float32))
    top, bottom = lax.fori_loop(0, 7, both_ends, (nothing, nothing))
    bottom = eliminate(8, [bottom])
    _, middle = eliminate(7, [top, bottom])
    answer[7] = middle

    def back(m, solved):
        result = rhs[m] + COUPLE_Y * apply([inverses[m, r] for r in range(8)], solved)
        answer[m] = result
        return result

    def outward(i, carry):
        return back(7 - i, carry[0]), back(8 + i, carry[1])

    below = back(8, middle)
    lax.fori_loop(1, 8, outward, (middle, below))
    sx, sy = lax.axis_index("sx"), lax.axis_index("sy")
    own = table[pl.ds(pl.multiple_of(lax.axis_index("tm") * 8, 8), 8), :]
    group = lane_index(8) // 32
    added = jnp.zeros((8, L), jnp.float32)
    for g in range(4):
        y = answer[sy * 4 + g, pl.ds(sx, 1), :]
        value = jnp.sum(own * y, axis=1, keepdims=True)
        added = jnp.where(group == g, value, added)
    for tp in range(4):
        rows = [received[MEMBER[s], tp] for s in range(TM)]
        turned = jnp.concatenate(rows, axis=0).T
        for t2 in range(2):
            t = 2 * tp + t2
            plus = jnp.broadcast_to(added[t : t + 1, :], (8, L))
            for x in range(8):
                r = t2 * 64 + x * 8
                out[pl.ds(t * 64 + x, 8, stride=8), :] = turned[r : r + 8] + plus


def call(kernel, name, out_shape, arrays, scratch=(), rates=None, keep=True):
    if keep:
        out_shape = jax.tree.map(lambda o: pltpu.VMEM(o.shape, o.dtype), out_shape)
    if rates is None:
        arrays = [pltpu.with_memory_space_constraint(x, pltpu.VMEM) for x in arrays]
    scalars = [] if rates is None else [rates]
    many = isinstance(out_shape, tuple)
    return pl.pallas_call(
        kernel,
        name=name,
        out_shape=out_shape,
        in_specs=smem(len(scalars)) + vmem(len(arrays)),
        out_specs=tuple(vmem(len(out_shape))) if many else vmem(1)[0],
        scratch_shapes=list(scratch),
    )(*scalars, *arrays)


def block_swaps():
    pairs = [(MEMBER[TM - 1] * SY + sy, MEMBER[0] * SY + sy + 1) for sy in range(SY - 1)]
    return pairs + [(q, p) for p, q in pairs]


def local(driving_input, regime, reaction_rates):
    forward, inverse, natural, lanes = (jnp.asarray(t) for t in (FORWARD, INVERSE, NATURAL, LANES))
    packed, rate_rows, sums = call(
        pack_kernel,
        "pack",
        (shape(TM, 4 * SPAN_Y, L), shape(L + 16, L), shape(8, L)),
        [driving_input.reshape(512, L), regime.reshape(64, L)],
        rates=reaction_rates,
    )
    received = lax.all_to_all(packed, "tm", split_axis=0, concat_axis=0, tiled=True)
    window, rate, swap = call(
        transform_kernel,
        "transform",
        (shape(8 * SPAN_Y, 8, L), shape(16, L), shape(PART, 8, L)),
        [received.reshape(TM * 4 * SPAN_Y, L), rate_rows, forward],
    )
    swapped = lax.ppermute(swap, ("tm", "sy"), block_swaps())
    tiles = len(EDGE) + 2
    to_left, to_right = call(
        edge_kernel, "edges", (shape(tiles, 8, L),) * 2, [window, rate, swapped]
    )
    across = [(i, i + 1) for i in range(SX - 1)]
    left = lax.ppermute(to_right, "sx", across)
    right = lax.ppermute(to_left, "sx", [(q, p) for p, q in across])
    message = call(
        solve_kernel,
        "sweeps",
        shape(TM * TILES * 8, L),
        [window, rate, swapped, left, right, sums, lanes, inverse],
        [pltpu.VMEM((SPAN_Y, SPAN_X, 8, L), jnp.float32)] * 5,
    )
    returned = lax.all_to_all(
        message.reshape(TM, TILES, 8, L), "tm", split_axis=0, concat_axis=0, tiled=True
    )
    shared = call(gather_kernel, "gather", shape(SX * SY, 8, L), [returned])
    gathered = lax.all_to_all(shared, ("sx", "sy"), split_axis=0, concat_axis=0, tiled=True)
    result = call(
        coarse_kernel,
        "coarse",
        shape(512, L),
        [gathered.reshape(256, L), returned, lanes, natural],
        [pltpu.VMEM((16, 8, L), jnp.float32)] * 3 + [pltpu.VMEM((16, 8, 8, L), jnp.float32)],
        keep=False,
    )
    return result.reshape(driving_input.shape)


def solution(mesh):
    placed = (P("tm", None, "sx", "sy"), P(None, "sx", "sy"), P())
    return jax.shard_map(
        local, mesh=mesh, in_specs=placed, out_specs=P("tm", None, "sx", "sy"), check_vma=False
    )
```

```python
import jax
import jax.numpy as jnp
import numpy as np
from jax import lax
from jax.experimental import pallas as pl
from jax.experimental.pallas import tpu as pltpu
from jax.sharding import PartitionSpec as P

L = 128
NZ = 8
BLOCK = 8
WY = 3
WX = 4
SPAN_Y = BLOCK + 2 * WY
SPAN_X = BLOCK + 2 * WX
ROWS = 12
PART = 8 * WY + 1
TM, SX, SY = 16, 8, 4
FACES = 2 * (32 * NZ + 8 * NZ)
VOLUME = 8 * 32 * NZ
COUPLE_X = 32.0 * NZ
COUPLE_Y = 8.0 * NZ
TILES = 5


def strip_of(d):
    return d // 2 if d % 2 == 0 else TM - 1 - d // 2


MEMBER = {strip_of(d): d for d in range(TM)}


def tables():
    n = np.arange(L)
    k = np.arange(64)
    ang = 2.0 * np.pi * ((n[:, None] * k[None, :]) % L) / L
    half = np.where(n % 2 == 0, 1.0, -1.0)
    forward = np.concatenate([np.cos(ang), -np.sin(ang)], axis=1)
    forward[:, 64] = half
    weight = np.full((1, 64), 2.0)
    weight[0, 0] = 1.0
    inverse = np.concatenate([weight * np.cos(ang), -weight * np.sin(ang)], axis=1) / L
    inverse[:, 64] = half / L
    theta = 2.0 * np.pi * k / L
    shift = np.concatenate([1.0 - np.cos(theta)] * 2)
    shift[64] = 2.0
    sine = np.concatenate([np.sin(theta), -np.sin(theta)])
    sine[0] = sine[64] = 0.0
    order = np.array([8 * d + 2 * tp + t2 for t2 in range(2) for d in range(TM) for tp in range(4)])
    lanes = np.zeros((8, L))
    lanes[0] = shift
    lanes[1] = sine
    padded = np.zeros((2, TM, TILES, L))
    padded[:, :, :4] = inverse[order].reshape(2, TM, 4, L)
    as32 = lambda a: np.asarray(a, np.float32)
    return as32(forward[order]), as32(padded.reshape(-1, L)), as32(inverse), as32(lanes)


FORWARD, INVERSE, NATURAL, LANES = tables()


def vmem(count):
    return [pl.BlockSpec(memory_space=pltpu.VMEM)] * count


def smem(count):
    return [pl.BlockSpec(memory_space=pltpu.SMEM)] * count


def shape(*dims):
    return jax.ShapeDtypeStruct(dims, jnp.float32)


def dot(a, b, dims):
    return lax.dot_general(
        a, b, (dims, ((), ())), precision=lax.Precision.HIGHEST, preferred_element_type=jnp.float32
    )


def lane_index(rows):
    return lax.broadcasted_iota(jnp.int32, (rows, L), 1)


def halves(low, high):
    first = lane_index(low.shape[0]) < 64
    return (
        jnp.where(first, low, pltpu.roll(high, 64, 1)),
        jnp.where(first, pltpu.roll(low, 64, 1), high),
    )


def pack_kernel(rates, field, regime, out, rate_rows, sums):
    margin = jnp.zeros((8, L), jnp.float32)
    for tp in range(4):
        rows = [
            field[pl.ds((2 * tp + t2) * 64 + x, 8, stride=8), :] for t2 in range(2) for x in range(8)
        ]
        turned = jnp.concatenate(rows, axis=0).T
        starts = (
            jnp.concatenate([turned, margin], axis=0),
            jnp.concatenate([margin[:WY], turned, margin[WY:]], axis=0),
        )
        for d in range(TM):
            s = strip_of(d)
            out[d, ROWS * tp : ROWS * (tp + 1)] = starts[s % 2][8 * s : 8 * s + ROWS]
    columns = []
    for x in range(8):
        kind = regime[pl.ds(x, 8, stride=8), :]
        c = jnp.zeros((8, L), jnp.float32)
        for r in range(8):
            c = c + jnp.where(kind == r, rates[r], 0.0)
        columns.append(c)
    columns.append(jnp.zeros((64, L), jnp.float32))
    c_turned = jnp.concatenate(columns, axis=0).T
    rate_rows[...] = jnp.concatenate([margin, c_turned, margin], axis=0)
    group = lane_index(1) // 32
    row = jnp.zeros((1, L), jnp.float32)
    for g in range(4):
        total = jnp.sum(c_turned[32 * g : 32 * g + 32], axis=0, keepdims=True)
        row = jnp.where(group == g, jnp.sum(total, axis=1, keepdims=True), row)
    sums[...] = jnp.broadcast_to(row, (8, L))


def own_strip():
    tm = lax.axis_index("tm")
    return jnp.where(tm & 1 == 0, tm >> 1, TM - 1 - (tm >> 1))


def transform_kernel(received, rate_rows, table, window, rate, swap):
    rows = []
    for pair in range(ROWS // 2):
        both = [received[pl.ds(2 * pair + j, 64, stride=ROWS), :] for j in range(2)]
        turned = jnp.concatenate(both, axis=0).T
        rows += list(halves(turned[:64], turned[64:]))
    spectrum = dot(jnp.concatenate(rows[: 8 + WY], axis=0), table[...], ((1,), (0,)))
    strip = own_strip()
    even = strip & 1 == 0
    zero = jnp.zeros((8, L), jnp.float32)
    for i in range(8 * WY):
        window[i] = zero
        window[8 * (WY + 8) + i] = zero
    offset = jnp.where(even, 8 * WY, 0)
    for i in range(8 * (8 + WY)):
        window[offset + i] = spectrum[8 * i : 8 * i + 8]
    near = rate_rows[pl.ds(pl.multiple_of(strip * 8, 8), 24), :]
    mine = jnp.concatenate([near[8 - WY : 16 + WY], jnp.zeros((2, L), jnp.float32)], axis=0)
    rate[...] = mine
    for i in range(8 * WY):
        swap[i] = jnp.where(even, window[8 * WY + i], window[64 + i])
    swap[PART - 1] = jnp.where(even, pltpu.roll(mine[0:8], 8 - WY, 0), mine[8:16])


def x_range(distance):
    return range(distance - 1, SPAN_Y + 1 - distance)


EDGE = [(d, y) for d in range(1, WX + 1) for y in x_range(d)]


def completed(window, rate, swapped):
    strip = own_strip()
    even = jnp.where(strip & 1 == 0, 1.0, 0.0)
    odd = 1.0 - even

    def tile(y, x):
        if y < WY:
            return window[8 * y + x] + even * swapped[8 * y + x]
        if y < WY + 8:
            return window[8 * y + x]
        return window[8 * y + x] + odd * swapped[8 * (y - WY - 8) + x]

    first = jnp.where(strip == 0, 1.0, 0.0)
    last = jnp.where(strip == TM - 1, 1.0, 0.0)
    row = lax.broadcasted_iota(jnp.int32, (8, L), 0)
    other = jnp.where(row < WY, swapped[PART - 1], 0.0)
    low = rate[0:8, :] + first * other
    high = rate[8:16, :] + last * pltpu.roll(other, WY, 0)
    return tile, (low, high)


def edge_kernel(window, rate, swapped, to_left, to_right):
    tile, rates = completed(window, rate, swapped)
    for i, (d, y) in enumerate(EDGE):
        to_left[i] = tile(y, d - 1)
        to_right[i] = tile(y, 8 - d)
    for j, c in enumerate(rates):
        to_left[len(EDGE) + j] = c
        to_right[len(EDGE) + j] = c


def solve_kernel(
    window, rate, swapped, left, right, sums, lanes, table, out, source, a, b, x0, x1
):
    sx, sy, strip = lax.axis_index("sx"), lax.axis_index("sy"), own_strip()
    valid = [
        jnp.where(inside, 1.0, 0.0)
        for inside in (
            sx > 0,
            sx < SX - 1,
            (sy > 0) | (strip > 0),
            (sy < SY - 1) | (strip < TM - 1),
        )
    ]
    tile, rates = completed(window, rate, swapped)
    zero = jnp.zeros((8, L), jnp.float32)
    for y in range(SPAN_Y):
        for x in range(WX):
            source[y, x] = zero
            source[y, SPAN_X - 1 - x] = zero
        for x in range(8):
            source[y, WX + x] = tile(y, x)
    for i, (d, y) in enumerate(EDGE):
        source[y, WX - d] = left[i]
        source[y, WX + 7 + d] = right[i]
    lane = lane_index(8)
    rows = []
    for j, mid in enumerate(rates):
        rows.append(
            jnp.where(
                lane < 32,
                pltpu.roll(left[len(EDGE) + j], 96, 1),
                jnp.where(
                    lane < 96, pltpu.roll(mid, 32, 1), pltpu.roll(right[len(EDGE) + j], 96, 1)
                ),
            )
        )
    rows.append(jnp.zeros((112, L), jnp.float32))
    turned = jnp.concatenate(rows, axis=0).T
    base = jnp.broadcast_to(lanes[0:1, :] + 6.0, (8, L))
    sine = jnp.broadcast_to(lanes[1:2, :], (8, L))
    sine_square = sine * sine
    for y in range(SPAN_Y):
        for x in range(SPAN_X):
            d = jnp.broadcast_to(turned[8 * x : 8 * x + 8, y : y + 1], (8, L)) + base
            inverse = 1.0 / (d * d + sine_square)
            if x < WX:
                inverse = inverse * valid[0]
            elif x >= WX + 8:
                inverse = inverse * valid[1]
            if y < WY:
                inverse = inverse * valid[2]
            elif y >= WY + 8:
                inverse = inverse * valid[3]
            ax = d * inverse
            bx = sine * inverse
            a[y, x] = ax
            b[y, x] = bx
            s = source[y, x]
            x0[y, x] = ax * s + bx * pltpu.roll(s, 64, 1)

    def sweep(old, new, margin):
        def row(y, carry):
            for x in range(margin, SPAN_X - margin):
                v = old[y, x]
                u = source[y, x] + (old[y, x + 1] + old[y, x - 1])
                u = u + (old[y + 1, x] + old[y - 1, x])
                u = u + (pltpu.roll(v, 1, 0) + pltpu.roll(v, 7, 0))
                new[y, x] = a[y, x] * u + b[y, x] * pltpu.roll(u, 64, 1)
            return carry

        lax.fori_loop(margin, SPAN_Y - margin, row, 0)

    sweep(x0, x1, 1)
    sweep(x1, x0, 2)
    sweep(x0, x1, 3)
    lo, hi = WX, WX + 8

    def change(y, x):
        return x1[y, x] - x0[y, x]

    acc = zero
    faces = []
    for y in range(WY, WY + 8):
        line = zero
        for x in range(lo, hi):
            line = line + change(y, x)
        end = y in (WY, WY + 7)
        acc = acc + (5.0 if end else 6.0) * line
        acc = acc + (change(y, lo - 1) - change(y, lo)) + (change(y, hi) - change(y, hi - 1))
        if end:
            faces.append(line)
    solved = x1[WY : WY + 8, lo:hi].reshape(512, L)
    result = dot(table[...], solved, ((1,), (1,)))
    for pair in range(4):
        cut = result[:, 128 * pair : 128 * pair + 128]
        for j, value in enumerate(halves(cut[: TM * TILES], cut[TM * TILES :])):
            out[pl.ds(2 * pair + j, TM * TILES, stride=8), :] = value
    homes = (
        strip >> 2,
        jnp.where(strip == 0, 4, (strip - 1) >> 2),
        jnp.where(strip == TM - 1, 5, (strip + 1) >> 2),
    )
    index = lax.broadcasted_iota(jnp.int32, (8, L), 0)
    share = jnp.where((index == 6) & (strip == 0), sums[...], 0.0)
    for home, v in zip(homes, (acc, *faces)):
        v = jnp.broadcast_to(jnp.sum(v, axis=0, keepdims=True), (8, L))
        share = share + jnp.where(index == home, v, 0.0)
    for d in range(TM):
        out[8 * (TILES * d + 4) : 8 * (TILES * d + 5), :] = share


def gather_kernel(received, out):
    block = received[0, 4]
    for d in range(1, TM):
        block = block + received[d, 4]
    for j in range(SX * SY):
        out[j] = block


def inverse_of(rows):
    rows = list(rows)
    index = lax.broadcasted_iota(jnp.int32, (8, L), 0)
    for p in range(8):
        here = index == p
        pivot = jnp.broadcast_to(rows[p][p : p + 1], (8, L))
        scale = 1.0 / pivot
        lead = jnp.where(here, scale, rows[p] * scale)
        for r in range(8):
            if r != p:
                factor = jnp.broadcast_to(rows[r][p : p + 1], (8, L))
                rows[r] = jnp.where(here, 0.0, rows[r]) - factor * lead
        rows[p] = lead
    return rows


def apply(rows, v):
    terms = [rows[c] * jnp.broadcast_to(v[c : c + 1], (8, L)) for c in range(8)]
    while len(terms) > 1:
        terms = [terms[i] + terms[i + 1] for i in range(0, len(terms), 2)]
    return terms[0]


def coarse_kernel(gathered, received, lanes, table, out, answer):
    index = lax.broadcasted_iota(jnp.int32, (8, L), 0)
    shift = jnp.broadcast_to(lanes[0:1, :] * float(VOLUME) + float(FACES), (8, L))

    def rows_of(sy, row):
        return gathered[pl.ds(sy * 8 + row, 8, stride=32), :]

    def right(m):
        sy, g = m // 4, m % 4
        rhs = rows_of(sy, g)
        if g == 0 and sy > 0:
            rhs = rhs + rows_of(sy - 1, 5)
        if g == 3 and sy < SY - 1:
            rhs = rhs + rows_of(sy + 1, 4)
        return rhs

    sums = [rows_of(sy, 6) for sy in range(SY)]

    def block(m, before):
        g = 32 * (m % 4)
        diagonal = jnp.broadcast_to(sums[m // 4][:, g : g + 1], (8, L)) + shift
        rows = []
        for r in range(8):
            row = jnp.where(index == r, diagonal, 0.0)
            row = jnp.where((index == r - 1) | (index == r + 1), -COUPLE_X, row)
            for other in before:
                row = row - (COUPLE_Y * COUPLE_Y) * other[r]
            rows.append(row)
        return rows

    inv, part = {}, {}

    def eliminate(m, sources):
        matrix = inverse_of(block(m, [inv[q] for q in sources]))
        rhs = right(m)
        for q in sources:
            rhs = rhs + COUPLE_Y * part[q]
        inv[m] = matrix
        part[m] = apply(matrix, rhs)

    for i in range(8):
        if i < 7:
            eliminate(i, [i - 1] if i else [])
        eliminate(15 - i, [16 - i] if i else [])
    eliminate(7, [6, 8])
    solved = {7: part[7]}
    for i in range(1, 9):
        for m, q in ((7 - i, 8 - i), (7 + i, 6 + i)):
            if 0 <= m < 16:
                solved[m] = part[m] + COUPLE_Y * apply(inv[m], solved[q])
    for m in range(16):
        answer[8 * m : 8 * m + 8, :] = solved[m]
    sx, sy = lax.axis_index("sx"), lax.axis_index("sy")
    own = table[pl.ds(pl.multiple_of(lax.axis_index("tm") * 8, 8), 8), :]
    group = lane_index(8) // 32
    added = jnp.zeros((8, L), jnp.float32)
    for g in range(4):
        y = answer[pl.ds((sy * 4 + g) * 8 + sx, 1), :]
        value = jnp.sum(own * y, axis=1, keepdims=True)
        added = jnp.where(group == g, value, added)
    for tp in range(4):
        rows = [received[MEMBER[s], tp] for s in range(TM)]
        turned = jnp.concatenate(rows, axis=0).T
        for t2 in range(2):
            t = 2 * tp + t2
            plus = jnp.broadcast_to(added[t : t + 1, :], (8, L))
            for x in range(8):
                r = t2 * 64 + x * 8
                out[pl.ds(t * 64 + x, 8, stride=8), :] = turned[r : r + 8] + plus


def call(kernel, name, out_shape, arrays, scratch=(), rates=None, keep=True):
    if keep:
        out_shape = jax.tree.map(lambda o: pltpu.VMEM(o.shape, o.dtype), out_shape)
    if rates is None:
        arrays = [pltpu.with_memory_space_constraint(x, pltpu.VMEM) for x in arrays]
    scalars = [] if rates is None else [rates]
    many = isinstance(out_shape, tuple)
    return pl.pallas_call(
        kernel,
        name=name,
        out_shape=out_shape,
        in_specs=smem(len(scalars)) + vmem(len(arrays)),
        out_specs=tuple(vmem(len(out_shape))) if many else vmem(1)[0],
        scratch_shapes=list(scratch),
    )(*scalars, *arrays)


def swaps():
    def rank(g):
        return MEMBER[g % TM] * SY + g // TM

    pairs = [(rank(g), rank(g + 1)) for g in range(1, SY * TM - 1, 2)]
    return pairs + [(q, p) for p, q in pairs]


def local(driving_input, regime, reaction_rates):
    forward, inverse, natural, lanes = (jnp.asarray(t) for t in (FORWARD, INVERSE, NATURAL, LANES))
    packed, rate_rows, sums = call(
        pack_kernel,
        "pack",
        (shape(TM, 4 * ROWS, L), shape(L + 16, L), shape(8, L)),
        [driving_input.reshape(512, L), regime.reshape(64, L)],
        rates=reaction_rates,
    )
    received = lax.all_to_all(packed, "tm", split_axis=0, concat_axis=0, tiled=True)
    window, rate, swap = call(
        transform_kernel,
        "transform",
        (shape(8 * SPAN_Y, 8, L), shape(16, L), shape(PART, 8, L)),
        [received.reshape(TM * 4 * ROWS, L), rate_rows, forward],
    )
    swapped = lax.ppermute(swap, ("tm", "sy"), swaps())
    tiles = len(EDGE) + 2
    to_left, to_right = call(
        edge_kernel, "edges", (shape(tiles, 8, L),) * 2, [window, rate, swapped]
    )
    across = [(i, i + 1) for i in range(SX - 1)]
    left = lax.ppermute(to_right, "sx", across)
    right = lax.ppermute(to_left, "sx", [(q, p) for p, q in across])
    message = call(
        solve_kernel,
        "sweeps",
        shape(TM * TILES * 8, L),
        [window, rate, swapped, left, right, sums, lanes, inverse],
        [pltpu.VMEM((SPAN_Y, SPAN_X, 8, L), jnp.float32)] * 5,
    )
    returned = lax.all_to_all(
        message.reshape(TM, TILES, 8, L), "tm", split_axis=0, concat_axis=0, tiled=True
    )
    shared = call(gather_kernel, "gather", shape(SX * SY, 8, L), [returned])
    gathered = lax.all_to_all(shared, ("sx", "sy"), split_axis=0, concat_axis=0, tiled=True)
    result = call(
        coarse_kernel,
        "coarse",
        shape(512, L),
        [gathered.reshape(256, L), returned, lanes, natural],
        [pltpu.VMEM((L, L), jnp.float32)],
        keep=False,
    )
    return result.reshape(driving_input.shape)


def solution(mesh):
    placed = (P("tm", None, "sx", "sy"), P(None, "sx", "sy"), P())
    return jax.shard_map(
        local, mesh=mesh, in_specs=placed, out_specs=P("tm", None, "sx", "sy"), check_vma=False
    )
```

```python
import jax
import jax.numpy as jnp
import numpy as np
from jax import lax
from jax.experimental import pallas as pl
from jax.experimental.pallas import tpu as pltpu
from jax.sharding import PartitionSpec as P

L = 128
NZ = 8
BLOCK = 8
WY = 3
WX = 4
SPAN_Y = BLOCK + 2 * WY
SPAN_X = BLOCK + 2 * WX
ROWS = 12
PART = 8 * WY + 1
TM, SX, SY = 16, 8, 4
FACES = 2 * (32 * NZ + 8 * NZ)
VOLUME = 8 * 32 * NZ
COUPLE_X = 32.0 * NZ
COUPLE_Y = 8.0 * NZ
TILES = 5


def strip_of(d):
    return d // 2 if d % 2 == 0 else TM - 1 - d // 2


MEMBER = {strip_of(d): d for d in range(TM)}


def two_parts(table):
    value = np.asarray(table, jnp.bfloat16)
    rest = np.asarray(table - np.asarray(value, np.float64), jnp.bfloat16)
    return np.stack([value, rest])


def tables():
    n = np.arange(L)
    k = np.arange(64)
    ang = 2.0 * np.pi * ((n[:, None] * k[None, :]) % L) / L
    half = np.where(n % 2 == 0, 1.0, -1.0)
    forward = np.concatenate([np.cos(ang), -np.sin(ang)], axis=1)
    forward[:, 64] = half
    weight = np.full((1, 64), 2.0)
    weight[0, 0] = 1.0
    inverse = np.concatenate([weight * np.cos(ang), -weight * np.sin(ang)], axis=1) / L
    inverse[:, 64] = half / L
    theta = 2.0 * np.pi * k / L
    shift = np.concatenate([1.0 - np.cos(theta)] * 2)
    shift[64] = 2.0
    sine = np.concatenate([np.sin(theta), -np.sin(theta)])
    sine[0] = sine[64] = 0.0
    order = np.array([8 * d + 2 * tp + t2 for t2 in range(2) for d in range(TM) for tp in range(4)])
    lanes = np.zeros((8, L))
    lanes[0] = shift
    lanes[1] = sine
    padded = np.zeros((2, TM, TILES, L))
    padded[:, :, :4] = inverse[order].reshape(2, TM, 4, L)
    as32 = lambda a: np.asarray(a, np.float32)
    return two_parts(forward[order]), two_parts(padded.reshape(-1, L)), as32(inverse), as32(lanes)


FORWARD, INVERSE, NATURAL, LANES = tables()


def vmem(count):
    return [pl.BlockSpec(memory_space=pltpu.VMEM)] * count


def smem(count):
    return [pl.BlockSpec(memory_space=pltpu.SMEM)] * count


def shape(*dims):
    return jax.ShapeDtypeStruct(dims, jnp.float32)


def dot(a, table, dims, table_first=False):
    value = a.astype(jnp.bfloat16)
    rest = (a - value.astype(jnp.float32)).astype(jnp.bfloat16)
    total = None
    for x, t in ((rest, table[0]), (value, table[1]), (value, table[0])):
        pair = (t, x) if table_first else (x, t)
        term = lax.dot_general(*pair, (dims, ((), ())), preferred_element_type=jnp.float32)
        total = term if total is None else total + term
    return total


def lane_index(rows):
    return lax.broadcasted_iota(jnp.int32, (rows, L), 1)


def halves(low, high):
    first = lane_index(low.shape[0]) < 64
    return (
        jnp.where(first, low, pltpu.roll(high, 64, 1)),
        jnp.where(first, pltpu.roll(low, 64, 1), high),
    )


def pack_kernel(rates, field, regime, out, rate_rows, sums):
    margin = jnp.zeros((8, L), jnp.float32)
    for tp in range(4):
        rows = [
            field[pl.ds((2 * tp + t2) * 64 + x, 8, stride=8), :] for t2 in range(2) for x in range(8)
        ]
        turned = jnp.concatenate(rows, axis=0).T
        starts = (
            jnp.concatenate([turned, margin], axis=0),
            jnp.concatenate([margin[:WY], turned, margin[WY:]], axis=0),
        )
        for d in range(TM):
            s = strip_of(d)
            out[d, ROWS * tp : ROWS * (tp + 1)] = starts[s % 2][8 * s : 8 * s + ROWS]
    columns = []
    for x in range(8):
        kind = regime[pl.ds(x, 8, stride=8), :]
        c = jnp.zeros((8, L), jnp.float32)
        for r in range(8):
            c = c + jnp.where(kind == r, rates[r], 0.0)
        columns.append(c)
    columns.append(jnp.zeros((64, L), jnp.float32))
    c_turned = jnp.concatenate(columns, axis=0).T
    rate_rows[...] = jnp.concatenate([margin, c_turned, margin], axis=0)
    group = lane_index(1) // 32
    row = jnp.zeros((1, L), jnp.float32)
    for g in range(4):
        total = jnp.sum(c_turned[32 * g : 32 * g + 32], axis=0, keepdims=True)
        row = jnp.where(group == g, jnp.sum(total, axis=1, keepdims=True), row)
    sums[...] = jnp.broadcast_to(row, (8, L))


def own_strip():
    tm = lax.axis_index("tm")
    return jnp.where(tm & 1 == 0, tm >> 1, TM - 1 - (tm >> 1))


def transform_kernel(received, rate_rows, table, window, rate, swap):
    rows = []
    for pair in range(ROWS // 2):
        both = [received[pl.ds(2 * pair + j, 64, stride=ROWS), :] for j in range(2)]
        turned = jnp.concatenate(both, axis=0).T
        rows += list(halves(turned[:64], turned[64:]))
    spectrum = dot(jnp.concatenate(rows[: 8 + WY], axis=0), table, ((1,), (0,)))
    strip = own_strip()
    even = strip & 1 == 0
    zero = jnp.zeros((8, L), jnp.float32)
    for i in range(8 * WY):
        window[i] = zero
        window[8 * (WY + 8) + i] = zero
    offset = jnp.where(even, 8 * WY, 0)
    for i in range(8 * (8 + WY)):
        window[offset + i] = spectrum[8 * i : 8 * i + 8]
    near = rate_rows[pl.ds(pl.multiple_of(strip * 8, 8), 24), :]
    mine = jnp.concatenate([near[8 - WY : 16 + WY], jnp.zeros((2, L), jnp.float32)], axis=0)
    rate[...] = mine
    for i in range(8 * WY):
        swap[i] = jnp.where(even, window[8 * WY + i], window[64 + i])
    swap[PART - 1] = jnp.where(even, pltpu.roll(mine[0:8], 8 - WY, 0), mine[8:16])


def x_range(distance):
    return range(distance - 1, SPAN_Y + 1 - distance)


EDGE = [(d, y) for d in range(1, WX + 1) for y in x_range(d)]


def completed(window, rate, swapped):
    strip = own_strip()
    even = jnp.where(strip & 1 == 0, 1.0, 0.0)
    odd = 1.0 - even

    def tile(y, x):
        if y < WY:
            return window[8 * y + x] + even * swapped[8 * y + x]
        if y < WY + 8:
            return window[8 * y + x]
        return window[8 * y + x] + odd * swapped[8 * (y - WY - 8) + x]

    first = jnp.where(strip == 0, 1.0, 0.0)
    last = jnp.where(strip == TM - 1, 1.0, 0.0)
    row = lax.broadcasted_iota(jnp.int32, (8, L), 0)
    other = jnp.where(row < WY, swapped[PART - 1], 0.0)
    low = rate[0:8, :] + first * other
    high = rate[8:16, :] + last * pltpu.roll(other, WY, 0)
    return tile, (low, high)


def edge_kernel(window, rate, swapped, to_odd, to_even):
    tile, rates = completed(window, rate, swapped)
    even = lax.axis_index("sx") & 1 == 0
    for i, (d, y) in enumerate(EDGE):
        left, right = tile(y, d - 1), tile(y, 8 - d)
        to_odd[i] = jnp.where(even, right, left)
        to_even[i] = jnp.where(even, left, right)
    for j, c in enumerate(rates):
        to_odd[len(EDGE) + j] = c
        to_even[len(EDGE) + j] = c


def inside():
    sx, sy, strip = lax.axis_index("sx"), lax.axis_index("sy"), own_strip()
    return [
        jnp.where(ok, 1.0, 0.0)
        for ok in (
            sx > 0,
            sx < SX - 1,
            (sy > 0) | (strip > 0),
            (sy < SY - 1) | (strip < TM - 1),
        )
    ]


def cell_terms(c, lanes):
    d = c + lanes[0:1, :] + 6.0
    sine = lanes[1:2, :]
    inverse = 1.0 / (d * d + sine * sine)
    return d * inverse, sine * inverse


def prepare_kernel(window, rate, swapped, lanes, source, a, b, first):
    tile, rates = completed(window, rate, swapped)
    valid = inside()
    rows = jnp.concatenate([*rates, jnp.zeros((112, L), jnp.float32)], axis=0)
    turned = rows.T
    for y in range(SPAN_Y):
        for x in range(8):
            c = jnp.broadcast_to(turned[8 * x : 8 * x + 8, y : y + 1], (8, L))
            ax, bx = cell_terms(c, lanes)
            if not WY <= y < WY + 8:
                ok = valid[2] if y < WY else valid[3]
                ax, bx = ax * ok, bx * ok
            s = tile(y, x)
            source[y, x] = s
            a[y, x] = ax
            b[y, x] = bx
            first[y, x] = ax * s + bx * pltpu.roll(s, 64, 1)


def solve_kernel(
    own_s, own_a, own_b, own_x, from_odd, from_even, sums, lanes, table, out, hs, ha, hb, hx, x0, x1
):
    strip = own_strip()
    valid = inside()
    even = lax.axis_index("sx") & 1 == 0
    zero = jnp.zeros((8, L), jnp.float32)

    def left(i):
        return jnp.where(even, from_even[i], from_odd[i])

    def right(i):
        return jnp.where(even, from_odd[i], from_even[i])

    for y in range(SPAN_Y):
        for h in range(8):
            hs[y, h] = zero
    for i, (d, y) in enumerate(EDGE):
        hs[y, WX - d] = left(i)
        hs[y, WX - 1 + d] = right(i)
    lane = lane_index(8)
    rows = []
    for j in range(2):
        n = len(EDGE) + j
        rows.append(jnp.where(lane < 32, pltpu.roll(left(n), 96, 1), pltpu.roll(right(n), 32, 1)))
    rows.append(jnp.zeros((112, L), jnp.float32))
    turned = jnp.concatenate(rows, axis=0).T
    for y in range(SPAN_Y):
        for h in range(8):
            distance = WX - h if h < WX else h - WX + 1
            if y not in x_range(distance):
                ha[y, h] = zero
                hb[y, h] = zero
                hx[y, h] = zero
                continue
            c = jnp.broadcast_to(turned[8 * h : 8 * h + 8, y : y + 1], (8, L))
            ax, bx = cell_terms(c, lanes)
            ok = valid[0] if h < WX else valid[1]
            if y < WY:
                ok = ok * valid[2]
            elif y >= WY + 8:
                ok = ok * valid[3]
            ax, bx = ax * ok, bx * ok
            s = hs[y, h]
            ha[y, h] = ax
            hb[y, h] = bx
            hx[y, h] = ax * s + bx * pltpu.roll(s, 64, 1)

    def split(own, halo):
        def get(y, x):
            if x < WX:
                return halo[y, x]
            if x < WX + 8:
                return own[y, x - WX]
            return halo[y, x - 8]

        return get

    source, a, b = split(own_s, hs), split(own_a, ha), split(own_b, hb)

    def whole(ref):
        return lambda y, x: ref[y, x]

    def sweep(old, new, margin):
        def row(y, carry):
            for x in range(margin, SPAN_X - margin):
                v = old(y, x)
                u = source(y, x) + (old(y, x + 1) + old(y, x - 1))
                u = u + (old(y + 1, x) + old(y - 1, x))
                u = u + (pltpu.roll(v, 1, 0) + pltpu.roll(v, 7, 0))
                new[y, x] = a(y, x) * u + b(y, x) * pltpu.roll(u, 64, 1)
            return carry

        lax.fori_loop(margin, SPAN_Y - margin, row, 0)

    sweep(split(own_x, hx), x1, 1)
    sweep(whole(x1), x0, 2)
    sweep(whole(x0), x1, 3)
    lo, hi = WX, WX + 8

    def change(y, x):
        return x1[y, x] - x0[y, x]

    acc = zero
    faces = []
    for y in range(WY, WY + 8):
        line = zero
        for x in range(lo, hi):
            line = line + change(y, x)
        end = y in (WY, WY + 7)
        acc = acc + (5.0 if end else 6.0) * line
        acc = acc + (change(y, lo - 1) - change(y, lo)) + (change(y, hi) - change(y, hi - 1))
        if end:
            faces.append(line)
    solved = x1[WY : WY + 8, lo:hi].reshape(512, L)
    result = dot(solved, table, ((1,), (1,)), table_first=True)
    for pair in range(4):
        cut = result[:, 128 * pair : 128 * pair + 128]
        for j, value in enumerate(halves(cut[: TM * TILES], cut[TM * TILES :])):
            out[pl.ds(2 * pair + j, TM * TILES, stride=8), :] = value
    homes = (
        strip >> 2,
        jnp.where(strip == 0, 4, (strip - 1) >> 2),
        jnp.where(strip == TM - 1, 5, (strip + 1) >> 2),
    )
    index = lax.broadcasted_iota(jnp.int32, (8, L), 0)
    share = jnp.where((index == 6) & (strip == 0), sums[...], 0.0)
    for home, v in zip(homes, (acc, *faces)):
        v = jnp.broadcast_to(jnp.sum(v, axis=0, keepdims=True), (8, L))
        share = share + jnp.where(index == home, v, 0.0)
    for d in range(TM):
        out[8 * (TILES * d + 4) : 8 * (TILES * d + 5), :] = share


def gather_kernel(received, out):
    block = received[0, 4]
    for d in range(1, TM):
        block = block + received[d, 4]
    for j in range(SX * SY):
        out[j] = block


def inverse_of(rows):
    rows = list(rows)
    index = lax.broadcasted_iota(jnp.int32, (8, L), 0)
    for p in range(8):
        here = index == p
        pivot = jnp.broadcast_to(rows[p][p : p + 1], (8, L))
        scale = 1.0 / pivot
        lead = jnp.where(here, scale, rows[p] * scale)
        for r in range(8):
            if r != p:
                factor = jnp.broadcast_to(rows[r][p : p + 1], (8, L))
                rows[r] = jnp.where(here, 0.0, rows[r]) - factor * lead
        rows[p] = lead
    return rows


def apply(rows, v):
    terms = [rows[c] * jnp.broadcast_to(v[c : c + 1], (8, L)) for c in range(8)]
    while len(terms) > 1:
        terms = [terms[i] + terms[i + 1] for i in range(0, len(terms), 2)]
    return terms[0]


def coarse_kernel(gathered, received, lanes, table, out, answer):
    index = lax.broadcasted_iota(jnp.int32, (8, L), 0)
    shift = jnp.broadcast_to(lanes[0:1, :] * float(VOLUME) + float(FACES), (8, L))

    def rows_of(sy, row):
        return gathered[pl.ds(sy * 8 + row, 8, stride=32), :]

    def right(m):
        sy, g = m // 4, m % 4
        rhs = rows_of(sy, g)
        if g == 0 and sy > 0:
            rhs = rhs + rows_of(sy - 1, 5)
        if g == 3 and sy < SY - 1:
            rhs = rhs + rows_of(sy + 1, 4)
        return rhs

    sums = [rows_of(sy, 6) for sy in range(SY)]

    def block(m, before):
        g = 32 * (m % 4)
        diagonal = jnp.broadcast_to(sums[m // 4][:, g : g + 1], (8, L)) + shift
        rows = []
        for r in range(8):
            row = jnp.where(index == r, diagonal, 0.0)
            row = jnp.where((index == r - 1) | (index == r + 1), -COUPLE_X, row)
            for other in before:
                row = row - (COUPLE_Y * COUPLE_Y) * other[r]
            rows.append(row)
        return rows

    inv, part = {}, {}

    def eliminate(m, sources):
        matrix = inverse_of(block(m, [inv[q] for q in sources]))
        rhs = right(m)
        for q in sources:
            rhs = rhs + COUPLE_Y * part[q]
        inv[m] = matrix
        part[m] = apply(matrix, rhs)

    for i in range(8):
        if i < 7:
            eliminate(i, [i - 1] if i else [])
        eliminate(15 - i, [16 - i] if i else [])
    eliminate(7, [6, 8])
    solved = {7: part[7]}
    for i in range(1, 9):
        for m, q in ((7 - i, 8 - i), (7 + i, 6 + i)):
            if 0 <= m < 16:
                solved[m] = part[m] + COUPLE_Y * apply(inv[m], solved[q])
    for m in range(16):
        answer[8 * m : 8 * m + 8, :] = solved[m]
    sx, sy = lax.axis_index("sx"), lax.axis_index("sy")
    own = table[pl.ds(pl.multiple_of(lax.axis_index("tm") * 8, 8), 8), :]
    group = lane_index(8) // 32
    added = jnp.zeros((8, L), jnp.float32)
    for g in range(4):
        y = answer[pl.ds((sy * 4 + g) * 8 + sx, 1), :]
        value = jnp.sum(own * y, axis=1, keepdims=True)
        added = jnp.where(group == g, value, added)
    for tp in range(4):
        rows = [received[MEMBER[s], tp] for s in range(TM)]
        turned = jnp.concatenate(rows, axis=0).T
        for t2 in range(2):
            t = 2 * tp + t2
            plus = jnp.broadcast_to(added[t : t + 1, :], (8, L))
            for x in range(8):
                r = t2 * 64 + x * 8
                out[pl.ds(t * 64 + x, 8, stride=8), :] = turned[r : r + 8] + plus


def call(kernel, name, out_shape, arrays, scratch=(), rates=None, keep=True, flops=0):
    if keep:
        out_shape = jax.tree.map(lambda o: pltpu.VMEM(o.shape, o.dtype), out_shape)
    if rates is None:
        arrays = [pltpu.with_memory_space_constraint(x, pltpu.VMEM) for x in arrays]
    scalars = [] if rates is None else [rates]
    many = isinstance(out_shape, tuple)
    return pl.pallas_call(
        kernel,
        name=name,
        out_shape=out_shape,
        in_specs=smem(len(scalars)) + vmem(len(arrays)),
        out_specs=tuple(vmem(len(out_shape))) if many else vmem(1)[0],
        scratch_shapes=list(scratch),
        compiler_params=pltpu.CompilerParams(vmem_limit_bytes=24 * 2**20),
        cost_estimate=pl.CostEstimate(flops=flops, transcendentals=0, bytes_accessed=0),
    )(*scalars, *arrays)


def swaps():
    def rank(g):
        return MEMBER[g % TM] * SY + g // TM

    pairs = [(rank(g), rank(g + 1)) for g in range(1, SY * TM - 1, 2)]
    return pairs + [(q, p) for p, q in pairs]


def local(driving_input, regime, reaction_rates):
    forward, inverse, natural, lanes = (jnp.asarray(t) for t in (FORWARD, INVERSE, NATURAL, LANES))
    packed, rate_rows, sums = call(
        pack_kernel,
        "pack",
        (shape(TM, 4 * ROWS, L), shape(L + 16, L), shape(8, L)),
        [driving_input.reshape(512, L), regime.reshape(64, L)],
        rates=reaction_rates,
    )
    received = lax.all_to_all(packed, "tm", split_axis=0, concat_axis=0, tiled=True)
    window, rate, swap = call(
        transform_kernel,
        "transform",
        (shape(8 * SPAN_Y, 8, L), shape(16, L), shape(PART, 8, L)),
        [received.reshape(TM * 4 * ROWS, L), rate_rows, forward],
    )
    swapped = lax.ppermute(swap, ("tm", "sy"), swaps())
    tiles = len(EDGE) + 2
    to_odd, to_even = call(
        edge_kernel, "edges", (shape(tiles, 8, L),) * 2, [window, rate, swapped]
    )

    def x_swaps(first):
        pairs = [(i, i + 1) for i in range(first, SX - 1, 2)]
        return pairs + [(q, p) for p, q in pairs]

    from_odd = lax.ppermute(to_odd, "sx", x_swaps(0))
    from_even = lax.ppermute(to_even, "sx", x_swaps(1))
    prepared = call(
        prepare_kernel,
        "prepare",
        (shape(SPAN_Y, 8, 8, L),) * 4,
        [window, rate, swapped, lanes],
        flops=10**7,
    )
    half = pltpu.VMEM((SPAN_Y, 8, 8, L), jnp.float32)
    message = call(
        solve_kernel,
        "sweeps",
        shape(TM * TILES * 8, L),
        [*prepared, from_odd, from_even, sums, lanes, inverse],
        [half] * 4 + [pltpu.VMEM((SPAN_Y, SPAN_X, 8, L), jnp.float32)] * 2,
    )
    returned = lax.all_to_all(
        message.reshape(TM, TILES, 8, L), "tm", split_axis=0, concat_axis=0, tiled=True
    )
    shared = call(gather_kernel, "gather", shape(SX * SY, 8, L), [returned])
    gathered = lax.all_to_all(shared, ("sx", "sy"), split_axis=0, concat_axis=0, tiled=True)
    result = call(
        coarse_kernel,
        "coarse",
        shape(512, L),
        [gathered.reshape(256, L), returned, lanes, natural],
        [pltpu.VMEM((L, L), jnp.float32)],
        keep=False,
    )
    return result.reshape(driving_input.shape)


def solution(mesh):
    placed = (P("tm", None, "sx", "sy"), P(None, "sx", "sy"), P())
    return jax.shard_map(
        local, mesh=mesh, in_specs=placed, out_specs=P("tm", None, "sx", "sy"), check_vma=False
    )
```

```python
import jax
import jax.numpy as jnp
import numpy as np
from jax import lax
from jax.experimental import pallas as pl
from jax.experimental.pallas import tpu as pltpu
from jax.sharding import PartitionSpec as P

L = 128
NZ = 8
BLOCK = 8
WY = 3
WX = 4
SPAN_Y = BLOCK + 2 * WY
SPAN_X = BLOCK + 2 * WX
ROWS = 12
PART = 8 * WY + 1
TM, SX, SY = 16, 8, 4
FACES = 2 * (32 * NZ + 8 * NZ)
VOLUME = 8 * 32 * NZ
COUPLE_X = 32.0 * NZ
COUPLE_Y = 8.0 * NZ
TILES = 5


def strip_of(d):
    return d // 2 if d % 2 == 0 else TM - 1 - d // 2


MEMBER = {strip_of(d): d for d in range(TM)}


def two_parts(table):
    value = np.asarray(table, jnp.bfloat16)
    rest = np.asarray(table - np.asarray(value, np.float64), jnp.bfloat16)
    return np.stack([value, rest])


def tables():
    n = np.arange(L)
    k = np.arange(64)
    ang = 2.0 * np.pi * ((n[:, None] * k[None, :]) % L) / L
    half = np.where(n % 2 == 0, 1.0, -1.0)
    forward = np.concatenate([np.cos(ang), -np.sin(ang)], axis=1)
    forward[:, 64] = half
    weight = np.full((1, 64), 2.0)
    weight[0, 0] = 1.0
    inverse = np.concatenate([weight * np.cos(ang), -weight * np.sin(ang)], axis=1) / L
    inverse[:, 64] = half / L
    theta = 2.0 * np.pi * k / L
    shift = np.concatenate([1.0 - np.cos(theta)] * 2)
    shift[64] = 2.0
    sine = np.concatenate([np.sin(theta), -np.sin(theta)])
    sine[0] = sine[64] = 0.0
    order = np.array([8 * d + 2 * tp + t2 for t2 in range(2) for d in range(TM) for tp in range(4)])
    lanes = np.zeros((8, L))
    lanes[0] = shift
    lanes[1] = sine
    padded = np.zeros((2, TM, TILES, L))
    padded[:, :, :4] = inverse[order].reshape(2, TM, 4, L)
    as32 = lambda a: np.asarray(a, np.float32)
    return two_parts(forward[order]), two_parts(padded.reshape(-1, L)), as32(inverse), as32(lanes)


FORWARD, INVERSE, NATURAL, LANES = tables()


def vmem(count):
    return [pl.BlockSpec(memory_space=pltpu.VMEM)] * count


def smem(count):
    return [pl.BlockSpec(memory_space=pltpu.SMEM)] * count


def shape(*dims):
    return jax.ShapeDtypeStruct(dims, jnp.float32)


def dot(a, table, dims, table_first=False):
    value = a.astype(jnp.bfloat16)
    rest = (a - value.astype(jnp.float32)).astype(jnp.bfloat16)
    total = None
    for x, t in ((rest, table[0]), (value, table[1]), (value, table[0])):
        pair = (t, x) if table_first else (x, t)
        term = lax.dot_general(*pair, (dims, ((), ())), preferred_element_type=jnp.float32)
        total = term if total is None else total + term
    return total


def lane_index(rows):
    return lax.broadcasted_iota(jnp.int32, (rows, L), 1)


def halves(low, high):
    first = lane_index(low.shape[0]) < 64
    return (
        jnp.where(first, low, pltpu.roll(high, 64, 1)),
        jnp.where(first, pltpu.roll(low, 64, 1), high),
    )


def pack_kernel(rates, field, regime, out, rate_rows, sums):
    margin = jnp.zeros((8, L), jnp.float32)
    for tp in range(4):
        rows = [
            field[pl.ds((2 * tp + t2) * 64 + x, 8, stride=8), :] for t2 in range(2) for x in range(8)
        ]
        turned = jnp.concatenate(rows, axis=0).T
        starts = (
            jnp.concatenate([turned, margin], axis=0),
            jnp.concatenate([margin[:WY], turned, margin[WY:]], axis=0),
        )
        for d in range(TM):
            s = strip_of(d)
            out[d, ROWS * tp : ROWS * (tp + 1)] = starts[s % 2][8 * s : 8 * s + ROWS]
    columns = []
    for x in range(8):
        kind = regime[pl.ds(x, 8, stride=8), :]
        c = jnp.zeros((8, L), jnp.float32)
        for r in range(8):
            c = c + jnp.where(kind == r, rates[r], 0.0)
        columns.append(c)
    columns.append(jnp.zeros((64, L), jnp.float32))
    c_turned = jnp.concatenate(columns, axis=0).T
    rate_rows[...] = jnp.concatenate([margin, c_turned, margin], axis=0)
    group = lane_index(1) // 32
    row = jnp.zeros((1, L), jnp.float32)
    for g in range(4):
        total = jnp.sum(c_turned[32 * g : 32 * g + 32], axis=0, keepdims=True)
        row = jnp.where(group == g, jnp.sum(total, axis=1, keepdims=True), row)
    sums[...] = jnp.broadcast_to(row, (8, L))


def own_strip():
    tm = lax.axis_index("tm")
    return jnp.where(tm & 1 == 0, tm >> 1, TM - 1 - (tm >> 1))


def transform_kernel(received, rate_rows, table, window, rate, swap):
    rows = []
    for pair in range(ROWS // 2):
        both = [received[pl.ds(2 * pair + j, 64, stride=ROWS), :] for j in range(2)]
        turned = jnp.concatenate(both, axis=0).T
        rows += list(halves(turned[:64], turned[64:]))
    spectrum = dot(jnp.concatenate(rows[: 8 + WY], axis=0), table, ((1,), (0,)))
    strip = own_strip()
    even = strip & 1 == 0
    zero = jnp.zeros((8, L), jnp.float32)
    for i in range(8 * WY):
        window[i] = zero
        window[8 * (WY + 8) + i] = zero
    offset = jnp.where(even, 8 * WY, 0)
    for i in range(8 * (8 + WY)):
        window[offset + i] = spectrum[8 * i : 8 * i + 8]
    near = rate_rows[pl.ds(pl.multiple_of(strip * 8, 8), 24), :]
    mine = jnp.concatenate([near[8 - WY : 16 + WY], jnp.zeros((2, L), jnp.float32)], axis=0)
    rate[...] = mine
    for i in range(8 * WY):
        swap[i] = jnp.where(even, window[8 * WY + i], window[64 + i])
    swap[PART - 1] = jnp.where(even, pltpu.roll(mine[0:8], 8 - WY, 0), mine[8:16])


def x_range(distance):
    return range(distance - 1, SPAN_Y + 1 - distance)


EDGE = [(d, y) for d in range(1, WX + 1) for y in x_range(d)]


def completed(window, rate, swapped):
    strip = own_strip()
    even = jnp.where(strip & 1 == 0, 1.0, 0.0)
    odd = 1.0 - even

    def tile(y, x):
        if y < WY:
            return window[8 * y + x] + even * swapped[8 * y + x]
        if y < WY + 8:
            return window[8 * y + x]
        return window[8 * y + x] + odd * swapped[8 * (y - WY - 8) + x]

    first = jnp.where(strip == 0, 1.0, 0.0)
    last = jnp.where(strip == TM - 1, 1.0, 0.0)
    row = lax.broadcasted_iota(jnp.int32, (8, L), 0)
    other = jnp.where(row < WY, swapped[PART - 1], 0.0)
    low = rate[0:8, :] + first * other
    high = rate[8:16, :] + last * pltpu.roll(other, WY, 0)
    return tile, (low, high)


def edge_kernel(window, rate, swapped, to_left, to_right):
    tile, rates = completed(window, rate, swapped)
    for i, (d, y) in enumerate(EDGE):
        to_left[i] = tile(y, d - 1)
        to_right[i] = tile(y, 8 - d)
    for j, c in enumerate(rates):
        to_left[len(EDGE) + j] = c
        to_right[len(EDGE) + j] = c


def inside():
    sx, sy, strip = lax.axis_index("sx"), lax.axis_index("sy"), own_strip()
    return [
        jnp.where(ok, 1.0, 0.0)
        for ok in (
            sx > 0,
            sx < SX - 1,
            (sy > 0) | (strip > 0),
            (sy < SY - 1) | (strip < TM - 1),
        )
    ]


def cell_terms(c, lanes):
    d = c + lanes[0:1, :] + 6.0
    sine = lanes[1:2, :]
    inverse = 1.0 / (d * d + sine * sine)
    return d * inverse, sine * inverse


def prepare_kernel(window, rate, swapped, lanes, source, a, b, first):
    tile, rates = completed(window, rate, swapped)
    valid = inside()
    rows = jnp.concatenate([*rates, jnp.zeros((112, L), jnp.float32)], axis=0)
    turned = rows.T
    for y in range(SPAN_Y):
        for x in range(8):
            c = jnp.broadcast_to(turned[8 * x : 8 * x + 8, y : y + 1], (8, L))
            ax, bx = cell_terms(c, lanes)
            if not WY <= y < WY + 8:
                ok = valid[2] if y < WY else valid[3]
                ax, bx = ax * ok, bx * ok
            s = tile(y, x)
            source[y, x] = s
            a[y, x] = ax
            b[y, x] = bx
            first[y, x] = ax * s + bx * pltpu.roll(s, 64, 1)


def solve_kernel(
    own_s, own_a, own_b, own_x, left, right, sums, lanes, table, out, hs, ha, hb, hx, x0, x1
):
    strip = own_strip()
    valid = inside()
    zero = jnp.zeros((8, L), jnp.float32)

    for y in range(SPAN_Y):
        for h in range(8):
            hs[y, h] = zero
    for i, (d, y) in enumerate(EDGE):
        hs[y, WX - d] = left[i]
        hs[y, WX - 1 + d] = right[i]
    lane = lane_index(8)
    rows = []
    for j in range(2):
        n = len(EDGE) + j
        rows.append(jnp.where(lane < 32, pltpu.roll(left[n], 96, 1), pltpu.roll(right[n], 32, 1)))
    rows.append(jnp.zeros((112, L), jnp.float32))
    turned = jnp.concatenate(rows, axis=0).T
    for y in range(SPAN_Y):
        for h in range(8):
            distance = WX - h if h < WX else h - WX + 1
            if y not in x_range(distance):
                ha[y, h] = zero
                hb[y, h] = zero
                hx[y, h] = zero
                continue
            c = jnp.broadcast_to(turned[8 * h : 8 * h + 8, y : y + 1], (8, L))
            ax, bx = cell_terms(c, lanes)
            ok = valid[0] if h < WX else valid[1]
            if y < WY:
                ok = ok * valid[2]
            elif y >= WY + 8:
                ok = ok * valid[3]
            ax, bx = ax * ok, bx * ok
            s = hs[y, h]
            ha[y, h] = ax
            hb[y, h] = bx
            hx[y, h] = ax * s + bx * pltpu.roll(s, 64, 1)

    def split(own, halo):
        def get(y, x):
            if x < WX:
                return halo[y, x]
            if x < WX + 8:
                return own[y, x - WX]
            return halo[y, x - 8]

        return get

    source, a, b = split(own_s, hs), split(own_a, ha), split(own_b, hb)

    def whole(ref):
        return lambda y, x: ref[y, x]

    def sweep(old, new, margin):
        def row(y, carry):
            for x in range(margin, SPAN_X - margin):
                v = old(y, x)
                u = source(y, x) + (old(y, x + 1) + old(y, x - 1))
                u = u + (old(y + 1, x) + old(y - 1, x))
                u = u + (pltpu.roll(v, 1, 0) + pltpu.roll(v, 7, 0))
                new[y, x] = a(y, x) * u + b(y, x) * pltpu.roll(u, 64, 1)
            return carry

        lax.fori_loop(margin, SPAN_Y - margin, row, 0)

    sweep(split(own_x, hx), x1, 1)
    sweep(whole(x1), x0, 2)
    sweep(whole(x0), x1, 3)
    lo, hi = WX, WX + 8

    def change(y, x):
        return x1[y, x] - x0[y, x]

    acc = zero
    faces = []
    for y in range(WY, WY + 8):
        line = zero
        for x in range(lo, hi):
            line = line + change(y, x)
        end = y in (WY, WY + 7)
        acc = acc + (5.0 if end else 6.0) * line
        acc = acc + (change(y, lo - 1) - change(y, lo)) + (change(y, hi) - change(y, hi - 1))
        if end:
            faces.append(line)
    solved = x1[WY : WY + 8, lo:hi].reshape(512, L)
    result = dot(solved, table, ((1,), (1,)), table_first=True)
    for pair in range(4):
        cut = result[:, 128 * pair : 128 * pair + 128]
        for j, value in enumerate(halves(cut[: TM * TILES], cut[TM * TILES :])):
            out[pl.ds(2 * pair + j, TM * TILES, stride=8), :] = value
    homes = (
        strip >> 2,
        jnp.where(strip == 0, 4, (strip - 1) >> 2),
        jnp.where(strip == TM - 1, 5, (strip + 1) >> 2),
    )
    index = lax.broadcasted_iota(jnp.int32, (8, L), 0)
    share = jnp.where((index == 6) & (strip == 0), sums[...], 0.0)
    for home, v in zip(homes, (acc, *faces)):
        v = jnp.broadcast_to(jnp.sum(v, axis=0, keepdims=True), (8, L))
        share = share + jnp.where(index == home, v, 0.0)
    for d in range(TM):
        out[8 * (TILES * d + 4) : 8 * (TILES * d + 5), :] = share


def gather_kernel(received, out):
    block = received[0, 4]
    for d in range(1, TM):
        block = block + received[d, 4]
    for j in range(SX * SY):
        out[j] = block


def inverse_of(rows):
    rows = list(rows)
    index = lax.broadcasted_iota(jnp.int32, (8, L), 0)
    for p in range(8):
        here = index == p
        pivot = jnp.broadcast_to(rows[p][p : p + 1], (8, L))
        scale = 1.0 / pivot
        lead = jnp.where(here, scale, rows[p] * scale)
        for r in range(8):
            if r != p:
                factor = jnp.broadcast_to(rows[r][p : p + 1], (8, L))
                rows[r] = jnp.where(here, 0.0, rows[r]) - factor * lead
        rows[p] = lead
    return rows


def apply(rows, v):
    terms = [rows[c] * jnp.broadcast_to(v[c : c + 1], (8, L)) for c in range(8)]
    while len(terms) > 1:
        terms = [terms[i] + terms[i + 1] for i in range(0, len(terms), 2)]
    return terms[0]


def coarse_kernel(gathered, received, lanes, table, out, answer):
    index = lax.broadcasted_iota(jnp.int32, (8, L), 0)
    shift = jnp.broadcast_to(lanes[0:1, :] * float(VOLUME) + float(FACES), (8, L))

    def rows_of(sy, row):
        return gathered[pl.ds(sy * 8 + row, 8, stride=32), :]

    def right(m):
        sy, g = m // 4, m % 4
        rhs = rows_of(sy, g)
        if g == 0 and sy > 0:
            rhs = rhs + rows_of(sy - 1, 5)
        if g == 3 and sy < SY - 1:
            rhs = rhs + rows_of(sy + 1, 4)
        return rhs

    sums = [rows_of(sy, 6) for sy in range(SY)]

    def block(m, before):
        g = 32 * (m % 4)
        diagonal = jnp.broadcast_to(sums[m // 4][:, g : g + 1], (8, L)) + shift
        rows = []
        for r in range(8):
            row = jnp.where(index == r, diagonal, 0.0)
            row = jnp.where((index == r - 1) | (index == r + 1), -COUPLE_X, row)
            for other in before:
                row = row - (COUPLE_Y * COUPLE_Y) * other[r]
            rows.append(row)
        return rows

    inv, part = {}, {}

    def eliminate(m, sources):
        matrix = inverse_of(block(m, [inv[q] for q in sources]))
        rhs = right(m)
        for q in sources:
            rhs = rhs + COUPLE_Y * part[q]
        inv[m] = matrix
        part[m] = apply(matrix, rhs)

    for i in range(8):
        if i < 7:
            eliminate(i, [i - 1] if i else [])
        eliminate(15 - i, [16 - i] if i else [])
    eliminate(7, [6, 8])
    solved = {7: part[7]}
    for i in range(1, 9):
        for m, q in ((7 - i, 8 - i), (7 + i, 6 + i)):
            if 0 <= m < 16:
                solved[m] = part[m] + COUPLE_Y * apply(inv[m], solved[q])
    for m in range(16):
        answer[8 * m : 8 * m + 8, :] = solved[m]
    sx, sy = lax.axis_index("sx"), lax.axis_index("sy")
    own = table[pl.ds(pl.multiple_of(lax.axis_index("tm") * 8, 8), 8), :]
    group = lane_index(8) // 32
    added = jnp.zeros((8, L), jnp.float32)
    for g in range(4):
        y = answer[pl.ds((sy * 4 + g) * 8 + sx, 1), :]
        value = jnp.sum(own * y, axis=1, keepdims=True)
        added = jnp.where(group == g, value, added)
    for tp in range(4):
        rows = [received[MEMBER[s], tp] for s in range(TM)]
        turned = jnp.concatenate(rows, axis=0).T
        for t2 in range(2):
            t = 2 * tp + t2
            plus = jnp.broadcast_to(added[t : t + 1, :], (8, L))
            for x in range(8):
                r = t2 * 64 + x * 8
                out[pl.ds(t * 64 + x, 8, stride=8), :] = turned[r : r + 8] + plus


def call(kernel, name, out_shape, arrays, scratch=(), rates=None, keep=True, flops=0):
    if keep:
        out_shape = jax.tree.map(lambda o: pltpu.VMEM(o.shape, o.dtype), out_shape)
    if rates is None:
        arrays = [pltpu.with_memory_space_constraint(x, pltpu.VMEM) for x in arrays]
    scalars = [] if rates is None else [rates]
    limit = 24 * 2**20 if rates is None else None
    many = isinstance(out_shape, tuple)
    return pl.pallas_call(
        kernel,
        name=name,
        out_shape=out_shape,
        in_specs=smem(len(scalars)) + vmem(len(arrays)),
        out_specs=tuple(vmem(len(out_shape))) if many else vmem(1)[0],
        scratch_shapes=list(scratch),
        compiler_params=pltpu.CompilerParams(vmem_limit_bytes=limit),
        cost_estimate=pl.CostEstimate(flops=flops, transcendentals=0, bytes_accessed=0),
    )(*scalars, *arrays)


def swaps():
    def rank(g):
        return MEMBER[g % TM] * SY + g // TM

    pairs = [(rank(g), rank(g + 1)) for g in range(1, SY * TM - 1, 2)]
    return pairs + [(q, p) for p, q in pairs]


def local(driving_input, regime, reaction_rates):
    forward, inverse, natural, lanes = (jnp.asarray(t) for t in (FORWARD, INVERSE, NATURAL, LANES))
    packed, rate_rows, sums = call(
        pack_kernel,
        "pack",
        (shape(TM, 4 * ROWS, L), shape(L + 16, L), shape(8, L)),
        [driving_input.reshape(512, L), regime.reshape(64, L)],
        rates=reaction_rates,
    )
    received = lax.all_to_all(packed, "tm", split_axis=0, concat_axis=0, tiled=True)
    window, rate, swap = call(
        transform_kernel,
        "transform",
        (shape(8 * SPAN_Y, 8, L), shape(16, L), shape(PART, 8, L)),
        [received.reshape(TM * 4 * ROWS, L), rate_rows, forward],
    )
    swapped = lax.ppermute(swap, ("tm", "sy"), swaps())
    tiles = len(EDGE) + 2
    to_left, to_right = call(
        edge_kernel, "edges", (shape(tiles, 8, L),) * 2, [window, rate, swapped]
    )
    across = [(i, i + 1) for i in range(SX - 1)]
    left = lax.ppermute(to_right, "sx", across)
    right = lax.ppermute(to_left, "sx", [(q, p) for p, q in across])
    prepared = call(
        prepare_kernel,
        "prepare",
        (shape(SPAN_Y, 8, 8, L),) * 4,
        [window, rate, swapped, lanes],
        flops=10**7,
    )
    half = pltpu.VMEM((SPAN_Y, 8, 8, L), jnp.float32)
    message = call(
        solve_kernel,
        "sweeps",
        shape(TM * TILES * 8, L),
        [*prepared, left, right, sums, lanes, inverse],
        [half] * 4 + [pltpu.VMEM((SPAN_Y, SPAN_X, 8, L), jnp.float32)] * 2,
    )
    returned = lax.all_to_all(
        message.reshape(TM, TILES, 8, L), "tm", split_axis=0, concat_axis=0, tiled=True
    )
    shared = call(gather_kernel, "gather", shape(SX * SY, 8, L), [returned])
    gathered = lax.all_to_all(shared, ("sx", "sy"), split_axis=0, concat_axis=0, tiled=True)
    result = call(
        coarse_kernel,
        "coarse",
        shape(512, L),
        [gathered.reshape(256, L), returned, lanes, natural],
        [pltpu.VMEM((L, L), jnp.float32)],
        keep=False,
    )
    return result.reshape(driving_input.shape)


def solution(mesh):
    placed = (P("tm", None, "sx", "sy"), P(None, "sx", "sy"), P())
    return jax.shard_map(
        local, mesh=mesh, in_specs=placed, out_specs=P("tm", None, "sx", "sy"), check_vma=False
    )
```

```python
import jax
import jax.numpy as jnp
import numpy as np
from jax import lax
from jax.experimental import pallas as pl
from jax.experimental.pallas import tpu as pltpu
from jax.sharding import PartitionSpec as P

L = 128
NZ = 8
BLOCK = 8
WY = 3
WX = 4
SPAN_Y = BLOCK + 2 * WY
SPAN_X = BLOCK + 2 * WX
ROWS = 12
PART = 8 * WY + 1
TM, SX, SY = 16, 8, 4
FACES = 2 * (32 * NZ + 8 * NZ)
VOLUME = 8 * 32 * NZ
COUPLE_X = 32.0 * NZ
COUPLE_Y = 8.0 * NZ
TILES = 5


def strip_of(d):
    return d // 2 if d % 2 == 0 else TM - 1 - d // 2


MEMBER = {strip_of(d): d for d in range(TM)}


def two_parts(table):
    value = np.asarray(table, jnp.bfloat16)
    rest = np.asarray(table - np.asarray(value, np.float64), jnp.bfloat16)
    return np.stack([value, rest])


def tables():
    n = np.arange(L)
    k = np.arange(64)
    ang = 2.0 * np.pi * ((n[:, None] * k[None, :]) % L) / L
    half = np.where(n % 2 == 0, 1.0, -1.0)
    forward = np.concatenate([np.cos(ang), -np.sin(ang)], axis=1)
    forward[:, 64] = half
    weight = np.full((1, 64), 2.0)
    weight[0, 0] = 1.0
    inverse = np.concatenate([weight * np.cos(ang), -weight * np.sin(ang)], axis=1) / L
    inverse[:, 64] = half / L
    theta = 2.0 * np.pi * k / L
    shift = np.concatenate([1.0 - np.cos(theta)] * 2)
    shift[64] = 2.0
    sine = np.concatenate([np.sin(theta), -np.sin(theta)])
    sine[0] = sine[64] = 0.0
    order = np.array([8 * d + 2 * tp + t2 for t2 in range(2) for d in range(TM) for tp in range(4)])
    lanes = np.zeros((8, L))
    lanes[0] = shift
    lanes[1] = sine
    padded = np.zeros((2, TM, TILES, L))
    padded[:, :, :4] = inverse[order].reshape(2, TM, 4, L)
    as32 = lambda a: np.asarray(a, np.float32)
    return two_parts(forward[order]), two_parts(padded.reshape(-1, L)), as32(inverse), as32(lanes)


FORWARD, INVERSE, NATURAL, LANES = tables()


def vmem(count):
    return [pl.BlockSpec(memory_space=pltpu.VMEM)] * count


def smem(count):
    return [pl.BlockSpec(memory_space=pltpu.SMEM)] * count


def shape(*dims):
    return jax.ShapeDtypeStruct(dims, jnp.float32)


def dot(a, table, dims, table_first=False):
    value = a.astype(jnp.bfloat16)
    rest = (a - value.astype(jnp.float32)).astype(jnp.bfloat16)
    total = None
    for x, t in ((rest, table[0]), (value, table[1]), (value, table[0])):
        pair = (t, x) if table_first else (x, t)
        term = lax.dot_general(*pair, (dims, ((), ())), preferred_element_type=jnp.float32)
        total = term if total is None else total + term
    return total


def lane_index(rows):
    return lax.broadcasted_iota(jnp.int32, (rows, L), 1)


def halves(low, high):
    first = lane_index(low.shape[0]) < 64
    return (
        jnp.where(first, low, pltpu.roll(high, 64, 1)),
        jnp.where(first, pltpu.roll(low, 64, 1), high),
    )


def x_major(rows):
    return jnp.swapaxes(rows.reshape(8, 8, L), 0, 1).reshape(64, L)


def pack_kernel(rates, field, regime, out, rate_rows, sums):
    margin = jnp.zeros((8, L), jnp.float32)
    for tp in range(4):
        rows = [x_major(field[64 * t : 64 * t + 64, :]) for t in (2 * tp, 2 * tp + 1)]
        turned = jnp.concatenate(rows, axis=0).T
        starts = (
            jnp.concatenate([turned, margin], axis=0),
            jnp.concatenate([margin[:WY], turned, margin[WY:]], axis=0),
        )
        for d in range(TM):
            s = strip_of(d)
            out[d, ROWS * tp : ROWS * (tp + 1)] = starts[s % 2][8 * s : 8 * s + ROWS]
    kind = regime[...]
    c = jnp.zeros((64, L), jnp.float32)
    for r in range(8):
        c = c + jnp.where(kind == r, rates[r], 0.0)
    c_turned = jnp.concatenate([x_major(c), jnp.zeros((64, L), jnp.float32)], axis=0).T
    rate_rows[...] = jnp.concatenate([margin, c_turned, margin], axis=0)
    group = lane_index(1) // 32
    row = jnp.zeros((1, L), jnp.float32)
    for g in range(4):
        total = jnp.sum(c_turned[32 * g : 32 * g + 32], axis=0, keepdims=True)
        row = jnp.where(group == g, jnp.sum(total, axis=1, keepdims=True), row)
    sums[...] = jnp.broadcast_to(row, (8, L))


def own_strip():
    tm = lax.axis_index("tm")
    return jnp.where(tm & 1 == 0, tm >> 1, TM - 1 - (tm >> 1))


def transform_kernel(received, rate_rows, table, window, rate, swap):
    rows = []
    for pair in range(ROWS // 2):
        both = [received[pl.ds(2 * pair + j, 64, stride=ROWS), :] for j in range(2)]
        turned = jnp.concatenate(both, axis=0).T
        rows += list(halves(turned[:64], turned[64:]))
    spectrum = dot(jnp.concatenate(rows[: 8 + WY], axis=0), table, ((1,), (0,)))
    strip = own_strip()
    even = strip & 1 == 0
    zero = jnp.zeros((8, L), jnp.float32)
    for i in range(8 * WY):
        window[i] = zero
        window[8 * (WY + 8) + i] = zero
    offset = jnp.where(even, 8 * WY, 0)
    for i in range(8 * (8 + WY)):
        window[offset + i] = spectrum[8 * i : 8 * i + 8]
    near = rate_rows[pl.ds(pl.multiple_of(strip * 8, 8), 24), :]
    mine = jnp.concatenate([near[8 - WY : 16 + WY], jnp.zeros((2, L), jnp.float32)], axis=0)
    rate[...] = mine
    for i in range(8 * WY):
        swap[i] = jnp.where(even, window[8 * WY + i], window[64 + i])
    swap[PART - 1] = jnp.where(even, pltpu.roll(mine[0:8], 8 - WY, 0), mine[8:16])


def x_range(distance):
    return range(distance - 1, SPAN_Y + 1 - distance)


EDGE = [(d, y) for d in range(1, WX + 1) for y in x_range(d)]


def completed(window, rate, swapped):
    strip = own_strip()
    even = jnp.where(strip & 1 == 0, 1.0, 0.0)
    odd = 1.0 - even

    def tile(y, x):
        if y < WY:
            return window[8 * y + x] + even * swapped[8 * y + x]
        if y < WY + 8:
            return window[8 * y + x]
        return window[8 * y + x] + odd * swapped[8 * (y - WY - 8) + x]

    first = jnp.where(strip == 0, 1.0, 0.0)
    last = jnp.where(strip == TM - 1, 1.0, 0.0)
    row = lax.broadcasted_iota(jnp.int32, (8, L), 0)
    other = jnp.where(row < WY, swapped[PART - 1], 0.0)
    low = rate[0:8, :] + first * other
    high = rate[8:16, :] + last * pltpu.roll(other, WY, 0)
    return tile, (low, high)


def edge_kernel(window, rate, swapped, to_left, to_right):
    tile, rates = completed(window, rate, swapped)
    for i, (d, y) in enumerate(EDGE):
        to_left[i] = tile(y, d - 1)
        to_right[i] = tile(y, 8 - d)
    for j, c in enumerate(rates):
        to_left[len(EDGE) + j] = c
        to_right[len(EDGE) + j] = c


def inside():
    sx, sy, strip = lax.axis_index("sx"), lax.axis_index("sy"), own_strip()
    return [
        jnp.where(ok, 1.0, 0.0)
        for ok in (
            sx > 0,
            sx < SX - 1,
            (sy > 0) | (strip > 0),
            (sy < SY - 1) | (strip < TM - 1),
        )
    ]


def cell_terms(c, lanes):
    d = c + lanes[0:1, :] + 6.0
    sine = lanes[1:2, :]
    inverse = 1.0 / (d * d + sine * sine)
    return d * inverse, sine * inverse


def prepare_kernel(window, rate, swapped, lanes, source, a, b, first):
    tile, rates = completed(window, rate, swapped)
    valid = inside()
    rows = jnp.concatenate([*rates, jnp.zeros((112, L), jnp.float32)], axis=0)
    turned = rows.T
    for y in range(SPAN_Y):
        for x in range(8):
            c = jnp.broadcast_to(turned[8 * x : 8 * x + 8, y : y + 1], (8, L))
            ax, bx = cell_terms(c, lanes)
            if not WY <= y < WY + 8:
                ok = valid[2] if y < WY else valid[3]
                ax, bx = ax * ok, bx * ok
            s = tile(y, x)
            source[y, x] = s
            a[y, x] = ax
            b[y, x] = bx
            first[y, x] = ax * s + bx * pltpu.roll(s, 64, 1)


def solve_kernel(
    own_s, own_a, own_b, own_x, left, right, sums, lanes, table, out, hs, ha, hb, hx, x0, x1
):
    strip = own_strip()
    valid = inside()
    zero = jnp.zeros((8, L), jnp.float32)

    for y in range(SPAN_Y):
        for h in range(8):
            hs[y, h] = zero
    for i, (d, y) in enumerate(EDGE):
        hs[y, WX - d] = left[i]
        hs[y, WX - 1 + d] = right[i]
    lane = lane_index(8)
    rows = []
    for j in range(2):
        n = len(EDGE) + j
        rows.append(jnp.where(lane < 32, pltpu.roll(left[n], 96, 1), pltpu.roll(right[n], 32, 1)))
    rows.append(jnp.zeros((112, L), jnp.float32))
    turned = jnp.concatenate(rows, axis=0).T
    for y in range(SPAN_Y):
        for h in range(8):
            distance = WX - h if h < WX else h - WX + 1
            if y not in x_range(distance):
                ha[y, h] = zero
                hb[y, h] = zero
                hx[y, h] = zero
                continue
            c = jnp.broadcast_to(turned[8 * h : 8 * h + 8, y : y + 1], (8, L))
            ax, bx = cell_terms(c, lanes)
            ok = valid[0] if h < WX else valid[1]
            if y < WY:
                ok = ok * valid[2]
            elif y >= WY + 8:
                ok = ok * valid[3]
            ax, bx = ax * ok, bx * ok
            s = hs[y, h]
            ha[y, h] = ax
            hb[y, h] = bx
            hx[y, h] = ax * s + bx * pltpu.roll(s, 64, 1)

    def split(own, halo):
        def get(y, x):
            if x < WX:
                return halo[y, x]
            if x < WX + 8:
                return own[y, x - WX]
            return halo[y, x - 8]

        return get

    source, a, b = split(own_s, hs), split(own_a, ha), split(own_b, hb)

    def whole(ref):
        return lambda y, x: ref[y, x]

    def sweep(old, new, margin):
        def row(y, carry):
            for x in range(margin, SPAN_X - margin):
                v = old(y, x)
                u = source(y, x) + (old(y, x + 1) + old(y, x - 1))
                u = u + (old(y + 1, x) + old(y - 1, x))
                u = u + (pltpu.roll(v, 1, 0) + pltpu.roll(v, 7, 0))
                new[y, x] = a(y, x) * u + b(y, x) * pltpu.roll(u, 64, 1)
            return carry

        lax.fori_loop(margin, SPAN_Y - margin, row, 0)

    sweep(split(own_x, hx), x1, 1)
    sweep(whole(x1), x0, 2)
    sweep(whole(x0), x1, 3)
    lo, hi = WX, WX + 8

    def change(y, x):
        return x1[y, x] - x0[y, x]

    acc = zero
    faces = []
    for y in range(WY, WY + 8):
        line = zero
        for x in range(lo, hi):
            line = line + change(y, x)
        end = y in (WY, WY + 7)
        acc = acc + (5.0 if end else 6.0) * line
        acc = acc + (change(y, lo - 1) - change(y, lo)) + (change(y, hi) - change(y, hi - 1))
        if end:
            faces.append(line)
    solved = x1[WY : WY + 8, lo:hi].reshape(512, L)
    result = dot(solved, table, ((1,), (1,)), table_first=True)
    by_y = []
    for pair in range(4):
        cut = result[:, 128 * pair : 128 * pair + 128]
        by_y += list(halves(cut[: TM * TILES], cut[TM * TILES :]))
    out[...] = jnp.swapaxes(jnp.stack(by_y), 0, 1).reshape(TM * TILES * 8, L)
    homes = (
        strip >> 2,
        jnp.where(strip == 0, 4, (strip - 1) >> 2),
        jnp.where(strip == TM - 1, 5, (strip + 1) >> 2),
    )
    index = lax.broadcasted_iota(jnp.int32, (8, L), 0)
    share = jnp.where((index == 6) & (strip == 0), sums[...], 0.0)
    for home, v in zip(homes, (acc, *faces)):
        v = jnp.broadcast_to(jnp.sum(v, axis=0, keepdims=True), (8, L))
        share = share + jnp.where(index == home, v, 0.0)
    for d in range(TM):
        out[8 * (TILES * d + 4) : 8 * (TILES * d + 5), :] = share


def gather_kernel(received, out):
    block = received[0, 4]
    for d in range(1, TM):
        block = block + received[d, 4]
    for j in range(SX * SY):
        out[j] = block


def inverse_of(rows):
    rows = list(rows)
    index = lax.broadcasted_iota(jnp.int32, (8, L), 0)
    for p in range(8):
        here = index == p
        pivot = jnp.broadcast_to(rows[p][p : p + 1], (8, L))
        scale = 1.0 / pivot
        lead = jnp.where(here, scale, rows[p] * scale)
        for r in range(8):
            if r != p:
                factor = jnp.broadcast_to(rows[r][p : p + 1], (8, L))
                rows[r] = jnp.where(here, 0.0, rows[r]) - factor * lead
        rows[p] = lead
    return rows


def apply(rows, v):
    terms = [rows[c] * jnp.broadcast_to(v[c : c + 1], (8, L)) for c in range(8)]
    while len(terms) > 1:
        terms = [terms[i] + terms[i + 1] for i in range(0, len(terms), 2)]
    return terms[0]


def coarse_kernel(gathered, received, lanes, table, out, answer):
    index = lax.broadcasted_iota(jnp.int32, (8, L), 0)
    shift = jnp.broadcast_to(lanes[0:1, :] * float(VOLUME) + float(FACES), (8, L))

    by_row = [jnp.swapaxes(gathered[:, sy], 0, 1) for sy in range(SY)]

    def rows_of(sy, row):
        return by_row[sy][row]

    def right(m):
        sy, g = m // 4, m % 4
        rhs = rows_of(sy, g)
        if g == 0 and sy > 0:
            rhs = rhs + rows_of(sy - 1, 5)
        if g == 3 and sy < SY - 1:
            rhs = rhs + rows_of(sy + 1, 4)
        return rhs

    sums = [rows_of(sy, 6) for sy in range(SY)]

    def block(m, before):
        g = 32 * (m % 4)
        diagonal = jnp.broadcast_to(sums[m // 4][:, g : g + 1], (8, L)) + shift
        rows = []
        for r in range(8):
            row = jnp.where(index == r, diagonal, 0.0)
            row = jnp.where((index == r - 1) | (index == r + 1), -COUPLE_X, row)
            for other in before:
                row = row - (COUPLE_Y * COUPLE_Y) * other[r]
            rows.append(row)
        return rows

    inv, part = {}, {}

    def eliminate(m, sources):
        matrix = inverse_of(block(m, [inv[q] for q in sources]))
        rhs = right(m)
        for q in sources:
            rhs = rhs + COUPLE_Y * part[q]
        inv[m] = matrix
        part[m] = apply(matrix, rhs)

    for i in range(8):
        if i < 7:
            eliminate(i, [i - 1] if i else [])
        eliminate(15 - i, [16 - i] if i else [])
    eliminate(7, [6, 8])
    solved = {7: part[7]}
    for i in range(1, 9):
        for m, q in ((7 - i, 8 - i), (7 + i, 6 + i)):
            if 0 <= m < 16:
                solved[m] = part[m] + COUPLE_Y * apply(inv[m], solved[q])
    for m in range(16):
        answer[8 * m : 8 * m + 8, :] = solved[m]
    sx, sy = lax.axis_index("sx"), lax.axis_index("sy")
    own = table[pl.ds(pl.multiple_of(lax.axis_index("tm") * 8, 8), 8), :]
    group = lane_index(8) // 32
    added = jnp.zeros((8, L), jnp.float32)
    for g in range(4):
        y = answer[pl.ds((sy * 4 + g) * 8 + sx, 1), :]
        value = jnp.sum(own * y, axis=1, keepdims=True)
        added = jnp.where(group == g, value, added)
    for tp in range(4):
        rows = [received[MEMBER[s], tp] for s in range(TM)]
        turned = jnp.concatenate(rows, axis=0).T
        for t2 in range(2):
            t = 2 * tp + t2
            out[64 * t : 64 * t + 64, :] = x_major(turned[64 * t2 : 64 * t2 + 64]) + added[t : t + 1, :]


def call(kernel, name, out_shape, arrays, scratch=(), rates=None, keep=True, flops=0):
    if keep:
        out_shape = jax.tree.map(lambda o: pltpu.VMEM(o.shape, o.dtype), out_shape)
    if rates is None:
        arrays = [pltpu.with_memory_space_constraint(x, pltpu.VMEM) for x in arrays]
    scalars = [] if rates is None else [rates]
    limit = 24 * 2**20 if rates is None else None
    many = isinstance(out_shape, tuple)
    return pl.pallas_call(
        kernel,
        name=name,
        out_shape=out_shape,
        in_specs=smem(len(scalars)) + vmem(len(arrays)),
        out_specs=tuple(vmem(len(out_shape))) if many else vmem(1)[0],
        scratch_shapes=list(scratch),
        compiler_params=pltpu.CompilerParams(vmem_limit_bytes=limit),
        cost_estimate=pl.CostEstimate(flops=flops, transcendentals=0, bytes_accessed=0),
    )(*scalars, *arrays)


def swaps():
    def rank(g):
        return MEMBER[g % TM] * SY + g // TM

    pairs = [(rank(g), rank(g + 1)) for g in range(1, SY * TM - 1, 2)]
    return pairs + [(q, p) for p, q in pairs]


def local(driving_input, regime, reaction_rates):
    forward, inverse, natural, lanes = (jnp.asarray(t) for t in (FORWARD, INVERSE, NATURAL, LANES))
    packed, rate_rows, sums = call(
        pack_kernel,
        "pack",
        (shape(TM, 4 * ROWS, L), shape(L + 16, L), shape(8, L)),
        [driving_input.reshape(512, L), regime.reshape(64, L)],
        rates=reaction_rates,
    )
    received = lax.all_to_all(packed, "tm", split_axis=0, concat_axis=0, tiled=True)
    window, rate, swap = call(
        transform_kernel,
        "transform",
        (shape(8 * SPAN_Y, 8, L), shape(16, L), shape(PART, 8, L)),
        [received.reshape(TM * 4 * ROWS, L), rate_rows, forward],
    )
    swapped = lax.ppermute(swap, ("tm", "sy"), swaps())
    tiles = len(EDGE) + 2
    to_left, to_right = call(
        edge_kernel, "edges", (shape(tiles, 8, L),) * 2, [window, rate, swapped]
    )
    across = [(i, i + 1) for i in range(SX - 1)]
    left = lax.ppermute(to_right, "sx", across)
    right = lax.ppermute(to_left, "sx", [(q, p) for p, q in across])
    prepared = call(
        prepare_kernel,
        "prepare",
        (shape(SPAN_Y, 8, 8, L),) * 4,
        [window, rate, swapped, lanes],
        flops=10**7,
    )
    half = pltpu.VMEM((SPAN_Y, 8, 8, L), jnp.float32)
    message = call(
        solve_kernel,
        "sweeps",
        shape(TM * TILES * 8, L),
        [*prepared, left, right, sums, lanes, inverse],
        [half] * 4 + [pltpu.VMEM((SPAN_Y, SPAN_X, 8, L), jnp.float32)] * 2,
    )
    returned = lax.all_to_all(
        message.reshape(TM, TILES, 8, L), "tm", split_axis=0, concat_axis=0, tiled=True
    )
    shared = call(gather_kernel, "gather", shape(SX * SY, 8, L), [returned])
    gathered = lax.all_to_all(shared, ("sx", "sy"), split_axis=0, concat_axis=0, tiled=True)
    result = call(
        coarse_kernel,
        "coarse",
        shape(512, L),
        [gathered.reshape(SX, SY, 8, L), returned, lanes, natural],
        [pltpu.VMEM((L, L), jnp.float32)],
        keep=False,
    )
    return result.reshape(driving_input.shape)


def solution(mesh):
    placed = (P("tm", None, "sx", "sy"), P(None, "sx", "sy"), P())
    return jax.shard_map(
        local, mesh=mesh, in_specs=placed, out_specs=P("tm", None, "sx", "sy"), check_vma=False
    )
```

```python
import jax
import jax.numpy as jnp
import numpy as np
from jax import lax
from jax.experimental import pallas as pl
from jax.experimental.pallas import tpu as pltpu
from jax.sharding import PartitionSpec as P

L = 128
NZ = 8
BLOCK = 8
WY = 3
WX = 4
SPAN_Y = BLOCK + 2 * WY
SPAN_X = BLOCK + 2 * WX
ROWS = 12
PART = 8 * WY + 1
TM, SX, SY = 16, 8, 4
FACES = 2 * (32 * NZ + 8 * NZ)
VOLUME = 8 * 32 * NZ
COUPLE_X = 32.0 * NZ
COUPLE_Y = 8.0 * NZ
TILES = 5


def strip_of(d):
    return d // 2 if d % 2 == 0 else TM - 1 - d // 2


MEMBER = {strip_of(d): d for d in range(TM)}


def two_parts(table):
    value = np.asarray(table, jnp.bfloat16)
    rest = np.asarray(table - np.asarray(value, np.float64), jnp.bfloat16)
    return np.stack([value, rest])


def tables():
    n = np.arange(L)
    k = np.arange(64)
    ang = 2.0 * np.pi * ((n[:, None] * k[None, :]) % L) / L
    half = np.where(n % 2 == 0, 1.0, -1.0)
    forward = np.concatenate([np.cos(ang), -np.sin(ang)], axis=1)
    forward[:, 64] = half
    weight = np.full((1, 64), 2.0)
    weight[0, 0] = 1.0
    inverse = np.concatenate([weight * np.cos(ang), -weight * np.sin(ang)], axis=1) / L
    inverse[:, 64] = half / L
    theta = 2.0 * np.pi * k / L
    shift = np.concatenate([1.0 - np.cos(theta)] * 2)
    shift[64] = 2.0
    sine = np.concatenate([np.sin(theta), -np.sin(theta)])
    sine[0] = sine[64] = 0.0
    order = np.array([8 * d + 2 * tp + t2 for t2 in range(2) for d in range(TM) for tp in range(4)])
    lanes = np.zeros((8, L))
    lanes[0] = shift
    lanes[1] = sine
    padded = np.zeros((2, TM, TILES, L))
    padded[:, :, :4] = inverse[order].reshape(2, TM, 4, L)
    as32 = lambda a: np.asarray(a, np.float32)
    return two_parts(forward[order]), two_parts(padded.reshape(-1, L)), as32(inverse), as32(lanes)


FORWARD, INVERSE, NATURAL, LANES = tables()


def vmem(count):
    return [pl.BlockSpec(memory_space=pltpu.VMEM)] * count


def smem(count):
    return [pl.BlockSpec(memory_space=pltpu.SMEM)] * count


def shape(*dims):
    return jax.ShapeDtypeStruct(dims, jnp.float32)


def dot(a, table, dims, table_first=False):
    value = a.astype(jnp.bfloat16)
    rest = (a - value.astype(jnp.float32)).astype(jnp.bfloat16)
    total = None
    for x, t in ((rest, table[0]), (value, table[1]), (value, table[0])):
        pair = (t, x) if table_first else (x, t)
        term = lax.dot_general(*pair, (dims, ((), ())), preferred_element_type=jnp.float32)
        total = term if total is None else total + term
    return total


def lane_index(rows):
    return lax.broadcasted_iota(jnp.int32, (rows, L), 1)


def halves(low, high):
    first = lane_index(low.shape[0]) < 64
    return (
        jnp.where(first, low, pltpu.roll(high, 64, 1)),
        jnp.where(first, pltpu.roll(low, 64, 1), high),
    )


def x_major(rows):
    return jnp.swapaxes(rows.reshape(8, 8, L), 0, 1).reshape(64, L)


def pack_kernel(rates, field, regime, out, rate_rows, sums):
    margin = jnp.zeros((8, L), jnp.float32)
    for tp in range(4):
        rows = [x_major(field[64 * t : 64 * t + 64, :]) for t in (2 * tp, 2 * tp + 1)]
        turned = jnp.concatenate(rows, axis=0).T
        starts = (
            jnp.concatenate([turned, margin], axis=0),
            jnp.concatenate([margin[:WY], turned, margin[WY:]], axis=0),
        )
        for d in range(TM):
            s = strip_of(d)
            out[d, ROWS * tp : ROWS * (tp + 1)] = starts[s % 2][8 * s : 8 * s + ROWS]
    kind = regime[...]
    c = jnp.zeros((64, L), jnp.float32)
    for r in range(8):
        c = c + jnp.where(kind == r, rates[r], 0.0)
    c_turned = jnp.concatenate([x_major(c), jnp.zeros((64, L), jnp.float32)], axis=0).T
    rate_rows[...] = jnp.concatenate([margin, c_turned, margin], axis=0)
    group = lane_index(1) // 32
    row = jnp.zeros((1, L), jnp.float32)
    for g in range(4):
        total = jnp.sum(c_turned[32 * g : 32 * g + 32], axis=0, keepdims=True)
        row = jnp.where(group == g, jnp.sum(total, axis=1, keepdims=True), row)
    sums[...] = jnp.broadcast_to(row, (8, L))


def own_strip():
    tm = lax.axis_index("tm")
    return jnp.where(tm & 1 == 0, tm >> 1, TM - 1 - (tm >> 1))


def transform_kernel(received, rate_rows, table, window, rate, swap):
    rows = []
    for pair in range(ROWS // 2):
        both = [received[pl.ds(2 * pair + j, 64, stride=ROWS), :] for j in range(2)]
        turned = jnp.concatenate(both, axis=0).T
        rows += list(halves(turned[:64], turned[64:]))
    spectrum = dot(jnp.concatenate(rows[: 8 + WY], axis=0), table, ((1,), (0,)))
    strip = own_strip()
    even = strip & 1 == 0
    zero = jnp.zeros((8, L), jnp.float32)
    for i in range(8 * WY):
        window[i] = zero
        window[8 * (WY + 8) + i] = zero
    offset = jnp.where(even, 8 * WY, 0)
    for i in range(8 * (8 + WY)):
        window[offset + i] = spectrum[8 * i : 8 * i + 8]
    near = rate_rows[pl.ds(pl.multiple_of(strip * 8, 8), 24), :]
    mine = jnp.concatenate([near[8 - WY : 16 + WY], jnp.zeros((2, L), jnp.float32)], axis=0)
    rate[...] = mine
    for i in range(8 * WY):
        swap[i] = jnp.where(even, window[8 * WY + i], window[64 + i])
    swap[PART - 1] = jnp.where(even, pltpu.roll(mine[0:8], 8 - WY, 0), mine[8:16])


def x_range(distance):
    return range(distance - 1, SPAN_Y + 1 - distance)


EDGE = [(d, y) for d in range(1, WX + 1) for y in x_range(d)]


def completed(window, rate, swapped):
    strip = own_strip()
    even = jnp.where(strip & 1 == 0, 1.0, 0.0)
    odd = 1.0 - even

    def tile(y, x):
        if y < WY:
            return window[8 * y + x] + even * swapped[8 * y + x]
        if y < WY + 8:
            return window[8 * y + x]
        return window[8 * y + x] + odd * swapped[8 * (y - WY - 8) + x]

    first = jnp.where(strip == 0, 1.0, 0.0)
    last = jnp.where(strip == TM - 1, 1.0, 0.0)
    row = lax.broadcasted_iota(jnp.int32, (8, L), 0)
    other = jnp.where(row < WY, swapped[PART - 1], 0.0)
    low = rate[0:8, :] + first * other
    high = rate[8:16, :] + last * pltpu.roll(other, WY, 0)
    return tile, (low, high)


def edge_kernel(window, rate, swapped, to_left, to_right):
    tile, rates = completed(window, rate, swapped)
    for i, (d, y) in enumerate(EDGE):
        to_left[i] = tile(y, d - 1)
        to_right[i] = tile(y, 8 - d)
    for j, c in enumerate(rates):
        to_left[len(EDGE) + j] = c
        to_right[len(EDGE) + j] = c


def inside():
    sx, sy, strip = lax.axis_index("sx"), lax.axis_index("sy"), own_strip()
    return [
        jnp.where(ok, 1.0, 0.0)
        for ok in (
            sx > 0,
            sx < SX - 1,
            (sy > 0) | (strip > 0),
            (sy < SY - 1) | (strip < TM - 1),
        )
    ]


def cell_terms(c, lanes):
    d = c + lanes[0:1, :] + 6.0
    sine = lanes[1:2, :]
    inverse = 1.0 / (d * d + sine * sine)
    return d * inverse, sine * inverse


def prepare_kernel(window, rate, swapped, lanes, source, a, b, first):
    tile, rates = completed(window, rate, swapped)
    valid = inside()
    rows = jnp.concatenate([*rates, jnp.zeros((112, L), jnp.float32)], axis=0)
    turned = rows.T
    for y in range(SPAN_Y):
        for x in range(8):
            c = jnp.broadcast_to(turned[8 * x : 8 * x + 8, y : y + 1], (8, L))
            ax, bx = cell_terms(c, lanes)
            if not WY <= y < WY + 8:
                ok = valid[2] if y < WY else valid[3]
                ax, bx = ax * ok, bx * ok
            s = tile(y, x)
            source[y, x] = s
            a[y, x] = ax
            b[y, x] = bx
            first[y, x] = ax * s + bx * pltpu.roll(s, 64, 1)


def solve_kernel(
    own_s, own_a, own_b, own_x, left, right, sums, lanes, table, out, hs, ha, hb, hx, x0, x1
):
    strip = own_strip()
    valid = inside()
    zero = jnp.zeros((8, L), jnp.float32)

    for y in range(SPAN_Y):
        for h in range(8):
            hs[y, h] = zero
    for i, (d, y) in enumerate(EDGE):
        hs[y, WX - d] = left[i]
        hs[y, WX - 1 + d] = right[i]
    lane = lane_index(8)
    rows = []
    for j in range(2):
        n = len(EDGE) + j
        rows.append(jnp.where(lane < 32, pltpu.roll(left[n], 96, 1), pltpu.roll(right[n], 32, 1)))
    rows.append(jnp.zeros((112, L), jnp.float32))
    turned = jnp.concatenate(rows, axis=0).T
    for y in range(SPAN_Y):
        for h in range(8):
            distance = WX - h if h < WX else h - WX + 1
            if y not in x_range(distance):
                ha[y, h] = zero
                hb[y, h] = zero
                hx[y, h] = zero
                continue
            c = jnp.broadcast_to(turned[8 * h : 8 * h + 8, y : y + 1], (8, L))
            ax, bx = cell_terms(c, lanes)
            ok = valid[0] if h < WX else valid[1]
            if y < WY:
                ok = ok * valid[2]
            elif y >= WY + 8:
                ok = ok * valid[3]
            ax, bx = ax * ok, bx * ok
            s = hs[y, h]
            ha[y, h] = ax
            hb[y, h] = bx
            hx[y, h] = ax * s + bx * pltpu.roll(s, 64, 1)

    def split(own, halo):
        def get(y, x):
            if x < WX:
                return halo[y, x]
            if x < WX + 8:
                return own[y, x - WX]
            return halo[y, x - 8]

        return get

    source, a, b = split(own_s, hs), split(own_a, ha), split(own_b, hb)

    def whole(ref):
        return lambda y, x: ref[y, x]

    def sweep(old, new, margin):
        for y in range(margin, SPAN_Y - margin):
            for x in range(margin, SPAN_X - margin):
                distance = max(WX - x, x - WX - 7, 1)
                if not distance - 1 + margin <= y < SPAN_Y + 1 - margin - distance:
                    continue
                v = old(y, x)
                u = source(y, x) + (old(y, x + 1) + old(y, x - 1))
                u = u + (old(y + 1, x) + old(y - 1, x))
                u = u + (pltpu.roll(v, 1, 0) + pltpu.roll(v, 7, 0))
                new[y, x] = a(y, x) * u + b(y, x) * pltpu.roll(u, 64, 1)

    sweep(split(own_x, hx), x1, 1)
    sweep(whole(x1), x0, 2)
    sweep(whole(x0), x1, 3)
    lo, hi = WX, WX + 8

    def change(y, x):
        return x1[y, x] - x0[y, x]

    acc = zero
    faces = []
    for y in range(WY, WY + 8):
        line = zero
        for x in range(lo, hi):
            line = line + change(y, x)
        end = y in (WY, WY + 7)
        acc = acc + (5.0 if end else 6.0) * line
        acc = acc + (change(y, lo - 1) - change(y, lo)) + (change(y, hi) - change(y, hi - 1))
        if end:
            faces.append(line)
    solved = x1[WY : WY + 8, lo:hi].reshape(512, L)
    result = dot(solved, table, ((1,), (1,)), table_first=True)
    by_y = []
    for pair in range(4):
        cut = result[:, 128 * pair : 128 * pair + 128]
        by_y += list(halves(cut[: TM * TILES], cut[TM * TILES :]))
    out[...] = jnp.swapaxes(jnp.stack(by_y), 0, 1).reshape(TM * TILES * 8, L)
    homes = (
        strip >> 2,
        jnp.where(strip == 0, 4, (strip - 1) >> 2),
        jnp.where(strip == TM - 1, 5, (strip + 1) >> 2),
    )
    index = lax.broadcasted_iota(jnp.int32, (8, L), 0)
    share = jnp.where((index == 6) & (strip == 0), sums[...], 0.0)
    for home, v in zip(homes, (acc, *faces)):
        v = jnp.broadcast_to(jnp.sum(v, axis=0, keepdims=True), (8, L))
        share = share + jnp.where(index == home, v, 0.0)
    for d in range(TM):
        out[8 * (TILES * d + 4) : 8 * (TILES * d + 5), :] = share


def gather_kernel(received, out):
    block = received[0, 4]
    for d in range(1, TM):
        block = block + received[d, 4]
    for j in range(SX * SY):
        out[j] = block


def inverse_of(rows):
    rows = list(rows)
    index = lax.broadcasted_iota(jnp.int32, (8, L), 0)
    for p in range(8):
        here = index == p
        pivot = jnp.broadcast_to(rows[p][p : p + 1], (8, L))
        scale = 1.0 / pivot
        lead = jnp.where(here, scale, rows[p] * scale)
        for r in range(8):
            if r != p:
                factor = jnp.broadcast_to(rows[r][p : p + 1], (8, L))
                rows[r] = jnp.where(here, 0.0, rows[r]) - factor * lead
        rows[p] = lead
    return rows


def apply(rows, v):
    terms = [rows[c] * jnp.broadcast_to(v[c : c + 1], (8, L)) for c in range(8)]
    while len(terms) > 1:
        terms = [terms[i] + terms[i + 1] for i in range(0, len(terms), 2)]
    return terms[0]


def coarse_kernel(gathered, received, lanes, table, out, answer):
    index = lax.broadcasted_iota(jnp.int32, (8, L), 0)
    shift = jnp.broadcast_to(lanes[0:1, :] * float(VOLUME) + float(FACES), (8, L))

    by_row = [jnp.swapaxes(gathered[:, sy], 0, 1) for sy in range(SY)]

    def rows_of(sy, row):
        return by_row[sy][row]

    def right(m):
        sy, g = m // 4, m % 4
        rhs = rows_of(sy, g)
        if g == 0 and sy > 0:
            rhs = rhs + rows_of(sy - 1, 5)
        if g == 3 and sy < SY - 1:
            rhs = rhs + rows_of(sy + 1, 4)
        return rhs

    sums = [rows_of(sy, 6) for sy in range(SY)]

    def block(m, before):
        g = 32 * (m % 4)
        diagonal = jnp.broadcast_to(sums[m // 4][:, g : g + 1], (8, L)) + shift
        rows = []
        for r in range(8):
            row = jnp.where(index == r, diagonal, 0.0)
            row = jnp.where((index == r - 1) | (index == r + 1), -COUPLE_X, row)
            for other in before:
                row = row - (COUPLE_Y * COUPLE_Y) * other[r]
            rows.append(row)
        return rows

    inv, part = {}, {}

    def eliminate(m, sources):
        matrix = inverse_of(block(m, [inv[q] for q in sources]))
        rhs = right(m)
        for q in sources:
            rhs = rhs + COUPLE_Y * part[q]
        inv[m] = matrix
        part[m] = apply(matrix, rhs)

    for i in range(8):
        if i < 7:
            eliminate(i, [i - 1] if i else [])
        eliminate(15 - i, [16 - i] if i else [])
    eliminate(7, [6, 8])
    solved = {7: part[7]}
    for i in range(1, 9):
        for m, q in ((7 - i, 8 - i), (7 + i, 6 + i)):
            if 0 <= m < 16:
                solved[m] = part[m] + COUPLE_Y * apply(inv[m], solved[q])
    for m in range(16):
        answer[8 * m : 8 * m + 8, :] = solved[m]
    sx, sy = lax.axis_index("sx"), lax.axis_index("sy")
    own = table[pl.ds(pl.multiple_of(lax.axis_index("tm") * 8, 8), 8), :]
    group = lane_index(8) // 32
    added = jnp.zeros((8, L), jnp.float32)
    for g in range(4):
        y = answer[pl.ds((sy * 4 + g) * 8 + sx, 1), :]
        value = jnp.sum(own * y, axis=1, keepdims=True)
        added = jnp.where(group == g, value, added)
    for tp in range(4):
        rows = [received[MEMBER[s], tp] for s in range(TM)]
        turned = jnp.concatenate(rows, axis=0).T
        for t2 in range(2):
            t = 2 * tp + t2
            out[64 * t : 64 * t + 64, :] = x_major(turned[64 * t2 : 64 * t2 + 64]) + added[t : t + 1, :]


def call(kernel, name, out_shape, arrays, scratch=(), rates=None, keep=True, flops=0):
    if keep:
        out_shape = jax.tree.map(lambda o: pltpu.VMEM(o.shape, o.dtype), out_shape)
    if rates is None:
        arrays = [pltpu.with_memory_space_constraint(x, pltpu.VMEM) for x in arrays]
    scalars = [] if rates is None else [rates]
    limit = 24 * 2**20 if rates is None else None
    many = isinstance(out_shape, tuple)
    return pl.pallas_call(
        kernel,
        name=name,
        out_shape=out_shape,
        in_specs=smem(len(scalars)) + vmem(len(arrays)),
        out_specs=tuple(vmem(len(out_shape))) if many else vmem(1)[0],
        scratch_shapes=list(scratch),
        compiler_params=pltpu.CompilerParams(vmem_limit_bytes=limit),
        cost_estimate=pl.CostEstimate(flops=flops, transcendentals=0, bytes_accessed=0),
    )(*scalars, *arrays)


def swaps():
    def rank(g):
        return MEMBER[g % TM] * SY + g // TM

    pairs = [(rank(g), rank(g + 1)) for g in range(1, SY * TM - 1, 2)]
    return pairs + [(q, p) for p, q in pairs]


def local(driving_input, regime, reaction_rates):
    forward, inverse, natural, lanes = (jnp.asarray(t) for t in (FORWARD, INVERSE, NATURAL, LANES))
    packed, rate_rows, sums = call(
        pack_kernel,
        "pack",
        (shape(TM, 4 * ROWS, L), shape(L + 16, L), shape(8, L)),
        [driving_input.reshape(512, L), regime.reshape(64, L)],
        rates=reaction_rates,
    )
    received = lax.all_to_all(packed, "tm", split_axis=0, concat_axis=0, tiled=True)
    window, rate, swap = call(
        transform_kernel,
        "transform",
        (shape(8 * SPAN_Y, 8, L), shape(16, L), shape(PART, 8, L)),
        [received.reshape(TM * 4 * ROWS, L), rate_rows, forward],
    )
    swapped = lax.ppermute(swap, ("tm", "sy"), swaps())
    tiles = len(EDGE) + 2
    to_left, to_right = call(
        edge_kernel, "edges", (shape(tiles, 8, L),) * 2, [window, rate, swapped]
    )
    across = [(i, i + 1) for i in range(SX - 1)]
    left = lax.ppermute(to_right, "sx", across)
    right = lax.ppermute(to_left, "sx", [(q, p) for p, q in across])
    prepared = call(
        prepare_kernel,
        "prepare",
        (shape(SPAN_Y, 8, 8, L),) * 4,
        [window, rate, swapped, lanes],
        flops=10**7,
    )
    half = pltpu.VMEM((SPAN_Y, 8, 8, L), jnp.float32)
    message = call(
        solve_kernel,
        "sweeps",
        shape(TM * TILES * 8, L),
        [*prepared, left, right, sums, lanes, inverse],
        [half] * 4 + [pltpu.VMEM((SPAN_Y, SPAN_X, 8, L), jnp.float32)] * 2,
    )
    returned = lax.all_to_all(
        message.reshape(TM, TILES, 8, L), "tm", split_axis=0, concat_axis=0, tiled=True
    )
    shared = call(gather_kernel, "gather", shape(SX * SY, 8, L), [returned])
    gathered = lax.all_to_all(shared, ("sx", "sy"), split_axis=0, concat_axis=0, tiled=True)
    result = call(
        coarse_kernel,
        "coarse",
        shape(512, L),
        [gathered.reshape(SX, SY, 8, L), returned, lanes, natural],
        [pltpu.VMEM((L, L), jnp.float32)],
        keep=False,
    )
    return result.reshape(driving_input.shape)


def solution(mesh):
    placed = (P("tm", None, "sx", "sy"), P(None, "sx", "sy"), P())
    return jax.shard_map(
        local, mesh=mesh, in_specs=placed, out_specs=P("tm", None, "sx", "sy"), check_vma=False
    )
```

```python
import jax
import jax.numpy as jnp
import numpy as np
from jax import lax
from jax.experimental import pallas as pl
from jax.experimental.pallas import tpu as pltpu
from jax.sharding import PartitionSpec as P

L = 128
NZ = 8
BLOCK = 8
WY = 3
WX = 4
SPAN_Y = BLOCK + 2 * WY
SPAN_X = BLOCK + 2 * WX
ROWS = 12
PART = 8 * WY + 1
TM, SX, SY = 16, 8, 4
FACES = 2 * (32 * NZ + 8 * NZ)
VOLUME = 8 * 32 * NZ
COUPLE_X = 32.0 * NZ
COUPLE_Y = 8.0 * NZ
TILES = 5


def strip_of(d):
    if d % 2 == 1:
        return 7 + d // 2
    return {0: 0, 2: TM - 1}.get(d, d // 2 - 1)


MEMBER = {strip_of(d): d for d in range(TM)}


def two_parts(table):
    value = np.asarray(table, jnp.bfloat16)
    rest = np.asarray(table - np.asarray(value, np.float64), jnp.bfloat16)
    return np.stack([value, rest])


def tables():
    n = np.arange(L)
    k = np.arange(64)
    ang = 2.0 * np.pi * ((n[:, None] * k[None, :]) % L) / L
    half = np.where(n % 2 == 0, 1.0, -1.0)
    forward = np.concatenate([np.cos(ang), -np.sin(ang)], axis=1)
    forward[:, 64] = half
    weight = np.full((1, 64), 2.0)
    weight[0, 0] = 1.0
    inverse = np.concatenate([weight * np.cos(ang), -weight * np.sin(ang)], axis=1) / L
    inverse[:, 64] = half / L
    theta = 2.0 * np.pi * k / L
    shift = np.concatenate([1.0 - np.cos(theta)] * 2)
    shift[64] = 2.0
    sine = np.concatenate([np.sin(theta), -np.sin(theta)])
    sine[0] = sine[64] = 0.0
    order = np.array([8 * d + 2 * tp + t2 for t2 in range(2) for d in range(TM) for tp in range(4)])
    lanes = np.zeros((8, L))
    lanes[0] = shift
    lanes[1] = sine
    padded = np.zeros((2, TM, TILES, L))
    padded[:, :, :4] = inverse[order].reshape(2, TM, 4, L)
    as32 = lambda a: np.asarray(a, np.float32)
    return two_parts(forward[order]), two_parts(padded.reshape(-1, L)), as32(inverse), as32(lanes)


FORWARD, INVERSE, NATURAL, LANES = tables()


def vmem(count):
    return [pl.BlockSpec(memory_space=pltpu.VMEM)] * count


def smem(count):
    return [pl.BlockSpec(memory_space=pltpu.SMEM)] * count


def shape(*dims):
    return jax.ShapeDtypeStruct(dims, jnp.float32)


def dot(a, table, dims, table_first=False):
    value = a.astype(jnp.bfloat16)
    rest = (a - value.astype(jnp.float32)).astype(jnp.bfloat16)
    total = None
    for x, t in ((rest, table[0]), (value, table[1]), (value, table[0])):
        pair = (t, x) if table_first else (x, t)
        term = lax.dot_general(*pair, (dims, ((), ())), preferred_element_type=jnp.float32)
        total = term if total is None else total + term
    return total


def lane_index(rows):
    return lax.broadcasted_iota(jnp.int32, (rows, L), 1)


def halves(low, high):
    first = lane_index(low.shape[0]) < 64
    return (
        jnp.where(first, low, pltpu.roll(high, 64, 1)),
        jnp.where(first, pltpu.roll(low, 64, 1), high),
    )


def x_major(rows):
    return jnp.swapaxes(rows.reshape(8, 8, L), 0, 1).reshape(64, L)


def pack_kernel(rates, field, regime, out, rate_rows, sums):
    margin = jnp.zeros((8, L), jnp.float32)
    for tp in range(4):
        rows = [x_major(field[64 * t : 64 * t + 64, :]) for t in (2 * tp, 2 * tp + 1)]
        turned = jnp.concatenate(rows, axis=0).T
        starts = (
            jnp.concatenate([turned, margin], axis=0),
            jnp.concatenate([margin[:WY], turned, margin[WY:]], axis=0),
        )
        for d in range(TM):
            s = strip_of(d)
            out[d, ROWS * tp : ROWS * (tp + 1)] = starts[s % 2][8 * s : 8 * s + ROWS]
    kind = regime[...]
    c = jnp.zeros((64, L), jnp.float32)
    for r in range(8):
        c = c + jnp.where(kind == r, rates[r], 0.0)
    c_turned = jnp.concatenate([x_major(c), jnp.zeros((64, L), jnp.float32)], axis=0).T
    rate_rows[...] = jnp.concatenate([margin, c_turned, margin], axis=0)
    group = lane_index(1) // 32
    row = jnp.zeros((1, L), jnp.float32)
    for g in range(4):
        total = jnp.sum(c_turned[32 * g : 32 * g + 32], axis=0, keepdims=True)
        row = jnp.where(group == g, jnp.sum(total, axis=1, keepdims=True), row)
    sums[...] = jnp.broadcast_to(row, (8, L))


def own_strip():
    tm = lax.axis_index("tm")
    ends = jnp.where(tm == 0, 0, TM - 1)
    even = jnp.where(tm <= 2, ends, (tm >> 1) - 1)
    return jnp.where(tm & 1 == 1, 7 + (tm >> 1), even)


def transform_kernel(received, rate_rows, table, window, rate, swap):
    rows = []
    for pair in range(ROWS // 2):
        both = [received[pl.ds(2 * pair + j, 64, stride=ROWS), :] for j in range(2)]
        turned = jnp.concatenate(both, axis=0).T
        rows += list(halves(turned[:64], turned[64:]))
    spectrum = dot(jnp.concatenate(rows[: 8 + WY], axis=0), table, ((1,), (0,)))
    strip = own_strip()
    even = strip & 1 == 0
    zero = jnp.zeros((8, L), jnp.float32)
    for i in range(8 * WY):
        window[i] = zero
        window[8 * (WY + 8) + i] = zero
    offset = jnp.where(even, 8 * WY, 0)
    for i in range(8 * (8 + WY)):
        window[offset + i] = spectrum[8 * i : 8 * i + 8]
    near = rate_rows[pl.ds(pl.multiple_of(strip * 8, 8), 24), :]
    mine = jnp.concatenate([near[8 - WY : 16 + WY], jnp.zeros((2, L), jnp.float32)], axis=0)
    rate[...] = mine
    for i in range(8 * WY):
        swap[i] = jnp.where(even, window[8 * WY + i], window[64 + i])
    swap[PART - 1] = jnp.where(even, pltpu.roll(mine[0:8], 8 - WY, 0), mine[8:16])


def x_range(distance):
    return range(distance - 1, SPAN_Y + 1 - distance)


EDGE = [(d, y) for d in range(1, WX + 1) for y in x_range(d)]


def completed(window, rate, swapped):
    strip = own_strip()
    even = jnp.where(strip & 1 == 0, 1.0, 0.0)
    odd = 1.0 - even

    def tile(y, x):
        if y < WY:
            return window[8 * y + x] + even * swapped[8 * y + x]
        if y < WY + 8:
            return window[8 * y + x]
        return window[8 * y + x] + odd * swapped[8 * (y - WY - 8) + x]

    first = jnp.where(strip == 0, 1.0, 0.0)
    last = jnp.where(strip == TM - 1, 1.0, 0.0)
    row = lax.broadcasted_iota(jnp.int32, (8, L), 0)
    other = jnp.where(row < WY, swapped[PART - 1], 0.0)
    low = rate[0:8, :] + first * other
    high = rate[8:16, :] + last * pltpu.roll(other, WY, 0)
    return tile, (low, high)


def edge_kernel(window, rate, swapped, to_left, to_right):
    tile, rates = completed(window, rate, swapped)
    for i, (d, y) in enumerate(EDGE):
        to_left[i] = tile(y, d - 1)
        to_right[i] = tile(y, 8 - d)
    for j, c in enumerate(rates):
        to_left[len(EDGE) + j] = c
        to_right[len(EDGE) + j] = c


def inside():
    sx, sy, strip = lax.axis_index("sx"), lax.axis_index("sy"), own_strip()
    return [
        jnp.where(ok, 1.0, 0.0)
        for ok in (
            sx > 0,
            sx < SX - 1,
            (sy > 0) | (strip > 0),
            (sy < SY - 1) | (strip < TM - 1),
        )
    ]


def cell_terms(c, lanes):
    d = c + lanes[0:1, :] + 6.0
    sine = lanes[1:2, :]
    inverse = 1.0 / (d * d + sine * sine)
    return d * inverse, sine * inverse


def prepare_kernel(window, rate, swapped, lanes, source, a, b, first):
    tile, rates = completed(window, rate, swapped)
    valid = inside()
    rows = jnp.concatenate([*rates, jnp.zeros((112, L), jnp.float32)], axis=0)
    turned = rows.T
    for y in range(SPAN_Y):
        for x in range(8):
            c = jnp.broadcast_to(turned[8 * x : 8 * x + 8, y : y + 1], (8, L))
            ax, bx = cell_terms(c, lanes)
            if not WY <= y < WY + 8:
                ok = valid[2] if y < WY else valid[3]
                ax, bx = ax * ok, bx * ok
            s = tile(y, x)
            source[y, x] = s
            a[y, x] = ax
            b[y, x] = bx
            first[y, x] = ax * s + bx * pltpu.roll(s, 64, 1)


def solve_kernel(
    own_s, own_a, own_b, own_x, left, right, sums, lanes, table, out, hs, ha, hb, hx, x0, x1
):
    strip = own_strip()
    valid = inside()
    zero = jnp.zeros((8, L), jnp.float32)

    for y in range(SPAN_Y):
        for h in range(8):
            hs[y, h] = zero
    for i, (d, y) in enumerate(EDGE):
        hs[y, WX - d] = left[i]
        hs[y, WX - 1 + d] = right[i]
    lane = lane_index(8)
    rows = []
    for j in range(2):
        n = len(EDGE) + j
        rows.append(jnp.where(lane < 32, pltpu.roll(left[n], 96, 1), pltpu.roll(right[n], 32, 1)))
    rows.append(jnp.zeros((112, L), jnp.float32))
    turned = jnp.concatenate(rows, axis=0).T
    for y in range(SPAN_Y):
        for h in range(8):
            distance = WX - h if h < WX else h - WX + 1
            if y not in x_range(distance):
                ha[y, h] = zero
                hb[y, h] = zero
                hx[y, h] = zero
                continue
            c = jnp.broadcast_to(turned[8 * h : 8 * h + 8, y : y + 1], (8, L))
            ax, bx = cell_terms(c, lanes)
            ok = valid[0] if h < WX else valid[1]
            if y < WY:
                ok = ok * valid[2]
            elif y >= WY + 8:
                ok = ok * valid[3]
            ax, bx = ax * ok, bx * ok
            s = hs[y, h]
            ha[y, h] = ax
            hb[y, h] = bx
            hx[y, h] = ax * s + bx * pltpu.roll(s, 64, 1)

    def split(own, halo):
        def get(y, x):
            if x < WX:
                return halo[y, x]
            if x < WX + 8:
                return own[y, x - WX]
            return halo[y, x - 8]

        return get

    source, a, b = split(own_s, hs), split(own_a, ha), split(own_b, hb)

    def whole(ref):
        return lambda y, x: ref[y, x]

    def sweep(old, new, margin):
        for y in range(margin, SPAN_Y - margin):
            for x in range(margin, SPAN_X - margin):
                distance = max(WX - x, x - WX - 7, 1)
                if not distance - 1 + margin <= y < SPAN_Y + 1 - margin - distance:
                    continue
                v = old(y, x)
                u = source(y, x) + (old(y, x + 1) + old(y, x - 1))
                u = u + (old(y + 1, x) + old(y - 1, x))
                u = u + (pltpu.roll(v, 1, 0) + pltpu.roll(v, 7, 0))
                new[y, x] = a(y, x) * u + b(y, x) * pltpu.roll(u, 64, 1)

    sweep(split(own_x, hx), x1, 1)
    sweep(whole(x1), x0, 2)
    sweep(whole(x0), x1, 3)
    lo, hi = WX, WX + 8

    def change(y, x):
        return x1[y, x] - x0[y, x]

    acc = zero
    faces = []
    for y in range(WY, WY + 8):
        line = zero
        for x in range(lo, hi):
            line = line + change(y, x)
        end = y in (WY, WY + 7)
        acc = acc + (5.0 if end else 6.0) * line
        acc = acc + (change(y, lo - 1) - change(y, lo)) + (change(y, hi) - change(y, hi - 1))
        if end:
            faces.append(line)
    solved = x1[WY : WY + 8, lo:hi].reshape(512, L)
    result = dot(solved, table, ((1,), (1,)), table_first=True)
    by_y = []
    for pair in range(4):
        cut = result[:, 128 * pair : 128 * pair + 128]
        by_y += list(halves(cut[: TM * TILES], cut[TM * TILES :]))
    out[...] = jnp.swapaxes(jnp.stack(by_y), 0, 1).reshape(TM * TILES * 8, L)
    homes = (
        strip >> 2,
        jnp.where(strip == 0, 4, (strip - 1) >> 2),
        jnp.where(strip == TM - 1, 5, (strip + 1) >> 2),
    )
    index = lax.broadcasted_iota(jnp.int32, (8, L), 0)
    share = jnp.where((index == 6) & (strip == 0), sums[...], 0.0)
    for home, v in zip(homes, (acc, *faces)):
        v = jnp.broadcast_to(jnp.sum(v, axis=0, keepdims=True), (8, L))
        share = share + jnp.where(index == home, v, 0.0)
    for d in range(TM):
        out[8 * (TILES * d + 4) : 8 * (TILES * d + 5), :] = share


def gather_kernel(received, out):
    block = received[0, 4]
    for d in range(1, TM):
        block = block + received[d, 4]
    for j in range(SX * SY):
        out[j] = block


def inverse_of(rows):
    rows = list(rows)
    index = lax.broadcasted_iota(jnp.int32, (8, L), 0)
    for p in range(8):
        here = index == p
        pivot = jnp.broadcast_to(rows[p][p : p + 1], (8, L))
        scale = 1.0 / pivot
        lead = jnp.where(here, scale, rows[p] * scale)
        for r in range(8):
            if r != p:
                factor = jnp.broadcast_to(rows[r][p : p + 1], (8, L))
                rows[r] = jnp.where(here, 0.0, rows[r]) - factor * lead
        rows[p] = lead
    return rows


def apply(rows, v):
    terms = [rows[c] * jnp.broadcast_to(v[c : c + 1], (8, L)) for c in range(8)]
    while len(terms) > 1:
        terms = [terms[i] + terms[i + 1] for i in range(0, len(terms), 2)]
    return terms[0]


def coarse_kernel(gathered, received, lanes, table, out, answer):
    index = lax.broadcasted_iota(jnp.int32, (8, L), 0)
    shift = jnp.broadcast_to(lanes[0:1, :] * float(VOLUME) + float(FACES), (8, L))

    by_row = [jnp.swapaxes(gathered[:, sy], 0, 1) for sy in range(SY)]

    def rows_of(sy, row):
        return by_row[sy][row]

    def right(m):
        sy, g = m // 4, m % 4
        rhs = rows_of(sy, g)
        if g == 0 and sy > 0:
            rhs = rhs + rows_of(sy - 1, 5)
        if g == 3 and sy < SY - 1:
            rhs = rhs + rows_of(sy + 1, 4)
        return rhs

    sums = [rows_of(sy, 6) for sy in range(SY)]

    def block(m, before):
        g = 32 * (m % 4)
        diagonal = jnp.broadcast_to(sums[m // 4][:, g : g + 1], (8, L)) + shift
        rows = []
        for r in range(8):
            row = jnp.where(index == r, diagonal, 0.0)
            row = jnp.where((index == r - 1) | (index == r + 1), -COUPLE_X, row)
            for other in before:
                row = row - (COUPLE_Y * COUPLE_Y) * other[r]
            rows.append(row)
        return rows

    inv, part = {}, {}

    def eliminate(m, sources):
        matrix = inverse_of(block(m, [inv[q] for q in sources]))
        rhs = right(m)
        for q in sources:
            rhs = rhs + COUPLE_Y * part[q]
        inv[m] = matrix
        part[m] = apply(matrix, rhs)

    for i in range(8):
        if i < 7:
            eliminate(i, [i - 1] if i else [])
        eliminate(15 - i, [16 - i] if i else [])
    eliminate(7, [6, 8])
    solved = {7: part[7]}
    for i in range(1, 9):
        for m, q in ((7 - i, 8 - i), (7 + i, 6 + i)):
            if 0 <= m < 16:
                solved[m] = part[m] + COUPLE_Y * apply(inv[m], solved[q])
    for m in range(16):
        answer[8 * m : 8 * m + 8, :] = solved[m]
    sx, sy = lax.axis_index("sx"), lax.axis_index("sy")
    own = table[pl.ds(pl.multiple_of(lax.axis_index("tm") * 8, 8), 8), :]
    group = lane_index(8) // 32
    added = jnp.zeros((8, L), jnp.float32)
    for g in range(4):
        y = answer[pl.ds((sy * 4 + g) * 8 + sx, 1), :]
        value = jnp.sum(own * y, axis=1, keepdims=True)
        added = jnp.where(group == g, value, added)
    for tp in range(4):
        rows = [received[MEMBER[s], tp] for s in range(TM)]
        turned = jnp.concatenate(rows, axis=0).T
        for t2 in range(2):
            t = 2 * tp + t2
            out[64 * t : 64 * t + 64, :] = x_major(turned[64 * t2 : 64 * t2 + 64]) + added[t : t + 1, :]


def call(kernel, name, out_shape, arrays, scratch=(), rates=None, keep=True, flops=0):
    if keep:
        out_shape = jax.tree.map(lambda o: pltpu.VMEM(o.shape, o.dtype), out_shape)
    if rates is None:
        arrays = [pltpu.with_memory_space_constraint(x, pltpu.VMEM) for x in arrays]
    scalars = [] if rates is None else [rates]
    limit = 24 * 2**20 if rates is None else None
    many = isinstance(out_shape, tuple)
    return pl.pallas_call(
        kernel,
        name=name,
        out_shape=out_shape,
        in_specs=smem(len(scalars)) + vmem(len(arrays)),
        out_specs=tuple(vmem(len(out_shape))) if many else vmem(1)[0],
        scratch_shapes=list(scratch),
        compiler_params=pltpu.CompilerParams(vmem_limit_bytes=limit),
        cost_estimate=pl.CostEstimate(flops=flops, transcendentals=0, bytes_accessed=0),
    )(*scalars, *arrays)


def swaps():
    def rank(g):
        return MEMBER[g % TM] * SY + g // TM

    pairs = [(rank(g), rank(g + 1)) for g in range(1, SY * TM - 1, 2)]
    return pairs + [(q, p) for p, q in pairs]


def local(driving_input, regime, reaction_rates):
    forward, inverse, natural, lanes = (jnp.asarray(t) for t in (FORWARD, INVERSE, NATURAL, LANES))
    packed, rate_rows, sums = call(
        pack_kernel,
        "pack",
        (shape(TM, 4 * ROWS, L), shape(L + 16, L), shape(8, L)),
        [driving_input.reshape(512, L), regime.reshape(64, L)],
        rates=reaction_rates,
    )
    received = lax.all_to_all(packed, "tm", split_axis=0, concat_axis=0, tiled=True)
    window, rate, swap = call(
        transform_kernel,
        "transform",
        (shape(8 * SPAN_Y, 8, L), shape(16, L), shape(PART, 8, L)),
        [received.reshape(TM * 4 * ROWS, L), rate_rows, forward],
    )
    swapped = lax.ppermute(swap, ("tm", "sy"), swaps())
    tiles = len(EDGE) + 2
    to_left, to_right = call(
        edge_kernel, "edges", (shape(tiles, 8, L),) * 2, [window, rate, swapped]
    )
    across = [(i, i + 1) for i in range(SX - 1)]
    left = lax.ppermute(to_right, "sx", across)
    right = lax.ppermute(to_left, "sx", [(q, p) for p, q in across])
    prepared = call(
        prepare_kernel,
        "prepare",
        (shape(SPAN_Y, 8, 8, L),) * 4,
        [window, rate, swapped, lanes],
        flops=10**7,
    )
    half = pltpu.VMEM((SPAN_Y, 8, 8, L), jnp.float32)
    message = call(
        solve_kernel,
        "sweeps",
        shape(TM * TILES * 8, L),
        [*prepared, left, right, sums, lanes, inverse],
        [half] * 4 + [pltpu.VMEM((SPAN_Y, SPAN_X, 8, L), jnp.float32)] * 2,
    )
    returned = lax.all_to_all(
        message.reshape(TM, TILES, 8, L), "tm", split_axis=0, concat_axis=0, tiled=True
    )
    shared = call(gather_kernel, "gather", shape(SX * SY, 8, L), [returned])
    gathered = lax.all_to_all(shared, ("sx", "sy"), split_axis=0, concat_axis=0, tiled=True)
    result = call(
        coarse_kernel,
        "coarse",
        shape(512, L),
        [gathered.reshape(SX, SY, 8, L), returned, lanes, natural],
        [pltpu.VMEM((L, L), jnp.float32)],
        keep=False,
    )
    return result.reshape(driving_input.shape)


def solution(mesh):
    placed = (P("tm", None, "sx", "sy"), P(None, "sx", "sy"), P())
    return jax.shard_map(
        local, mesh=mesh, in_specs=placed, out_specs=P("tm", None, "sx", "sy"), check_vma=False
    )
```

```python
import jax
import jax.numpy as jnp
import numpy as np
from jax import lax
from jax.experimental import pallas as pl
from jax.experimental.pallas import tpu as pltpu
from jax.sharding import PartitionSpec as P

L = 128
NZ = 8
BLOCK = 8
WY = 3
WX = 4
SPAN_Y = BLOCK + 2 * WY
SPAN_X = BLOCK + 2 * WX
ROWS = 12
PART = 8 * WY + 1
TM, SX, SY = 16, 8, 4
FACES = 2 * (32 * NZ + 8 * NZ)
VOLUME = 8 * 32 * NZ
COUPLE_X = 32.0 * NZ
COUPLE_Y = 8.0 * NZ
TILES = 5


def strip_of(d):
    return d // 2 if d % 2 == 0 else TM - 1 - d // 2


MEMBER = {strip_of(d): d for d in range(TM)}


def two_parts(table):
    value = np.asarray(table, jnp.bfloat16)
    rest = np.asarray(table - np.asarray(value, np.float64), jnp.bfloat16)
    return np.stack([value, rest])


def tables():
    n = np.arange(L)
    k = np.arange(64)
    ang = 2.0 * np.pi * ((n[:, None] * k[None, :]) % L) / L
    half = np.where(n % 2 == 0, 1.0, -1.0)
    forward = np.concatenate([np.cos(ang), -np.sin(ang)], axis=1)
    forward[:, 64] = half
    weight = np.full((1, 64), 2.0)
    weight[0, 0] = 1.0
    inverse = np.concatenate([weight * np.cos(ang), -weight * np.sin(ang)], axis=1) / L
    inverse[:, 64] = half / L
    theta = 2.0 * np.pi * k / L
    shift = np.concatenate([1.0 - np.cos(theta)] * 2)
    shift[64] = 2.0
    sine = np.concatenate([np.sin(theta), -np.sin(theta)])
    sine[0] = sine[64] = 0.0
    order = np.array([8 * d + 2 * tp + t2 for t2 in range(2) for d in range(TM) for tp in range(4)])
    lanes = np.zeros((8, L))
    lanes[0] = shift
    lanes[1] = sine
    padded = np.zeros((2, TM, TILES, L))
    padded[:, :, :4] = inverse[order].reshape(2, TM, 4, L)
    as32 = lambda a: np.asarray(a, np.float32)
    return two_parts(forward[order]), two_parts(padded.reshape(-1, L)), as32(inverse), as32(lanes)


FORWARD, INVERSE, NATURAL, LANES = tables()


def vmem(count):
    return [pl.BlockSpec(memory_space=pltpu.VMEM)] * count


def smem(count):
    return [pl.BlockSpec(memory_space=pltpu.SMEM)] * count


def shape(*dims):
    return jax.ShapeDtypeStruct(dims, jnp.float32)


def dot(a, table, dims, table_first=False):
    value = a.astype(jnp.bfloat16)
    rest = (a - value.astype(jnp.float32)).astype(jnp.bfloat16)
    total = None
    for x, t in ((rest, table[0]), (value, table[1]), (value, table[0])):
        pair = (t, x) if table_first else (x, t)
        term = lax.dot_general(*pair, (dims, ((), ())), preferred_element_type=jnp.float32)
        total = term if total is None else total + term
    return total


def lane_index(rows):
    return lax.broadcasted_iota(jnp.int32, (rows, L), 1)


def halves(low, high):
    first = lane_index(low.shape[0]) < 64
    return (
        jnp.where(first, low, pltpu.roll(high, 64, 1)),
        jnp.where(first, pltpu.roll(low, 64, 1), high),
    )


def x_major(rows):
    return jnp.swapaxes(rows.reshape(8, 8, L), 0, 1).reshape(64, L)


def pack_kernel(rates, field, regime, out, rate_rows, sums):
    margin = jnp.zeros((8, L), jnp.float32)
    for tp in range(4):
        rows = [x_major(field[64 * t : 64 * t + 64, :]) for t in (2 * tp, 2 * tp + 1)]
        turned = jnp.concatenate(rows, axis=0).T
        starts = (
            jnp.concatenate([turned, margin], axis=0),
            jnp.concatenate([margin[:WY], turned, margin[WY:]], axis=0),
        )
        for d in range(TM):
            s = strip_of(d)
            out[d, ROWS * tp : ROWS * (tp + 1)] = starts[s % 2][8 * s : 8 * s + ROWS]
    kind = regime[...]
    c = jnp.zeros((64, L), jnp.float32)
    for r in range(8):
        c = c + jnp.where(kind == r, rates[r], 0.0)
    c_turned = jnp.concatenate([x_major(c), jnp.zeros((64, L), jnp.float32)], axis=0).T
    rate_rows[...] = jnp.concatenate([margin, c_turned, margin], axis=0)
    group = lane_index(1) // 32
    row = jnp.zeros((1, L), jnp.float32)
    for g in range(4):
        total = jnp.sum(c_turned[32 * g : 32 * g + 32], axis=0, keepdims=True)
        row = jnp.where(group == g, jnp.sum(total, axis=1, keepdims=True), row)
    sums[...] = jnp.broadcast_to(row, (8, L))


def own_strip():
    tm = lax.axis_index("tm")
    return jnp.where(tm & 1 == 0, tm >> 1, TM - 1 - (tm >> 1))


def spectra(received, table, starts):
    rows = []
    for first, second in zip(starts[::2], starts[1::2]):
        both = [received[pl.ds(start, 64, stride=ROWS), :] for start in (first, second)]
        turned = jnp.concatenate(both, axis=0).T
        rows += list(halves(turned[:64], turned[64:]))
    return dot(jnp.concatenate(rows, axis=0), table, ((1,), (0,)))


def window_rates(rate_rows):
    near = rate_rows[pl.ds(pl.multiple_of(own_strip() * 8, 8), 24), :]
    return jnp.concatenate([near[8 - WY : 16 + WY], jnp.zeros((2, L), jnp.float32)], axis=0)


def swap_kernel(received, rate_rows, table, swap):
    even = own_strip() & 1 == 0
    start = jnp.where(even, 0, 8)
    spectrum = spectra(received, table, [start, start + 1, start + 2, start + 2])
    for i in range(8 * WY):
        swap[i] = spectrum[8 * i : 8 * i + 8]
    mine = window_rates(rate_rows)
    swap[PART - 1] = jnp.where(even, pltpu.roll(mine[0:8], 8 - WY, 0), mine[8:16])


def transform_kernel(received, rate_rows, table, window, rate):
    spectrum = spectra(received, table, range(ROWS))
    zero = jnp.zeros((8, L), jnp.float32)
    for i in range(8 * WY):
        window[i] = zero
        window[8 * (WY + 8) + i] = zero
    offset = jnp.where(own_strip() & 1 == 0, 8 * WY, 0)
    for i in range(8 * (8 + WY)):
        window[offset + i] = spectrum[8 * i : 8 * i + 8]
    rate[...] = window_rates(rate_rows)


def x_range(distance):
    return range(distance - 1, SPAN_Y + 1 - distance)


EDGE = [(d, y) for d in range(1, WX + 1) for y in x_range(d)]


def completed(window, rate, swapped):
    strip = own_strip()
    even = jnp.where(strip & 1 == 0, 1.0, 0.0)
    odd = 1.0 - even

    def tile(y, x):
        if y < WY:
            return window[8 * y + x] + even * swapped[8 * y + x]
        if y < WY + 8:
            return window[8 * y + x]
        return window[8 * y + x] + odd * swapped[8 * (y - WY - 8) + x]

    first = jnp.where(strip == 0, 1.0, 0.0)
    last = jnp.where(strip == TM - 1, 1.0, 0.0)
    row = lax.broadcasted_iota(jnp.int32, (8, L), 0)
    other = jnp.where(row < WY, swapped[PART - 1], 0.0)
    low = rate[0:8, :] + first * other
    high = rate[8:16, :] + last * pltpu.roll(other, WY, 0)
    return tile, (low, high)


def edge_kernel(window, rate, swapped, to_left, to_right):
    tile, rates = completed(window, rate, swapped)
    for i, (d, y) in enumerate(EDGE):
        to_left[i] = tile(y, d - 1)
        to_right[i] = tile(y, 8 - d)
    for j, c in enumerate(rates):
        to_left[len(EDGE) + j] = c
        to_right[len(EDGE) + j] = c


def inside():
    sx, sy, strip = lax.axis_index("sx"), lax.axis_index("sy"), own_strip()
    return [
        jnp.where(ok, 1.0, 0.0)
        for ok in (
            sx > 0,
            sx < SX - 1,
            (sy > 0) | (strip > 0),
            (sy < SY - 1) | (strip < TM - 1),
        )
    ]


def cell_terms(c, lanes):
    d = c + lanes[0:1, :] + 6.0
    sine = lanes[1:2, :]
    inverse = 1.0 / (d * d + sine * sine)
    return d * inverse, sine * inverse


def prepare_kernel(window, rate, swapped, lanes, source, a, b, first):
    tile, rates = completed(window, rate, swapped)
    valid = inside()
    rows = jnp.concatenate([*rates, jnp.zeros((112, L), jnp.float32)], axis=0)
    turned = rows.T
    for y in range(SPAN_Y):
        for x in range(8):
            c = jnp.broadcast_to(turned[8 * x : 8 * x + 8, y : y + 1], (8, L))
            ax, bx = cell_terms(c, lanes)
            if not WY <= y < WY + 8:
                ok = valid[2] if y < WY else valid[3]
                ax, bx = ax * ok, bx * ok
            s = tile(y, x)
            source[y, x] = s
            a[y, x] = ax
            b[y, x] = bx
            first[y, x] = ax * s + bx * pltpu.roll(s, 64, 1)


def solve_kernel(
    own_s, own_a, own_b, own_x, left, right, sums, lanes, table, out, hs, ha, hb, hx, x0, x1
):
    strip = own_strip()
    valid = inside()
    zero = jnp.zeros((8, L), jnp.float32)

    for y in range(SPAN_Y):
        for h in range(8):
            hs[y, h] = zero
    for i, (d, y) in enumerate(EDGE):
        hs[y, WX - d] = left[i]
        hs[y, WX - 1 + d] = right[i]
    lane = lane_index(8)
    rows = []
    for j in range(2):
        n = len(EDGE) + j
        rows.append(jnp.where(lane < 32, pltpu.roll(left[n], 96, 1), pltpu.roll(right[n], 32, 1)))
    rows.append(jnp.zeros((112, L), jnp.float32))
    turned = jnp.concatenate(rows, axis=0).T
    for y in range(SPAN_Y):
        for h in range(8):
            distance = WX - h if h < WX else h - WX + 1
            if y not in x_range(distance):
                ha[y, h] = zero
                hb[y, h] = zero
                hx[y, h] = zero
                continue
            c = jnp.broadcast_to(turned[8 * h : 8 * h + 8, y : y + 1], (8, L))
            ax, bx = cell_terms(c, lanes)
            ok = valid[0] if h < WX else valid[1]
            if y < WY:
                ok = ok * valid[2]
            elif y >= WY + 8:
                ok = ok * valid[3]
            ax, bx = ax * ok, bx * ok
            s = hs[y, h]
            ha[y, h] = ax
            hb[y, h] = bx
            hx[y, h] = ax * s + bx * pltpu.roll(s, 64, 1)

    def split(own, halo):
        def get(y, x):
            if x < WX:
                return halo[y, x]
            if x < WX + 8:
                return own[y, x - WX]
            return halo[y, x - 8]

        return get

    source, a, b = split(own_s, hs), split(own_a, ha), split(own_b, hb)

    def whole(ref):
        return lambda y, x: ref[y, x]

    def sweep(old, new, margin):
        for y in range(margin, SPAN_Y - margin):
            for x in range(margin, SPAN_X - margin):
                distance = max(WX - x, x - WX - 7, 1)
                if not distance - 1 + margin <= y < SPAN_Y + 1 - margin - distance:
                    continue
                v = old(y, x)
                u = source(y, x) + (old(y, x + 1) + old(y, x - 1))
                u = u + (old(y + 1, x) + old(y - 1, x))
                u = u + (pltpu.roll(v, 1, 0) + pltpu.roll(v, 7, 0))
                new[y, x] = a(y, x) * u + b(y, x) * pltpu.roll(u, 64, 1)

    sweep(split(own_x, hx), x1, 1)
    sweep(whole(x1), x0, 2)
    sweep(whole(x0), x1, 3)
    lo, hi = WX, WX + 8

    def change(y, x):
        return x1[y, x] - x0[y, x]

    acc = zero
    faces = []
    for y in range(WY, WY + 8):
        line = zero
        for x in range(lo, hi):
            line = line + change(y, x)
        end = y in (WY, WY + 7)
        acc = acc + (5.0 if end else 6.0) * line
        acc = acc + (change(y, lo - 1) - change(y, lo)) + (change(y, hi) - change(y, hi - 1))
        if end:
            faces.append(line)
    solved = x1[WY : WY + 8, lo:hi].reshape(512, L)
    result = dot(solved, table, ((1,), (1,)), table_first=True)
    by_y = []
    for pair in range(4):
        cut = result[:, 128 * pair : 128 * pair + 128]
        by_y += list(halves(cut[: TM * TILES], cut[TM * TILES :]))
    out[...] = jnp.swapaxes(jnp.stack(by_y), 0, 1).reshape(TM * TILES * 8, L)
    homes = (
        strip >> 2,
        jnp.where(strip == 0, 4, (strip - 1) >> 2),
        jnp.where(strip == TM - 1, 5, (strip + 1) >> 2),
    )
    index = lax.broadcasted_iota(jnp.int32, (8, L), 0)
    share = jnp.where((index == 6) & (strip == 0), sums[...], 0.0)
    for home, v in zip(homes, (acc, *faces)):
        v = jnp.broadcast_to(jnp.sum(v, axis=0, keepdims=True), (8, L))
        share = share + jnp.where(index == home, v, 0.0)
    for d in range(TM):
        out[8 * (TILES * d + 4) : 8 * (TILES * d + 5), :] = share


def gather_kernel(received, out):
    block = received[0, 4]
    for d in range(1, TM):
        block = block + received[d, 4]
    for j in range(SX * SY):
        out[j] = block


def inverse_of(rows):
    rows = list(rows)
    index = lax.broadcasted_iota(jnp.int32, (8, L), 0)
    for p in range(8):
        here = index == p
        pivot = jnp.broadcast_to(rows[p][p : p + 1], (8, L))
        scale = 1.0 / pivot
        lead = jnp.where(here, scale, rows[p] * scale)
        for r in range(8):
            if r != p:
                factor = jnp.broadcast_to(rows[r][p : p + 1], (8, L))
                rows[r] = jnp.where(here, 0.0, rows[r]) - factor * lead
        rows[p] = lead
    return rows


def apply(rows, v):
    terms = [rows[c] * jnp.broadcast_to(v[c : c + 1], (8, L)) for c in range(8)]
    while len(terms) > 1:
        terms = [terms[i] + terms[i + 1] for i in range(0, len(terms), 2)]
    return terms[0]


def coarse_kernel(gathered, received, lanes, table, out, answer):
    index = lax.broadcasted_iota(jnp.int32, (8, L), 0)
    shift = jnp.broadcast_to(lanes[0:1, :] * float(VOLUME) + float(FACES), (8, L))

    by_row = [jnp.swapaxes(gathered[:, sy], 0, 1) for sy in range(SY)]

    def rows_of(sy, row):
        return by_row[sy][row]

    def right(m):
        sy, g = m // 4, m % 4
        rhs = rows_of(sy, g)
        if g == 0 and sy > 0:
            rhs = rhs + rows_of(sy - 1, 5)
        if g == 3 and sy < SY - 1:
            rhs = rhs + rows_of(sy + 1, 4)
        return rhs

    sums = [rows_of(sy, 6) for sy in range(SY)]

    def block(m, before):
        g = 32 * (m % 4)
        diagonal = jnp.broadcast_to(sums[m // 4][:, g : g + 1], (8, L)) + shift
        rows = []
        for r in range(8):
            row = jnp.where(index == r, diagonal, 0.0)
            row = jnp.where((index == r - 1) | (index == r + 1), -COUPLE_X, row)
            for other in before:
                row = row - (COUPLE_Y * COUPLE_Y) * other[r]
            rows.append(row)
        return rows

    inv, part = {}, {}

    def eliminate(m, sources):
        matrix = inverse_of(block(m, [inv[q] for q in sources]))
        rhs = right(m)
        for q in sources:
            rhs = rhs + COUPLE_Y * part[q]
        inv[m] = matrix
        part[m] = apply(matrix, rhs)

    for i in range(8):
        if i < 7:
            eliminate(i, [i - 1] if i else [])
        eliminate(15 - i, [16 - i] if i else [])
    eliminate(7, [6, 8])
    solved = {7: part[7]}
    for i in range(1, 9):
        for m, q in ((7 - i, 8 - i), (7 + i, 6 + i)):
            if 0 <= m < 16:
                solved[m] = part[m] + COUPLE_Y * apply(inv[m], solved[q])
    for m in range(16):
        answer[8 * m : 8 * m + 8, :] = solved[m]
    sx, sy = lax.axis_index("sx"), lax.axis_index("sy")
    own = table[pl.ds(pl.multiple_of(lax.axis_index("tm") * 8, 8), 8), :]
    group = lane_index(8) // 32
    added = jnp.zeros((8, L), jnp.float32)
    for g in range(4):
        y = answer[pl.ds((sy * 4 + g) * 8 + sx, 1), :]
        value = jnp.sum(own * y, axis=1, keepdims=True)
        added = jnp.where(group == g, value, added)
    for tp in range(4):
        rows = [received[MEMBER[s], tp] for s in range(TM)]
        turned = jnp.concatenate(rows, axis=0).T
        for t2 in range(2):
            t = 2 * tp + t2
            out[64 * t : 64 * t + 64, :] = x_major(turned[64 * t2 : 64 * t2 + 64]) + added[t : t + 1, :]


def call(kernel, name, out_shape, arrays, scratch=(), rates=None, keep=True, flops=0):
    if keep:
        out_shape = jax.tree.map(lambda o: pltpu.VMEM(o.shape, o.dtype), out_shape)
    if rates is None:
        arrays = [pltpu.with_memory_space_constraint(x, pltpu.VMEM) for x in arrays]
    scalars = [] if rates is None else [rates]
    limit = 24 * 2**20 if rates is None else None
    many = isinstance(out_shape, tuple)
    return pl.pallas_call(
        kernel,
        name=name,
        out_shape=out_shape,
        in_specs=smem(len(scalars)) + vmem(len(arrays)),
        out_specs=tuple(vmem(len(out_shape))) if many else vmem(1)[0],
        scratch_shapes=list(scratch),
        compiler_params=pltpu.CompilerParams(vmem_limit_bytes=limit),
        cost_estimate=pl.CostEstimate(flops=flops, transcendentals=0, bytes_accessed=0),
    )(*scalars, *arrays)


def swaps():
    def rank(g):
        return MEMBER[g % TM] * SY + g // TM

    pairs = [(rank(g), rank(g + 1)) for g in range(1, SY * TM - 1, 2)]
    return pairs + [(q, p) for p, q in pairs]


def local(driving_input, regime, reaction_rates):
    forward, inverse, natural, lanes = (jnp.asarray(t) for t in (FORWARD, INVERSE, NATURAL, LANES))
    packed, rate_rows, sums = call(
        pack_kernel,
        "pack",
        (shape(TM, 4 * ROWS, L), shape(L + 16, L), shape(8, L)),
        [driving_input.reshape(512, L), regime.reshape(64, L)],
        rates=reaction_rates,
    )
    received = lax.all_to_all(packed, "tm", split_axis=0, concat_axis=0, tiled=True)
    arrays = [received.reshape(TM * 4 * ROWS, L), rate_rows, forward]
    swap = call(swap_kernel, "swap_rows", shape(PART, 8, L), arrays)
    swapped = lax.ppermute(swap, ("tm", "sy"), swaps())
    window, rate = call(
        transform_kernel, "transform", (shape(8 * SPAN_Y, 8, L), shape(16, L)), arrays, flops=10**7
    )
    tiles = len(EDGE) + 2
    to_left, to_right = call(
        edge_kernel, "edges", (shape(tiles, 8, L),) * 2, [window, rate, swapped]
    )
    across = [(i, i + 1) for i in range(SX - 1)]
    left = lax.ppermute(to_right, "sx", across)
    right = lax.ppermute(to_left, "sx", [(q, p) for p, q in across])
    prepared = call(
        prepare_kernel,
        "prepare",
        (shape(SPAN_Y, 8, 8, L),) * 4,
        [window, rate, swapped, lanes],
        flops=10**7,
    )
    half = pltpu.VMEM((SPAN_Y, 8, 8, L), jnp.float32)
    message = call(
        solve_kernel,
        "sweeps",
        shape(TM * TILES * 8, L),
        [*prepared, left, right, sums, lanes, inverse],
        [half] * 4 + [pltpu.VMEM((SPAN_Y, SPAN_X, 8, L), jnp.float32)] * 2,
    )
    returned = lax.all_to_all(
        message.reshape(TM, TILES, 8, L), "tm", split_axis=0, concat_axis=0, tiled=True
    )
    shared = call(gather_kernel, "gather", shape(SX * SY, 8, L), [returned])
    gathered = lax.all_to_all(shared, ("sx", "sy"), split_axis=0, concat_axis=0, tiled=True)
    result = call(
        coarse_kernel,
        "coarse",
        shape(512, L),
        [gathered.reshape(SX, SY, 8, L), returned, lanes, natural],
        [pltpu.VMEM((L, L), jnp.float32)],
        keep=False,
    )
    return result.reshape(driving_input.shape)


def solution(mesh):
    placed = (P("tm", None, "sx", "sy"), P(None, "sx", "sy"), P())
    return jax.shard_map(
        local, mesh=mesh, in_specs=placed, out_specs=P("tm", None, "sx", "sy"), check_vma=False
    )
```

```python
import jax
import jax.numpy as jnp
import numpy as np
from jax import lax
from jax.experimental import pallas as pl
from jax.experimental.pallas import tpu as pltpu
from jax.sharding import PartitionSpec as P

L = 128
NZ = 8
BLOCK = 8
WY = 3
WX = 4
SPAN_Y = BLOCK + 2 * WY
SPAN_X = BLOCK + 2 * WX
ROWS = 12
PART = 8 * WY + 1
TM, SX, SY = 16, 8, 4
FACES = 2 * (32 * NZ + 8 * NZ)
VOLUME = 8 * 32 * NZ
COUPLE_X = 32.0 * NZ
COUPLE_Y = 8.0 * NZ
TILES = 5


def strip_of(d):
    if d % 2 == 1:
        return 7 + d // 2
    return {0: 0, 2: TM - 1}.get(d, d // 2 - 1)


MEMBER = {strip_of(d): d for d in range(TM)}


def two_parts(table):
    value = np.asarray(table, jnp.bfloat16)
    rest = np.asarray(table - np.asarray(value, np.float64), jnp.bfloat16)
    return np.stack([value, rest])


def tables():
    n = np.arange(L)
    k = np.arange(64)
    ang = 2.0 * np.pi * ((n[:, None] * k[None, :]) % L) / L
    half = np.where(n % 2 == 0, 1.0, -1.0)
    forward = np.concatenate([np.cos(ang), -np.sin(ang)], axis=1)
    forward[:, 64] = half
    weight = np.full((1, 64), 2.0)
    weight[0, 0] = 1.0
    inverse = np.concatenate([weight * np.cos(ang), -weight * np.sin(ang)], axis=1) / L
    inverse[:, 64] = half / L
    theta = 2.0 * np.pi * k / L
    shift = np.concatenate([1.0 - np.cos(theta)] * 2)
    shift[64] = 2.0
    sine = np.concatenate([np.sin(theta), -np.sin(theta)])
    sine[0] = sine[64] = 0.0
    order = np.array([8 * d + 2 * tp + t2 for t2 in range(2) for d in range(TM) for tp in range(4)])
    lanes = np.zeros((8, L))
    lanes[0] = shift
    lanes[1] = sine
    padded = np.zeros((2, TM, TILES, L))
    padded[:, :, :4] = inverse[order].reshape(2, TM, 4, L)
    as32 = lambda a: np.asarray(a, np.float32)
    return two_parts(forward[order]), two_parts(padded.reshape(-1, L)), as32(inverse), as32(lanes)


FORWARD, INVERSE, NATURAL, LANES = tables()


def vmem(count):
    return [pl.BlockSpec(memory_space=pltpu.VMEM)] * count


def smem(count):
    return [pl.BlockSpec(memory_space=pltpu.SMEM)] * count


def shape(*dims):
    return jax.ShapeDtypeStruct(dims, jnp.float32)


def dot(a, table, dims, table_first=False):
    value = a.astype(jnp.bfloat16)
    rest = (a - value.astype(jnp.float32)).astype(jnp.bfloat16)
    total = None
    for x, t in ((rest, table[0]), (value, table[1]), (value, table[0])):
        pair = (t, x) if table_first else (x, t)
        term = lax.dot_general(*pair, (dims, ((), ())), preferred_element_type=jnp.float32)
        total = term if total is None else total + term
    return total


def lane_index(rows):
    return lax.broadcasted_iota(jnp.int32, (rows, L), 1)


def halves(low, high):
    first = lane_index(low.shape[0]) < 64
    return (
        jnp.where(first, low, pltpu.roll(high, 64, 1)),
        jnp.where(first, pltpu.roll(low, 64, 1), high),
    )


def x_major(rows):
    return jnp.swapaxes(rows.reshape(8, 8, L), 0, 1).reshape(64, L)


def pack_kernel(rates, field, regime, out, rate_rows, sums):
    margin = jnp.zeros((8, L), jnp.float32)
    for tp in range(4):
        rows = [x_major(field[64 * t : 64 * t + 64, :]) for t in (2 * tp, 2 * tp + 1)]
        turned = jnp.concatenate(rows, axis=0).T
        starts = (
            jnp.concatenate([turned, margin], axis=0),
            jnp.concatenate([margin[:WY], turned, margin[WY:]], axis=0),
        )
        for d in range(TM):
            s = strip_of(d)
            out[d, ROWS * tp : ROWS * (tp + 1)] = starts[s % 2][8 * s : 8 * s + ROWS]
    kind = regime[...]
    c = jnp.zeros((64, L), jnp.float32)
    for r in range(8):
        c = c + jnp.where(kind == r, rates[r], 0.0)
    c_turned = jnp.concatenate([x_major(c), jnp.zeros((64, L), jnp.float32)], axis=0).T
    rate_rows[...] = jnp.concatenate([margin, c_turned, margin], axis=0)
    group = lane_index(1) // 32
    row = jnp.zeros((1, L), jnp.float32)
    for g in range(4):
        total = jnp.sum(c_turned[32 * g : 32 * g + 32], axis=0, keepdims=True)
        row = jnp.where(group == g, jnp.sum(total, axis=1, keepdims=True), row)
    sums[...] = jnp.broadcast_to(row, (8, L))


def own_strip():
    tm = lax.axis_index("tm")
    ends = jnp.where(tm == 0, 0, TM - 1)
    even = jnp.where(tm <= 2, ends, (tm >> 1) - 1)
    return jnp.where(tm & 1 == 1, 7 + (tm >> 1), even)


def spectra(received, table, starts):
    rows = []
    for first, second in zip(starts[::2], starts[1::2]):
        both = [received[pl.ds(start, 64, stride=ROWS), :] for start in (first, second)]
        turned = jnp.concatenate(both, axis=0).T
        rows += list(halves(turned[:64], turned[64:]))
    return dot(jnp.concatenate(rows, axis=0), table, ((1,), (0,)))


def window_rates(rate_rows):
    near = rate_rows[pl.ds(pl.multiple_of(own_strip() * 8, 8), 24), :]
    return jnp.concatenate([near[8 - WY : 16 + WY], jnp.zeros((2, L), jnp.float32)], axis=0)


def swap_kernel(received, rate_rows, table, swap):
    even = own_strip() & 1 == 0
    start = jnp.where(even, 0, 8)
    spectrum = spectra(received, table, [start, start + 1, start + 2, start + 2])
    for i in range(8 * WY):
        swap[i] = spectrum[8 * i : 8 * i + 8]
    mine = window_rates(rate_rows)
    swap[PART - 1] = jnp.where(even, pltpu.roll(mine[0:8], 8 - WY, 0), mine[8:16])


def transform_kernel(received, rate_rows, table, window, rate):
    spectrum = spectra(received, table, range(ROWS))
    zero = jnp.zeros((8, L), jnp.float32)
    for i in range(8 * WY):
        window[i] = zero
        window[8 * (WY + 8) + i] = zero
    offset = jnp.where(own_strip() & 1 == 0, 8 * WY, 0)
    for i in range(8 * (8 + WY)):
        window[offset + i] = spectrum[8 * i : 8 * i + 8]
    rate[...] = window_rates(rate_rows)


def x_range(distance):
    return range(distance - 1, SPAN_Y + 1 - distance)


EDGE = [(d, y) for d in range(1, WX + 1) for y in x_range(d)]


def completed(window, rate, swapped):
    strip = own_strip()
    even = jnp.where(strip & 1 == 0, 1.0, 0.0)
    odd = 1.0 - even

    def tile(y, x):
        if y < WY:
            return window[8 * y + x] + even * swapped[8 * y + x]
        if y < WY + 8:
            return window[8 * y + x]
        return window[8 * y + x] + odd * swapped[8 * (y - WY - 8) + x]

    first = jnp.where(strip == 0, 1.0, 0.0)
    last = jnp.where(strip == TM - 1, 1.0, 0.0)
    row = lax.broadcasted_iota(jnp.int32, (8, L), 0)
    other = jnp.where(row < WY, swapped[PART - 1], 0.0)
    low = rate[0:8, :] + first * other
    high = rate[8:16, :] + last * pltpu.roll(other, WY, 0)
    return tile, (low, high)


def edge_kernel(window, rate, swapped, to_left, to_right):
    tile, rates = completed(window, rate, swapped)
    for i, (d, y) in enumerate(EDGE):
        to_left[i] = tile(y, d - 1)
        to_right[i] = tile(y, 8 - d)
    for j, c in enumerate(rates):
        to_left[len(EDGE) + j] = c
        to_right[len(EDGE) + j] = c


def inside():
    sx, sy, strip = lax.axis_index("sx"), lax.axis_index("sy"), own_strip()
    return [
        jnp.where(ok, 1.0, 0.0)
        for ok in (
            sx > 0,
            sx < SX - 1,
            (sy > 0) | (strip > 0),
            (sy < SY - 1) | (strip < TM - 1),
        )
    ]


def cell_terms(c, lanes):
    d = c + lanes[0:1, :] + 6.0
    sine = lanes[1:2, :]
    inverse = 1.0 / (d * d + sine * sine)
    return d * inverse, sine * inverse


def prepare_kernel(window, rate, swapped, lanes, source, a, b, first):
    tile, rates = completed(window, rate, swapped)
    valid = inside()
    rows = jnp.concatenate([*rates, jnp.zeros((112, L), jnp.float32)], axis=0)
    turned = rows.T
    for y in range(SPAN_Y):
        for x in range(8):
            c = jnp.broadcast_to(turned[8 * x : 8 * x + 8, y : y + 1], (8, L))
            ax, bx = cell_terms(c, lanes)
            if not WY <= y < WY + 8:
                ok = valid[2] if y < WY else valid[3]
                ax, bx = ax * ok, bx * ok
            s = tile(y, x)
            source[y, x] = s
            a[y, x] = ax
            b[y, x] = bx
            first[y, x] = ax * s + bx * pltpu.roll(s, 64, 1)


def solve_kernel(
    own_s, own_a, own_b, own_x, left, right, sums, lanes, table, out, hs, ha, hb, hx, x0, x1
):
    strip = own_strip()
    valid = inside()
    zero = jnp.zeros((8, L), jnp.float32)

    for y in range(SPAN_Y):
        for h in range(8):
            hs[y, h] = zero
    for i, (d, y) in enumerate(EDGE):
        hs[y, WX - d] = left[i]
        hs[y, WX - 1 + d] = right[i]
    lane = lane_index(8)
    rows = []
    for j in range(2):
        n = len(EDGE) + j
        rows.append(jnp.where(lane < 32, pltpu.roll(left[n], 96, 1), pltpu.roll(right[n], 32, 1)))
    rows.append(jnp.zeros((112, L), jnp.float32))
    turned = jnp.concatenate(rows, axis=0).T
    for y in range(SPAN_Y):
        for h in range(8):
            distance = WX - h if h < WX else h - WX + 1
            if y not in x_range(distance):
                ha[y, h] = zero
                hb[y, h] = zero
                hx[y, h] = zero
                continue
            c = jnp.broadcast_to(turned[8 * h : 8 * h + 8, y : y + 1], (8, L))
            ax, bx = cell_terms(c, lanes)
            ok = valid[0] if h < WX else valid[1]
            if y < WY:
                ok = ok * valid[2]
            elif y >= WY + 8:
                ok = ok * valid[3]
            ax, bx = ax * ok, bx * ok
            s = hs[y, h]
            ha[y, h] = ax
            hb[y, h] = bx
            hx[y, h] = ax * s + bx * pltpu.roll(s, 64, 1)

    def split(own, halo):
        def get(y, x):
            if x < WX:
                return halo[y, x]
            if x < WX + 8:
                return own[y, x - WX]
            return halo[y, x - 8]

        return get

    source, a, b = split(own_s, hs), split(own_a, ha), split(own_b, hb)

    def whole(ref):
        return lambda y, x: ref[y, x]

    def sweep(old, new, margin):
        for y in range(margin, SPAN_Y - margin):
            for x in range(margin, SPAN_X - margin):
                distance = max(WX - x, x - WX - 7, 1)
                if not distance - 1 + margin <= y < SPAN_Y + 1 - margin - distance:
                    continue
                v = old(y, x)
                u = source(y, x) + (old(y, x + 1) + old(y, x - 1))
                u = u + (old(y + 1, x) + old(y - 1, x))
                u = u + (pltpu.roll(v, 1, 0) + pltpu.roll(v, 7, 0))
                new[y, x] = a(y, x) * u + b(y, x) * pltpu.roll(u, 64, 1)

    sweep(split(own_x, hx), x1, 1)
    sweep(whole(x1), x0, 2)
    sweep(whole(x0), x1, 3)
    lo, hi = WX, WX + 8

    def change(y, x):
        return x1[y, x] - x0[y, x]

    acc = zero
    faces = []
    for y in range(WY, WY + 8):
        line = zero
        for x in range(lo, hi):
            line = line + change(y, x)
        end = y in (WY, WY + 7)
        acc = acc + (5.0 if end else 6.0) * line
        acc = acc + (change(y, lo - 1) - change(y, lo)) + (change(y, hi) - change(y, hi - 1))
        if end:
            faces.append(line)
    solved = x1[WY : WY + 8, lo:hi].reshape(512, L)
    result = dot(solved, table, ((1,), (1,)), table_first=True)
    by_y = []
    for pair in range(4):
        cut = result[:, 128 * pair : 128 * pair + 128]
        by_y += list(halves(cut[: TM * TILES], cut[TM * TILES :]))
    out[...] = jnp.swapaxes(jnp.stack(by_y), 0, 1).reshape(TM * TILES * 8, L)
    homes = (
        strip >> 2,
        jnp.where(strip == 0, 4, (strip - 1) >> 2),
        jnp.where(strip == TM - 1, 5, (strip + 1) >> 2),
    )
    index = lax.broadcasted_iota(jnp.int32, (8, L), 0)
    share = jnp.where((index == 6) & (strip == 0), sums[...], 0.0)
    for home, v in zip(homes, (acc, *faces)):
        v = jnp.broadcast_to(jnp.sum(v, axis=0, keepdims=True), (8, L))
        share = share + jnp.where(index == home, v, 0.0)
    for d in range(TM):
        out[8 * (TILES * d + 4) : 8 * (TILES * d + 5), :] = share


def gather_kernel(received, out):
    block = received[0, 4]
    for d in range(1, TM):
        block = block + received[d, 4]
    for j in range(SX * SY):
        out[j] = block


def inverse_of(rows):
    rows = list(rows)
    index = lax.broadcasted_iota(jnp.int32, (8, L), 0)
    for p in range(8):
        here = index == p
        pivot = jnp.broadcast_to(rows[p][p : p + 1], (8, L))
        scale = 1.0 / pivot
        lead = jnp.where(here, scale, rows[p] * scale)
        for r in range(8):
            if r != p:
                factor = jnp.broadcast_to(rows[r][p : p + 1], (8, L))
                rows[r] = jnp.where(here, 0.0, rows[r]) - factor * lead
        rows[p] = lead
    return rows


def apply(rows, v):
    terms = [rows[c] * jnp.broadcast_to(v[c : c + 1], (8, L)) for c in range(8)]
    while len(terms) > 1:
        terms = [terms[i] + terms[i + 1] for i in range(0, len(terms), 2)]
    return terms[0]


def coarse_kernel(gathered, received, lanes, table, out, answer):
    index = lax.broadcasted_iota(jnp.int32, (8, L), 0)
    shift = jnp.broadcast_to(lanes[0:1, :] * float(VOLUME) + float(FACES), (8, L))

    by_row = [jnp.swapaxes(gathered[:, sy], 0, 1) for sy in range(SY)]

    def rows_of(sy, row):
        return by_row[sy][row]

    def right(m):
        sy, g = m // 4, m % 4
        rhs = rows_of(sy, g)
        if g == 0 and sy > 0:
            rhs = rhs + rows_of(sy - 1, 5)
        if g == 3 and sy < SY - 1:
            rhs = rhs + rows_of(sy + 1, 4)
        return rhs

    sums = [rows_of(sy, 6) for sy in range(SY)]

    def block(m, before):
        g = 32 * (m % 4)
        diagonal = jnp.broadcast_to(sums[m // 4][:, g : g + 1], (8, L)) + shift
        rows = []
        for r in range(8):
            row = jnp.where(index == r, diagonal, 0.0)
            row = jnp.where((index == r - 1) | (index == r + 1), -COUPLE_X, row)
            for other in before:
                row = row - (COUPLE_Y * COUPLE_Y) * other[r]
            rows.append(row)
        return rows

    inv, part = {}, {}

    def eliminate(m, sources):
        matrix = inverse_of(block(m, [inv[q] for q in sources]))
        rhs = right(m)
        for q in sources:
            rhs = rhs + COUPLE_Y * part[q]
        inv[m] = matrix
        part[m] = apply(matrix, rhs)

    for i in range(8):
        if i < 7:
            eliminate(i, [i - 1] if i else [])
        eliminate(15 - i, [16 - i] if i else [])
    eliminate(7, [6, 8])
    solved = {7: part[7]}
    for i in range(1, 9):
        for m, q in ((7 - i, 8 - i), (7 + i, 6 + i)):
            if 0 <= m < 16:
                solved[m] = part[m] + COUPLE_Y * apply(inv[m], solved[q])
    for m in range(16):
        answer[8 * m : 8 * m + 8, :] = solved[m]
    sx, sy = lax.axis_index("sx"), lax.axis_index("sy")
    own = table[pl.ds(pl.multiple_of(lax.axis_index("tm") * 8, 8), 8), :]
    group = lane_index(8) // 32
    added = jnp.zeros((8, L), jnp.float32)
    for g in range(4):
        y = answer[pl.ds((sy * 4 + g) * 8 + sx, 1), :]
        value = jnp.sum(own * y, axis=1, keepdims=True)
        added = jnp.where(group == g, value, added)
    for tp in range(4):
        rows = [received[MEMBER[s], tp] for s in range(TM)]
        turned = jnp.concatenate(rows, axis=0).T
        for t2 in range(2):
            t = 2 * tp + t2
            out[64 * t : 64 * t + 64, :] = x_major(turned[64 * t2 : 64 * t2 + 64]) + added[t : t + 1, :]


def call(kernel, name, out_shape, arrays, scratch=(), rates=None, keep=True, flops=0):
    if keep:
        out_shape = jax.tree.map(lambda o: pltpu.VMEM(o.shape, o.dtype), out_shape)
    if rates is None:
        arrays = [pltpu.with_memory_space_constraint(x, pltpu.VMEM) for x in arrays]
    scalars = [] if rates is None else [rates]
    limit = 24 * 2**20 if rates is None else None
    many = isinstance(out_shape, tuple)
    return pl.pallas_call(
        kernel,
        name=name,
        out_shape=out_shape,
        in_specs=smem(len(scalars)) + vmem(len(arrays)),
        out_specs=tuple(vmem(len(out_shape))) if many else vmem(1)[0],
        scratch_shapes=list(scratch),
        compiler_params=pltpu.CompilerParams(vmem_limit_bytes=limit),
        cost_estimate=pl.CostEstimate(flops=flops, transcendentals=0, bytes_accessed=0),
    )(*scalars, *arrays)


def swaps():
    def rank(g):
        return MEMBER[g % TM] * SY + g // TM

    pairs = [(rank(g), rank(g + 1)) for g in range(1, SY * TM - 1, 2)]
    return pairs + [(q, p) for p, q in pairs]


def local(driving_input, regime, reaction_rates):
    forward, inverse, natural, lanes = (jnp.asarray(t) for t in (FORWARD, INVERSE, NATURAL, LANES))
    packed, rate_rows, sums = call(
        pack_kernel,
        "pack",
        (shape(TM, 4 * ROWS, L), shape(L + 16, L), shape(8, L)),
        [driving_input.reshape(512, L), regime.reshape(64, L)],
        rates=reaction_rates,
    )
    received = lax.all_to_all(packed, "tm", split_axis=0, concat_axis=0, tiled=True)
    arrays = [received.reshape(TM * 4 * ROWS, L), rate_rows, forward]
    swap = call(swap_kernel, "swap_rows", shape(PART, 8, L), arrays)
    swapped = lax.ppermute(swap, ("tm", "sy"), swaps())
    window, rate = call(
        transform_kernel, "transform", (shape(8 * SPAN_Y, 8, L), shape(16, L)), arrays, flops=10**7
    )
    tiles = len(EDGE) + 2
    to_left, to_right = call(
        edge_kernel, "edges", (shape(tiles, 8, L),) * 2, [window, rate, swapped]
    )
    across = [(i, i + 1) for i in range(SX - 1)]
    left = lax.ppermute(to_right, "sx", across)
    right = lax.ppermute(to_left, "sx", [(q, p) for p, q in across])
    prepared = call(
        prepare_kernel,
        "prepare",
        (shape(SPAN_Y, 8, 8, L),) * 4,
        [window, rate, swapped, lanes],
        flops=10**7,
    )
    half = pltpu.VMEM((SPAN_Y, 8, 8, L), jnp.float32)
    message = call(
        solve_kernel,
        "sweeps",
        shape(TM * TILES * 8, L),
        [*prepared, left, right, sums, lanes, inverse],
        [half] * 4 + [pltpu.VMEM((SPAN_Y, SPAN_X, 8, L), jnp.float32)] * 2,
    )
    returned = lax.all_to_all(
        message.reshape(TM, TILES, 8, L), "tm", split_axis=0, concat_axis=0, tiled=True
    )
    shared = call(gather_kernel, "gather", shape(SX * SY, 8, L), [returned])
    gathered = lax.all_to_all(shared, ("sx", "sy"), split_axis=0, concat_axis=0, tiled=True)
    result = call(
        coarse_kernel,
        "coarse",
        shape(512, L),
        [gathered.reshape(SX, SY, 8, L), returned, lanes, natural],
        [pltpu.VMEM((L, L), jnp.float32)],
        keep=False,
    )
    return result.reshape(driving_input.shape)


def solution(mesh):
    placed = (P("tm", None, "sx", "sy"), P(None, "sx", "sy"), P())
    return jax.shard_map(
        local, mesh=mesh, in_specs=placed, out_specs=P("tm", None, "sx", "sy"), check_vma=False
    )
```
